128 devices in a mesh: lon: 16 (over x, y_hi, core), lat: 8 (over y_lo, z).
Axes of the slice: x: 4, y: 4 (y_hi: 2, y_lo: 2; y = y_hi * 2 + y_lo), z: 4, core: 2. Of those that a mesh axis runs over, the one named last changes fastest.
Arguments:
- normed: bfloat16 [8, 192, 384, 192], P(None, 'lat', 'lon'), may hold values from -6 to 6
- cotangent: bfloat16 [8, 192, 384, 192], P(None, 'lat', 'lon'), may hold values from -6 to 6
- weight_qkv: bfloat16 [192, 576], replicated, may hold values from -0.4375 to 0.4375
- weight_proj: bfloat16 [192, 192], replicated, may hold values from -0.4375 to 0.4375
- bias_table: bfloat16 [128, 6, 20736], P('lat'), may hold values from -6 to 390
Outputs:
- input_grad: bfloat16 [8, 192, 384, 192], P(None, 'lat', 'lon')
- qkv_grad: float32 [192, 576], replicated
- proj_grad: float32 [192, 192], replicated
- bias_grad: float32 [128, 6, 20736], P('lat')
The draws below stay inside these ranges and needn't reach their ends.
All inputs are finite; a program needn't handle non-finite values.
Results may differ from the reference program's by a relative error of at most 0.019.
Values may be sent and summed in bfloat16 or wider, within the bound.
A program may use at most 192 MiB of HBM per device.

```python
import jax
import jax.numpy as jnp
from jax import lax

C = 192
HEADS = 6
WIN_Z = 2
WIN_LAT = 6
WIN_LON = 12
WTOK = 144
NZ = 8
TYPES = 128
NLAT = 192
NLON = 384


def draw_bias_table(key, part):
    keys_list = jax.random.split(jax.random.fold_in(key, 17), 1)
    shape = (TYPES, HEADS, WTOK, WTOK)
    baseline = jnp.clip(jax.random.normal(keys_list[0], shape, jnp.float32), -6.0, 6.0)
    return baseline.reshape(TYPES, HEADS, WTOK * WTOK).astype(jnp.bfloat16)


def block_levels(stream_key, shape, shards, least, largest):
    factor_of, own = 1.0, jax.random.fold_in(stream_key, 6)
    for position, blocks in shards:
        heights = jnp.exp(jax.random.uniform(jax.random.fold_in(own, position), (blocks,), jnp.float32, least / len(shards), largest / len(shards)))
        factor_of = factor_of * jnp.repeat(heights, shape[position] // blocks).reshape([-1 if axis == position else 1 for axis in range(len(shape))])
    return factor_of


def gaussian(rng, dims, width, most, cuts=(), kind=jnp.bfloat16):
    level = block_levels(rng, dims, cuts, -0.22, 0.18) if cuts else 1.0
    entries = jax.random.normal(rng, dims, jnp.float32) * width * level
    return jnp.minimum(jnp.maximum(entries, -most), most).astype(kind)


def setup_inputs(seed: int = 0) -> dict:
    keys = jax.random.split(jax.random.key(seed), 6)
    return {
        "normed": gaussian(keys[0], (NZ, NLAT, NLON, C), 1.0, 6.0, ((1, 8), (2, 16))),
        "cotangent": gaussian(keys[1], (NZ, NLAT, NLON, C), 1.0, 6.0, ((1, 8), (2, 16))),
        "weight_qkv": gaussian(keys[2], (C, 3 * C), C ** -0.5, 0.4375),
        "weight_proj": gaussian(keys[3], (C, C), C ** -0.5, 0.4375),
        "bias_table": draw_bias_table(jax.random.fold_in(keys[5], 71), 0),
    }


def window_split(grid_field):
    levels, height, breadth = grid_field.shape[:3]
    trailing_dims = grid_field.shape[3:]
    shaped = grid_field.reshape((levels // WIN_Z, WIN_Z, height // WIN_LAT, WIN_LAT, breadth // WIN_LON, WIN_LON) + trailing_dims)
    axes_order = (0, 2, 4, 1, 3, 5) + tuple(range(6, 6 + len(trailing_dims)))
    return shaped.transpose(axes_order).reshape((-1, WTOK) + trailing_dims)


def window_merge(windowed, levels, height, breadth):
    channels = windowed.shape[-1]
    shaped = windowed.reshape(levels // WIN_Z, height // WIN_LAT, breadth // WIN_LON, WIN_Z, WIN_LAT, WIN_LON, channels)
    return shaped.transpose(0, 3, 1, 4, 2, 5, 6).reshape(levels, height, breadth, channels)


def window_backward(block_in, block_cot, block_region, block_live, block_types, bias_rows, weight_qkv, weight_proj):
    windows = block_in.shape[0]
    channels = block_in.shape[2]
    head_dim = channels // HEADS
    softmax_scale = head_dim ** -0.5
    high = lax.Precision.HIGHEST
    f32 = jnp.float32
    projected = jnp.einsum('bnc,cf->bnf', block_in.astype(f32), weight_qkv.astype(f32), precision=high).astype(jnp.bfloat16)
    projected = projected.reshape(windows, WTOK, 3, HEADS, head_dim)
    queries = projected[:, :, 0]
    key_rows = projected[:, :, 1]
    values = projected[:, :, 2]
    bias_add = jnp.dot(block_types, bias_rows.astype(f32), precision=high).reshape(windows, HEADS, WTOK, WTOK)
    scores = jnp.einsum('bqhd,bkhd->bhqk', queries.astype(f32), key_rows.astype(f32), precision=high) * softmax_scale + bias_add
    allowed = (block_region[:, :, None] == block_region[:, None, :]) & (block_live[:, :, None] == block_live[:, None, :])
    allowed = allowed[:, None]
    peak_score = jnp.max(jnp.where(allowed, scores, -1e30), axis=-1, keepdims=True)
    exp_terms = jnp.where(allowed, jnp.exp(scores - peak_score), 0.0)
    attn_probs = exp_terms / jnp.sum(exp_terms, axis=-1, keepdims=True)
    probs_b = attn_probs.astype(jnp.bfloat16)
    mixed = jnp.einsum('bhqk,bkhd->bqhd', probs_b.astype(f32), values.astype(f32), precision=high).astype(jnp.bfloat16)
    mixed = mixed.reshape(windows, WTOK, channels)
    grad_proj = jnp.einsum('bnc,bnf->cf', mixed.astype(f32), block_cot.astype(f32), precision=high)
    mixed_grad = jnp.einsum('bnf,cf->bnc', block_cot.astype(f32), weight_proj.astype(f32), precision=high).astype(jnp.bfloat16)
    mixed_grad = mixed_grad.reshape(windows, WTOK, HEADS, head_dim)
    prob_grad = jnp.einsum('bqhd,bkhd->bhqk', mixed_grad.astype(f32), values.astype(f32), precision=high)
    row_delta = jnp.sum(attn_probs * prob_grad, axis=-1, keepdims=True)
    score_grad = attn_probs * (prob_grad - row_delta)
    grad_bias = jnp.dot(block_types.T, score_grad.reshape(windows, -1), precision=high)
    score_grad_b = score_grad.astype(jnp.bfloat16).astype(f32)
    query_grad = (jnp.einsum('bhqk,bkhd->bqhd', score_grad_b, key_rows.astype(f32), precision=high) * softmax_scale).astype(jnp.bfloat16)
    key_grad = (jnp.einsum('bhqk,bqhd->bkhd', score_grad_b, queries.astype(f32), precision=high) * softmax_scale).astype(jnp.bfloat16)
    value_grad = jnp.einsum('bhqk,bqhd->bkhd', probs_b.astype(f32), mixed_grad.astype(f32), precision=high).astype(jnp.bfloat16)
    cols_grad = jnp.stack([query_grad, key_grad, value_grad], axis=2).reshape(windows, WTOK, 3 * channels)
    grad_qkv = jnp.einsum('bnc,bnf->cf', block_in.astype(f32), cols_grad.astype(f32), precision=high)
    grad_in = jnp.einsum('bnf,cf->bnc', cols_grad.astype(f32), weight_qkv.astype(f32), precision=high).astype(jnp.bfloat16)
    return grad_in, grad_qkv, grad_proj, grad_bias


def reference(normed, cotangent, weight_qkv, weight_proj, bias_table):
    levels, height, breadth, channels = normed.shape
    level_shift = WIN_Z // 2
    lat_shift = WIN_LAT // 2
    lon_shift = WIN_LON // 2

    def to_frame(grid_field):
        rolled = jnp.roll(jnp.roll(grid_field, -lon_shift, axis=2), -level_shift, axis=0)
        padding = jnp.zeros((levels, lat_shift, breadth, channels), grid_field.dtype)
        return jnp.concatenate([rolled[:, lat_shift:], padding], axis=1)

    framed_in = window_split(to_frame(normed))
    framed_cot = window_split(to_frame(cotangent))
    level_index = jnp.arange(levels, dtype=jnp.int32)
    wrapped_levels = (level_index >= levels - level_shift).astype(jnp.int32)
    wrapped_field = jnp.broadcast_to(wrapped_levels[:, None, None], (levels, height, breadth))
    region_win = window_split(wrapped_field)
    row_index = jnp.arange(height, dtype=jnp.int32)
    live_rows = row_index < height - lat_shift
    live_field = jnp.broadcast_to(live_rows[None, :, None], (levels, height, breadth))
    live_win = window_split(live_field)
    level_windows = levels // WIN_Z
    lat_windows = height // WIN_LAT
    lon_windows = breadth // WIN_LON
    level_part = jnp.arange(level_windows, dtype=jnp.int32)[:, None, None]
    lat_part = jnp.arange(lat_windows, dtype=jnp.int32)[None, :, None]
    kinds = jnp.broadcast_to(lat_part * level_windows + level_part, (level_windows, lat_windows, lon_windows))
    onehot = (kinds.reshape(-1)[:, None] == jnp.arange(TYPES, dtype=jnp.int32)[None, :]).astype(jnp.float32)
    bias_rows = bias_table.reshape(TYPES, -1)
    window_total = framed_in.shape[0]
    block_size = max(divisor for divisor in range(1, 65) if window_total % divisor == 0)
    blocks = window_total // block_size

    def regroup(array):
        return array.reshape((blocks, block_size) + array.shape[1:])

    def step_block(totals, pieces):
        grad_in, grad_qkv, grad_proj, grad_bias = window_backward(pieces[0], pieces[1], pieces[2], pieces[3], pieces[4], bias_rows, weight_qkv, weight_proj)
        return (totals[0] + grad_qkv, totals[1] + grad_proj, totals[2] + grad_bias), grad_in

    start = (jnp.zeros((channels, 3 * channels), jnp.float32), jnp.zeros((channels, channels), jnp.float32), jnp.zeros((TYPES, HEADS * WTOK * WTOK), jnp.float32))
    totals, grads = lax.scan(step_block, start, (regroup(framed_in), regroup(framed_cot), regroup(region_win), regroup(live_win), regroup(onehot)))
    framed_grad = window_merge(grads.reshape(window_total, WTOK, channels), levels, height, breadth)
    zeros_rows = jnp.zeros((levels, lat_shift, breadth, channels), jnp.bfloat16)
    unshifted = jnp.concatenate([zeros_rows, framed_grad[:, :height - lat_shift]], axis=1)
    input_grad = jnp.roll(jnp.roll(unshifted, lon_shift, axis=2), level_shift, axis=0)
    return input_grad, totals[0], totals[1], totals[2].reshape(TYPES, HEADS, WTOK * WTOK)
```

```python
import functools
import jax
import jax.numpy as jnp
from jax import lax
from jax.experimental import pallas as pl
from jax.experimental.pallas import tpu as pltpu
from jax.sharding import PartitionSpec as P

HEADS = 6
WIN_Z = 2
WIN_LAT = 6
WIN_LON = 12
WTOK = 144
HD = 32
C = 192
MAIN = 128
TAIL = WTOK - MAIN
PACK = 896
SCALE = HD ** -0.5
LOG2E = 1.4426950408889634
BF = jnp.bfloat16
F32 = jnp.float32


def dot(a, b):
    return jnp.dot(a, b, preferred_element_type=F32)


def lane_head(shape):
    return lax.broadcasted_iota(jnp.int32, shape, 1) // HD


def core_kernel(x_ref, g_ref, wq_ref, wqt_ref, wpt_ref, bias_ref, penz_ref, penl_ref,
                gin_ref, gq_ref, gp_ref, gb_ref, gsum):
    t = pl.program_id(0)
    last = (lax.axis_index("lat") == lax.axis_size("lat") - 1)
    z_on = (t % 4 == 3).astype(F32)
    l_on = (jnp.logical_and(last, t // 4 == 3)).astype(F32)

    @pl.when(t == 0)
    def _():
        gq_ref[...] = jnp.zeros_like(gq_ref)
        gp_ref[...] = jnp.zeros_like(gp_ref)

    x = x_ref[0]
    cot = g_ref[0]
    proj = dot(x, wq_ref[...]).astype(BF)
    dmix = dot(cot, wpt_ref[...]).astype(BF)
    xt = x.T
    dq_l, dk_l, dv_l, mixm, mixt, cott = [], [], [], [], [], []
    for c in range(2):
        rows = slice(c * WTOK, (c + 1) * WTOK)
        q = proj[rows, 0:192]
        k = proj[rows, 256:448]
        v = proj[rows, 512:704]
        dm = dmix[rows]
        ct = cot[rows]
        qt, kt, vt, dmt = q.T, k.T, v.T, dm.T
        hm = lane_head((MAIN, C))
        ht = lane_head((TAIL, C))
        zq = jnp.zeros((HD, MAIN), BF)

        def blk(at, p):
            top = jnp.concatenate([at[64 * p:64 * p + 32, :MAIN], zq], axis=1)
            bot = jnp.concatenate([zq, at[64 * p + 32:64 * p + 64, :MAIN]], axis=1)
            two = jnp.concatenate([top, bot], axis=0)
            if p == 2:
                return two
            z64 = jnp.zeros((64, 256), BF)
            return jnp.concatenate([two, z64] if p == 0 else [z64, two], axis=0)

        def nat(a, p):
            lanes = slice(0, 128) if p < 2 else slice(128, 192)
            am = a[:MAIN, lanes]
            hh = hm[:, lanes]
            z = jnp.zeros_like(am)
            return jnp.concatenate([jnp.where(hh == 2 * p, am, z), jnp.where(hh == 2 * p + 1, am, z)], axis=0)

        def nat_tail(a):
            am = a[MAIN:]
            z = jnp.zeros_like(am)
            return jnp.concatenate([jnp.where(ht == h, am, z) for h in range(HEADS)], axis=0)

        q_tail, dm_tail = nat_tail(q), nat_tail(dm)
        dn = (((1,), (1,)), ((), ()))
        dk_a = dk_b = dv_a = dv_b = None
        mix_parts, dq_parts = [], []
        for p in range(4):
            if p < 3:
                ln = slice(256 * p, 256 * p + 256)
                sub = slice(0, 128) if p < 2 else slice(128, 192)
                s = dot(k[:, sub], blk(qt, p))
                dp = dot(v[:, sub], blk(dmt, p))
            else:
                ln = slice(768, 864)
                s = lax.dot_general(k, q_tail, dn, preferred_element_type=F32)
                dp = lax.dot_general(v, dm_tail, dn, preferred_element_type=F32)
            bias = bias_ref[0, :, ln].astype(F32) * LOG2E + z_on * penz_ref[:, ln].astype(F32) + l_on * penl_ref[:, ln].astype(F32)
            s = s * (SCALE * LOG2E) + bias
            m = jnp.max(s, axis=0, keepdims=True)
            e = jnp.exp2(s - m)
            r = 1.0 / jnp.sum(e, axis=0, keepdims=True)
            pr = e * r
            pb = pr.astype(BF)
            d = jnp.sum(pr * dp, axis=0, keepdims=True)
            gs = pr * (dp - d)
            gb = gs.astype(BF)
            if c == 0:
                gsum[:, ln] = gs
            else:
                gb_ref[0, :, ln] = (gsum[:, ln] + gs).astype(BF)
            if p < 3:
                mo = dot(vt[64 * p:64 * p + 64], pb).astype(BF)
                do = dot(kt[64 * p:64 * p + 64], gb)
                mix_parts += [mo[:32, :MAIN], mo[32:, MAIN:]]
                dq_parts += [do[:32, :MAIN], do[32:, MAIN:]]
                dkp = dot(gb, nat(q, p))
                dvp = dot(pb, nat(dm, p))
                if p < 2:
                    dk_a = dkp if dk_a is None else dk_a + dkp
                    dv_a = dvp if dv_a is None else dv_a + dvp
                else:
                    dk_b, dv_b = dkp, dvp
            else:
                mo = dot(vt, pb).astype(BF)
                do = (dot(kt, gb) * SCALE).astype(BF)
                rh = lax.broadcasted_iota(jnp.int32, (C, 96), 0) // HD
                lh = lax.broadcasted_iota(jnp.int32, (C, 96), 1) // TAIL
                mixt.append(jnp.where(rh == lh, mo, jnp.zeros_like(mo)))
                dot_t = do.T
                dq_tail = jnp.zeros((TAIL, C), BF)
                for h in range(HEADS):
                    dq_tail = jnp.where(ht == h, dot_t[TAIL * h:TAIL * h + TAIL], dq_tail)
                dk_a = dk_a + dot(gb, q_tail[:, :128])
                dk_b = dk_b + dot(gb, q_tail[:, 128:])
                dv_a = dv_a + dot(pb, dm_tail[:, :128])
                dv_b = dv_b + dot(pb, dm_tail[:, 128:])
        mixm.append(jnp.concatenate(mix_parts, axis=0))
        dqt = (jnp.concatenate(dq_parts, axis=0) * SCALE).astype(BF)
        dq_l.append(jnp.concatenate([dqt.T, dq_tail], axis=0))
        dk_l.append((jnp.concatenate([dk_a, dk_b], axis=1) * SCALE).astype(BF))
        dv_l.append(jnp.concatenate([dv_a, dv_b], axis=1).astype(BF))
        cott.append(jnp.concatenate([ct[MAIN:]] * HEADS, axis=0))
    mm = jnp.concatenate(mixm, axis=1)
    cm = jnp.concatenate([cot[0:MAIN], cot[WTOK:WTOK + MAIN]], axis=0)
    gp_ref[...] += dot(mm, cm) + dot(mixt[0], cott[0]) + dot(mixt[1], cott[1])
    dq = jnp.concatenate(dq_l, axis=0)
    dk = jnp.concatenate(dk_l, axis=0)
    dv = jnp.concatenate(dv_l, axis=0)
    gq_ref[0] += dot(xt, dq)
    gq_ref[1] += dot(xt, dk)
    gq_ref[2] += dot(xt, dv)
    gin = dot(dq, wqt_ref[0]) + dot(dk, wqt_ref[1]) + dot(dv, wqt_ref[2])
    gin_ref[0] = gin.astype(BF)


def penalties():
    k = jnp.arange(WTOK, dtype=jnp.int32)
    lane = jnp.arange(PACK, dtype=jnp.int32)
    q = jnp.where(lane < 768, lane % 128, 128 + lane % 16)
    z = (k[:, None] // 72) != (q[None, :] // 72)
    l = ((k[:, None] // 12) % 6 >= 3) != ((q[None, :] // 12) % 6 >= 3)
    return jnp.where(z, -1e30, 0.0).astype(BF), jnp.where(l, -1e30, 0.0).astype(BF)


def run_core(xw, gw, weight_qkv, weight_proj, bias_p):
    n = xw.shape[0]
    wq = weight_qkv.reshape(C, 3, C)
    wq_pad = jnp.pad(wq, ((0, 0), (0, 0), (0, 64))).reshape(C, 768)
    wqt = wq.transpose(1, 2, 0)
    wpt = weight_proj.T
    penz, penl = penalties()
    whole = lambda *s: pl.BlockSpec(s, lambda t: (0,) * len(s))
    return pl.pallas_call(
        core_kernel,
        grid=(n,),
        in_specs=[
            pl.BlockSpec((1, 2 * WTOK, C), lambda t: (t, 0, 0)),
            pl.BlockSpec((1, 2 * WTOK, C), lambda t: (t, 0, 0)),
            whole(C, 768), whole(3, C, C), whole(C, C),
            pl.BlockSpec((1, WTOK, PACK), lambda t: (t, 0, 0)),
            whole(WTOK, PACK), whole(WTOK, PACK),
        ],
        out_specs=[
            pl.BlockSpec((1, 2 * WTOK, C), lambda t: (t, 0, 0)),
            whole(3, C, C), whole(C, C),
            pl.BlockSpec((1, WTOK, PACK), lambda t: (t, 0, 0)),
        ],
        out_shape=[
            jax.ShapeDtypeStruct((n, 2 * WTOK, C), BF),
            jax.ShapeDtypeStruct((3, C, C), F32),
            jax.ShapeDtypeStruct((C, C), F32),
            jax.ShapeDtypeStruct((n, WTOK, PACK), BF),
        ],
        scratch_shapes=[pltpu.VMEM((WTOK, PACK), F32)],
        name="core",
    )(xw, gw, wq_pad, wqt, wpt, bias_p, penz, penl)


def bias_pack(bias_table):
    n = bias_table.shape[0]
    b = bias_table.reshape(n, HEADS, WTOK, WTOK).transpose(0, 3, 1, 2)
    main = b[..., :MAIN].reshape(n, WTOK, HEADS * MAIN)
    tail = b[..., MAIN:].reshape(n, WTOK, HEADS * TAIL)
    return jnp.concatenate([main, tail, jnp.zeros((n, WTOK, 32), b.dtype)], axis=2)


def bias_unpack(g):
    n = g.shape[0]
    main = g[..., :768].reshape(n, WTOK, HEADS, MAIN)
    tail = g[..., 768:864].reshape(n, WTOK, HEADS, TAIL)
    b = jnp.concatenate([main, tail], axis=3)
    return b.transpose(0, 2, 3, 1).reshape(n, HEADS, WTOK * WTOK)


def passed_along(block, axis, distance):
    devices = range(lax.axis_size(axis))
    route = [(i - distance, i) for i in devices if i - distance in devices]
    return lax.ppermute(block, axis, route)


def from_behind(block, axis, distance):
    devices = range(lax.axis_size(axis))
    route = [((i - distance) % len(devices), i) for i in devices]
    return lax.ppermute(block, axis, route)


def split_types(f):
    z, h, w, c = f.shape
    f = f.reshape(z // 2, 2, h // 6, 6, w // 12, 12, c).transpose(2, 0, 4, 1, 3, 5, 6)
    return f.reshape((h // 6) * (z // 2), (w // 12) * WTOK, c)


def merge_types(g, z, h, w):
    c = g.shape[-1]
    g = g.reshape(h // 6, z // 2, w // 12, 2, 6, 12, c).transpose(1, 3, 0, 4, 2, 5, 6)
    return g.reshape(z, h, w, c)


def frame(a):
    a = jnp.roll(a, -1, axis=0)
    up = passed_along(a[:, :3], "lat", -1)
    tall = jnp.concatenate([a[:, 3:], up], axis=1)
    across = from_behind(tall[:, :, :6], "lon", -1)
    return jnp.concatenate([tall[:, :, 6:], across], axis=2)


def of_everyone(x, axis):
    n = lax.axis_size(axis)
    e = lax.all_to_all(jnp.broadcast_to(x[None], (n, *x.shape)), axis, 0, 0, tiled=True)
    return jnp.sum(e.astype(F32), axis=0)


def local(normed, cotangent, weight_qkv, weight_proj, bias_table):
    levels, height, breadth, channels = normed.shape
    xw = split_types(frame(normed))
    gw = split_types(frame(cotangent))
    bias_p = bias_pack(bias_table)
    gin, gq, gp, gb = run_core(xw, gw, weight_qkv, weight_proj, bias_p)
    fg = merge_types(gin, levels, height, breadth)
    side = from_behind(fg[:, :, breadth - 6:], "lon", 1)
    tall = jnp.concatenate([side, fg[:, :, :breadth - 6]], axis=2)
    ret = passed_along(tall[:, height - 3:], "lat", 1)
    input_grad = jnp.roll(jnp.concatenate([ret, tall[:, :height - 3]], axis=1), 1, axis=0)
    gb = lax.psum_scatter(gb, "lon", scatter_dimension=0, tiled=True)
    gb = lax.all_gather(bias_unpack(gb), "lon", axis=0, tiled=True)
    bias_grad = gb.astype(F32)
    w = jnp.concatenate([gq.transpose(1, 0, 2).reshape(C, 3 * C), gp], axis=1).astype(BF)
    w = of_everyone(w, "lat")
    w = lax.psum(w.astype(BF), "lon").astype(F32)
    return input_grad, w[:, :3 * C], w[:, 3 * C:], bias_grad


def solution(mesh):
    in_specs = (P(None, "lat", "lon", None), P(None, "lat", "lon", None), P(), P(), P("lat", None, None))
    out_specs = (P(None, "lat", "lon", None), P(), P(), P("lat", None, None))
    return jax.shard_map(local, mesh=mesh, in_specs=in_specs, out_specs=out_specs, check_vma=False)
```

```python
import functools
import jax
import jax.numpy as jnp
from jax import lax
from jax.experimental import pallas as pl
from jax.experimental.pallas import tpu as pltpu
from jax.sharding import PartitionSpec as P

HEADS = 6
WTOK = 144
HD = 32
C = 192
MAIN = 128
TAIL = WTOK - MAIN
PACK = 896
NT = 16
SCALE = HD ** -0.5
LOG2E = 1.4426950408889634
BF = jnp.bfloat16
F32 = jnp.float32
MESH = pl.DeviceIdType.MESH
LEAD = 6
FIRST_PAIRS = 6
STEPS = 23


def dot(a, b):
    return jnp.dot(a, b, preferred_element_type=F32)


def lane_head(shape):
    return lax.broadcasted_iota(jnp.int32, shape, 1) // HD


def pack_kernel(b_ref, main_ref, tail_ref, sc):
    lane = lax.broadcasted_iota(jnp.int32, (NT, 128), 1)

    def group(g, _):
        base = pl.multiple_of(g * 1152, 128)
        tiles = [b_ref[0, :, pl.ds(base + 128 * j, 128)].astype(F32) for j in range(9)]
        for j in range(8):
            if j == 0:
                main, sec = tiles[0], tiles[1]
            else:
                r = pltpu.roll(tiles[j], 128 - 16 * j, 1)
                sec = pltpu.roll(tiles[j + 1], 128 - 16 * j, 1)
                main = jnp.where(lane < 128 - 16 * j, r, sec)
            row = pl.multiple_of(g * 128 + 16 * j, 16)
            sc[0, pl.ds(row, NT), :] = main
            sc[1, pl.ds(row, NT), :] = sec
        return 0

    lax.fori_loop(0, 18, group, 0, unroll=9)
    for t in range(NT):
        a = sc[0, pl.ds(t, WTOK, stride=NT), :].astype(BF)
        b = sc[1, pl.ds(t, WTOK, stride=NT), :].astype(BF)
        main_ref[t, 0:128, :] = a[:MAIN].T
        main_ref[t, 128:144, :] = b[:MAIN].T[:16]
        tail_ref[t, :, 0:128] = a[MAIN:]
        tail_ref[t, :, 128:144] = b[MAIN:, 0:16]


def pack(bias_view):
    return pl.pallas_call(
        pack_kernel, grid=(6,),
        in_specs=[pl.BlockSpec((1, NT, WTOK * WTOK), lambda h: (h, 0, 0))],
        out_specs=[pl.BlockSpec((NT, WTOK, MAIN), lambda h: (0, 0, h)),
                   pl.BlockSpec((NT, 16, WTOK), lambda h: (0, h, 0))],
        out_shape=[jax.ShapeDtypeStruct((NT, WTOK, 6 * MAIN), BF), jax.ShapeDtypeStruct((NT, 96, WTOK), BF)],
        scratch_shapes=[pltpu.VMEM((2, WTOK * NT, 128), F32)], name="pack",
        cost_estimate=pl.CostEstimate(flops=10**9, bytes_accessed=8 * 2**20, transcendentals=0),
    )(bias_view)


def unpack_kernel(m_ref, t_ref, out_ref, sc, tn):
    h = pl.program_id(0)

    @pl.when(h == 0)
    def _():
        for t in range(NT):
            tn[t] = t_ref[t].reshape(WTOK, 128).T

    for t in range(NT):
        m = m_ref[t].reshape(WTOK, 128)
        sc[0, pl.ds(t, MAIN, stride=NT), :] = m[:MAIN].T.astype(F32)
        sc[1, pl.ds(t, MAIN, stride=NT), 0:16] = m[MAIN:].T.astype(F32)
        tl = tn[t, pl.ds(pl.multiple_of(h * 16, 16), 16), :].astype(F32)
        sc[0, pl.ds(MAIN * NT + t, 16, stride=NT), :] = tl[:, :128]
        sc[1, pl.ds(MAIN * NT + t, 16, stride=NT), 0:16] = tl[:, 128:]
    lane = lax.broadcasted_iota(jnp.int32, (NT, 128), 1)

    def group(g, _):
        base = pl.multiple_of(g * 1152, 128)
        r, s = [], []
        for j in range(8):
            row = pl.multiple_of(g * 128 + 16 * j, 16)
            m = sc[0, pl.ds(row, NT), :]
            t = sc[1, pl.ds(row, NT), :]
            r.append(pltpu.roll(m, 16 * j, 1) if j else m)
            s.append(pltpu.roll(t, 16 * j, 1) if j else t)
        for j in range(9):
            if j == 0:
                v = r[0]
            else:
                low = jnp.where(lane < 16 * (j - 1), r[j - 1], s[j - 1]) if j > 1 else s[0]
                v = jnp.where(lane < 16 * j, low, r[j]) if j < 8 else low
            out_ref[0, :, pl.ds(base + 128 * j, 128)] = v
        return 0

    lax.fori_loop(0, 18, group, 0, unroll=9)


def unpack(f):
    return pl.pallas_call(
        unpack_kernel, grid=(6,),
        in_specs=[pl.BlockSpec((NT, 9, 16, 128), lambda h: (0, h, 0, 0)),
                  pl.BlockSpec((NT, 9, 16, 128), lambda h: (0, 6, 0, 0))],
        out_specs=pl.BlockSpec((1, NT, WTOK * WTOK), lambda h: (h, 0, 0)),
        out_shape=jax.ShapeDtypeStruct((6, NT, WTOK * WTOK), F32),
        scratch_shapes=[pltpu.VMEM((2, WTOK * NT, 128), F32), pltpu.VMEM((NT, 128, WTOK), BF)], name="unpack",
        cost_estimate=pl.CostEstimate(flops=10**9, bytes_accessed=12 * 2**20, transcendentals=0),
    )(f, f)


def add(*parts):
    total = parts[0].astype(F32)
    for part in parts[1:]:
        total = total + part.astype(F32)
    return total.astype(BF)


def window_pair(s, x2, g2, t_of, wq_ref, wqt_ref, wpt_ref, bm_ref, bt_ref, penz_ref, penl_ref, lat_last,
                gq, gp, gsum, gbuf):
    x = x2[...]
    cot = g2[...]
    proj = dot(x, wq_ref[...]).astype(BF)
    dmix = dot(cot, wpt_ref[...]).astype(BF)
    xt = x.T
    dq_l, dk_l, dv_l, mixm, mixt, cott = [], [], [], [], [], []
    for c in range(2):
        t = t_of[c]
        z_on = (t % 4 == 3).astype(F32)
        l_on = jnp.logical_and(lat_last, t // 4 == 3).astype(F32)
        rows = slice(c * WTOK, (c + 1) * WTOK)
        q = proj[rows, 0:192]
        k = proj[rows, 256:448]
        v = proj[rows, 512:704]
        dm = dmix[rows]
        ct = cot[rows]
        qt, kt, vt, dmt = q.T, k.T, v.T, dm.T
        hm = lane_head((MAIN, C))
        ht = lane_head((TAIL, C))
        zq = jnp.zeros((HD, MAIN), BF)

        def blk(at, p):
            top = jnp.concatenate([at[64 * p:64 * p + 32, :MAIN], zq], axis=1)
            bot = jnp.concatenate([zq, at[64 * p + 32:64 * p + 64, :MAIN]], axis=1)
            two = jnp.concatenate([top, bot], axis=0)
            if p == 2:
                return two
            z64 = jnp.zeros((64, 256), BF)
            return jnp.concatenate([two, z64] if p == 0 else [z64, two], axis=0)

        def nat(a, p):
            lanes = slice(0, 128) if p < 2 else slice(128, 192)
            am = a[:MAIN, lanes]
            hh = hm[:, lanes]
            z = jnp.zeros_like(am)
            return jnp.concatenate([jnp.where(hh == 2 * p, am, z), jnp.where(hh == 2 * p + 1, am, z)], axis=0)

        def nat_tail(a):
            am = a[MAIN:]
            z = jnp.zeros_like(am)
            return jnp.concatenate([jnp.where(ht == h, am, z) for h in range(HEADS)], axis=0)

        q_tail, dm_tail = nat_tail(q), nat_tail(dm)
        dn = (((1,), (1,)), ((), ()))
        dk_a = dk_b = dv_a = dv_b = None
        mix_parts, dq_parts = [], []
        for p in range(4):
            if p < 3:
                ln = slice(256 * p, 256 * p + 256)
                sub = slice(0, 128) if p < 2 else slice(128, 192)
                s_ = dot(k[:, sub], blk(qt, p))
                dp = dot(v[:, sub], blk(dmt, p))
                bias = bm_ref[t, :, ln].astype(F32)
            else:
                ln = slice(768, 864)
                s_ = lax.dot_general(k, q_tail, dn, preferred_element_type=F32)
                dp = lax.dot_general(v, dm_tail, dn, preferred_element_type=F32)
                bias = bt_ref[t].T.astype(F32)
            bias = bias * LOG2E + z_on * penz_ref[:, ln].astype(F32) + l_on * penl_ref[:, ln].astype(F32)
            s_ = s_ * (SCALE * LOG2E) + bias
            m = jnp.max(s_, axis=0, keepdims=True)
            e = jnp.exp2(s_ - m)
            r = 1.0 / jnp.sum(e, axis=0, keepdims=True)
            pr = e * r
            pb = pr.astype(BF)
            d = jnp.sum(pr * dp, axis=0, keepdims=True)
            gs = pr * (dp - d)
            gb = gs.astype(BF)
            tot = gsum[t, :, ln] + gs
            gsum[t, :, ln] = tot
            tot = tot.astype(BF)
            if p < 3:
                gbuf[t, 18 * p:18 * p + 9] = tot[:, :128].reshape(9, 16, 128)
                gbuf[t, 18 * p + 9:18 * p + 18] = tot[:, 128:].reshape(9, 16, 128)
            else:
                gbuf[t, 54:63, :, 0:96] = tot.reshape(9, 16, 96)
            if p < 3:
                mo = dot(vt[64 * p:64 * p + 64], pb).astype(BF)
                do = dot(kt[64 * p:64 * p + 64], gb)
                mix_parts += [mo[:32, :MAIN], mo[32:, MAIN:]]
                dq_parts += [do[:32, :MAIN], do[32:, MAIN:]]
                dkp = dot(gb, nat(q, p))
                dvp = dot(pb, nat(dm, p))
                if p < 2:
                    dk_a = dkp if dk_a is None else dk_a + dkp
                    dv_a = dvp if dv_a is None else dv_a + dvp
                else:
                    dk_b, dv_b = dkp, dvp
            else:
                mo = dot(vt, pb).astype(BF)
                do = (dot(kt, gb) * SCALE).astype(BF)
                rh = lax.broadcasted_iota(jnp.int32, (C, 96), 0) // HD
                lh = lax.broadcasted_iota(jnp.int32, (C, 96), 1) // TAIL
                mixt.append(jnp.where(rh == lh, mo, jnp.zeros_like(mo)))
                dot_t = do.T
                dq_tail = jnp.zeros((TAIL, C), BF)
                for h in range(HEADS):
                    dq_tail = jnp.where(ht == h, dot_t[TAIL * h:TAIL * h + TAIL], dq_tail)
                dk_a = dk_a + dot(gb, q_tail[:, :128])
                dk_b = dk_b + dot(gb, q_tail[:, 128:])
                dv_a = dv_a + dot(pb, dm_tail[:, :128])
                dv_b = dv_b + dot(pb, dm_tail[:, 128:])
        mixm.append(jnp.concatenate(mix_parts, axis=0))
        dqt = (jnp.concatenate(dq_parts, axis=0) * SCALE).astype(BF)
        dq_l.append(jnp.concatenate([dqt.T, dq_tail], axis=0))
        dk_l.append((jnp.concatenate([dk_a, dk_b], axis=1) * SCALE).astype(BF))
        dv_l.append(jnp.concatenate([dv_a, dv_b], axis=1).astype(BF))
        cott.append(jnp.concatenate([ct[MAIN:]] * HEADS, axis=0))
    mm = jnp.concatenate(mixm, axis=1)
    cm = jnp.concatenate([cot[0:MAIN], cot[WTOK:WTOK + MAIN]], axis=0)
    gp[...] += dot(mm, cm) + dot(mixt[0], cott[0]) + dot(mixt[1], cott[1])
    dq = jnp.concatenate(dq_l, axis=0)
    dk = jnp.concatenate(dk_l, axis=0)
    dv = jnp.concatenate(dv_l, axis=0)
    gq[0] += dot(xt, dq)
    gq[1] += dot(xt, dk)
    gq[2] += dot(xt, dv)
    return dot(dq, wqt_ref[0]) + dot(dk, wqt_ref[1]) + dot(dv, wqt_ref[2])


def fused_kernel(x_hbm, g_hbm, wq_ref, wqt_ref, wpt_ref, bm_ref, bt_ref, penz_ref, penl_ref, so_ref, se_ref,
                 to_ref, te_ref, out_ref, w_ref, f_hbm,
                 xo, go, xe, ge, x2, g2, fo, fe, fw, fs, gq, gp, gsum, gbuf, rd, hb, xa, xs, xb, ys, yr, fin,
                 wb, wr, wh, wx, wy, wz, wf,
                 load_sem, halo_s, halo_r, ss, rs, ws, wrs, out_sem):
    lon = lax.axis_index("lon")
    lat = lax.axis_index("lat")
    n_lon = 16
    core = lon % 2
    yh = (lon // 2) % 2
    xx = lon // 4
    zz = lat % 4
    yl = lat // 4
    yy = yh * 2 + yl
    partner = lon + 1 - 2 * core
    right = (lon + 4) % n_lon
    left = (lon + 12) % n_lon
    ymate = lon + 2 - 4 * yh
    east = (lon + 1) % n_lon
    west = (lon + 15) % n_lon
    has_south = lat < 7
    has_north = lat > 0
    lat_last = lat == 7

    def peer(lon_, lat_):
        return {"lon": lon_, "lat": lat_}

    def xpeer(d):
        return peer((xx + d) % 4 * 4 + yh * 2 + core, lat)

    def ypeer(d):
        o = (yy + d) % 4
        return peer(xx * 4 + o // 2 * 2 + core, o % 2 * 4 + zz)

    def zpeer(d):
        return peer(lon, yl * 4 + (zz + d) % 4)

    def remote(src, dst, ssem, rsem, dev):
        return pltpu.make_async_remote_copy(src_ref=src, dst_ref=dst, send_sem=ssem, recv_sem=rsem,
                                            device_id=dev, device_id_type=MESH)

    own_loads = [pltpu.make_async_copy(x_hbm, xo.at[:, 0:24], load_sem.at[0]),
                 pltpu.make_async_copy(g_hbm, go.at[:, 0:24], load_sem.at[1])]
    for cp in own_loads:
        cp.start()
    for buf in (xe, ge):
        buf[...] = jnp.zeros_like(buf)
    for buf in (xo, go):
        buf[:, 24:27] = jnp.zeros((8, 3, 24, C), BF)
    for buf in (fw, fs):
        buf[...] = jnp.zeros_like(buf)

    barrier = pltpu.get_barrier_semaphore()
    greet = [peer(partner, lat), xpeer(1), xpeer(2), xpeer(3)] + [ypeer(d) for d in (1, 2, 3)] + [zpeer(d) for d in (1, 2, 3)]
    for dev in greet:
        pl.semaphore_signal(barrier, inc=1, device_id=dev, device_id_type=MESH)
    for dev in (peer(east, lat), peer(west, lat)):
        pl.semaphore_signal(barrier, inc=1, device_id=dev, device_id_type=MESH)

    @pl.when(has_north)
    def _():
        pl.semaphore_signal(barrier, inc=1, device_id=peer(lon, lat - 1), device_id_type=MESH)
        pl.semaphore_signal(barrier, inc=1, device_id=peer(west, lat - 1), device_id_type=MESH)

    @pl.when(has_south)
    def _():
        pl.semaphore_signal(barrier, inc=1, device_id=peer(lon, lat + 1), device_id_type=MESH)
        pl.semaphore_signal(barrier, inc=1, device_id=peer(east, lat + 1), device_id_type=MESH)

    pl.semaphore_wait(barrier, 12 + 2 * has_north.astype(jnp.int32) + 2 * has_south.astype(jnp.int32))

    def halo(which):
        out = []
        for n, (src, ext, own) in enumerate(((x_hbm, xe, xo), (g_hbm, ge, go))):
            if which == "e":
                out.append(remote(src.at[:, :, 0:8], ext.at[:, 0:24], halo_s.at[n], halo_r.at[n], peer(west, lat)))
            if which == "s":
                out.append(remote(src.at[:, 0:3], own.at[:, 24:27], halo_s.at[2 + n], halo_r.at[2 + n],
                                  peer(lon, lat - 1)))
                out.append(remote(src.at[:, 0:3, 0:8], ext.at[:, 24:27], halo_s.at[4 + n], halo_r.at[4 + n],
                                  peer(west, lat - 1)))
        return out

    for cp in halo("e"):
        cp.start()

    @pl.when(has_north)
    def _():
        for cp in halo("s"):
            cp.start()

    gq[...] = jnp.zeros_like(gq)
    gp[...] = jnp.zeros_like(gp)
    fe[...] = jnp.zeros_like(fe)

    def clear(t, _):
        gsum[t] = jnp.zeros((WTOK, PACK), F32)
        gbuf[t, 54:64] = jnp.zeros((10, 16, 128), BF)
        return 0

    lax.fori_loop(0, NT, clear, 0)

    def clear_out(z, _):
        fo[z] = jnp.zeros((27, 24, C), BF)
        return 0

    lax.fori_loop(0, 8, clear_out, 0)
    for cp in own_loads:
        cp.wait()

    mine = core * 32
    other = 32 - mine
    o8 = (xx + 2) % 4 * 8
    r8 = (xx + 1) % 4 * 8
    l8 = (xx + 3) % 4 * 8
    m8 = xx * 8

    def stage_copies(k, t):
        def rc(kind, src, dst, lon_):
            return remote(src, dst, ss.at[kind, t], rs.at[kind, t], peer(lon_, lat))
        if k == 1:
            return [rc(0, gbuf.at[t, pl.ds(other, 32)], rd.at[t], partner)]
        if k == 2:
            return [rc(1, hb.at[t, pl.ds(o8, 4)], xa.at[t, 0:4], right),
                    rc(2, hb.at[t, pl.ds(o8 + 4, 4)], xa.at[t, 4:8], left)]
        if k == 3:
            return [rc(3, xs.at[t, 0:8], xb.at[t, 0:8], right), rc(4, xs.at[t, 8:16], xb.at[t, 8:16], left)]
        if k == 4:
            return [rc(5, ys.at[t], yr.at[t], ymate)]
        if k == 5:
            here = fin.at[t, pl.ds(mine + m8, 8)]
            return [rc(6, here, here, right), rc(7, here, here, left)]
        if k == 6:
            a = fin.at[t, pl.ds(mine + l8, 4)]
            b = fin.at[t, pl.ds(mine + r8 + 4, 4)]
            return [rc(8, a, a, right), rc(9, b, b, left)]
        half = fin.at[t, pl.ds(mine, 32)]
        return [rc(10, half, half, partner)]

    def stage(k, t):
        if k > 1:
            for cp in stage_copies(k - 1, t):
                cp.wait_recv()
        if k == 2:
            hb[t] = add(gbuf[t, pl.ds(mine, 32)], rd[t])
        if k == 3:
            xs[t, 0:4] = add(hb[t, pl.ds(r8, 4)], xa[t, 0:4])
            xs[t, 4:8] = hb[t, pl.ds(r8 + 4, 4)]
            xs[t, 8:12] = hb[t, pl.ds(l8, 4)]
            xs[t, 12:16] = add(hb[t, pl.ds(l8 + 4, 4)], xa[t, 4:8])
        if k == 4:
            ys[t] = add(hb[t, pl.ds(m8, 8)], xb[t, 0:8], xb[t, 8:16])
        if k == 5:
            fin[t, pl.ds(mine + m8, 8)] = add(ys[t], yr[t])
        if k < 8:
            for cp in stage_copies(k, t):
                cp.start()
        else:
            pltpu.make_async_copy(fin.at[t], f_hbm.at[t], out_sem.at[t]).start()

    def run_stage(k, s):
        d = s - (k - 1)

        @pl.when(jnp.logical_and(d >= FIRST_PAIRS, d < 2 * FIRST_PAIRS))
        def _():
            stage(k, 2 * (d - FIRST_PAIRS))
            stage(k, 2 * (d - FIRST_PAIRS) + 1)

        @pl.when(jnp.logical_and(d >= 2 * FIRST_PAIRS, d < NT))
        def _():
            stage(k, d)

    wm = core * 36
    wo = 36 - wm

    def w_copies(k):
        def rc(src, dst, i, j, dev):
            return remote(src, dst, ws.at[i], wrs.at[j], dev)
        if k == 1:
            return [rc(wb.at[pl.ds(wo, 36)], wr, 0, 0, peer(partner, lat))]
        if k == 2:
            return [rc(wh.at[pl.ds((xx + d) % 4 * 9, 9)], wx.at[d - 1], d, d, xpeer(d)) for d in (1, 2, 3)]
        if k == 3:
            return [rc(wy.at[yy], wy.at[yy], 3 + d, 3 + d, ypeer(d)) for d in (1, 2, 3)]
        if k == 4:
            return [rc(wz.at[zz], wz.at[zz], 6 + d, 6 + d, zpeer(d)) for d in (1, 2, 3)]
        if k == 5:
            here = wf.at[pl.ds(wm + xx * 9, 9)]
            return [rc(here, here, 9 + d, 9 + d, xpeer(d)) for d in (1, 2, 3)]
        half = wf.at[pl.ds(wm, 36)]
        return [rc(half, half, 13, 13, peer(partner, lat))]

    def w_stage(k):
        if k > 1:
            for cp in w_copies(k - 1):
                cp.wait_recv()
        if k == 1:
            for i in range(3):
                wb[24 * i:24 * i + 12] = gq[i, :, 0:128].astype(BF).reshape(12, 16, 128)
                wb[24 * i + 12:24 * i + 24, :, 0:64] = gq[i, :, 128:192].astype(BF).reshape(12, 16, 64)
                wb[24 * i + 12:24 * i + 24, :, 64:128] = gp[:, 64 * i:64 * i + 64].astype(BF).reshape(12, 16, 64)
        if k == 2:
            wh[...] = add(wb[pl.ds(wm, 36)], wr[...])
        if k == 3:
            wy[yy] = add(wh[pl.ds(xx * 9, 9)], wx[0], wx[1], wx[2])
        if k == 4:
            wz[zz] = add(wy[0], wy[1], wy[2], wy[3])
        if k == 5:
            wf[pl.ds(wm + xx * 9, 9)] = add(wz[0], wz[1], wz[2], wz[3])
        if k < 7:
            for cp in w_copies(k):
                cp.start()
        else:
            w_ref[...] = wf[...]

    def strips(part):
        if part == 0:
            return [remote(fe.at[:, 3:21], fw.at[:, 3:21], halo_s.at[6], halo_r.at[6], peer(east, lat))]
        if part == 1:
            return [remote(fe.at[:, 21:24], fw.at[:, 21:24], halo_s.at[7], halo_r.at[7], peer(east, lat))]
        return [remote(fe.at[:, 24:27], fw.at[:, 0:3], halo_s.at[8], halo_r.at[8], peer(east, lat + 1)),
                remote(fo.at[:, 24:27], fs, halo_s.at[9], halo_r.at[9], peer(lon, lat + 1))]

    def place(s):
        early = s < FIRST_PAIRS
        late = s >= 2 * FIRST_PAIRS
        base = jnp.where(early, 2 * s, jnp.where(late, s, 2 * (s - FIRST_PAIRS)))
        t_of = (base, jnp.where(late, s, base + 1))
        c_of = (jnp.where(early, 0, jnp.where(late, 0, 1)), jnp.where(early, 0, 1))
        return t_of, c_of

    def gather(s, with_east):
        t_of, c_of = place(s)
        for w in range(2):
            r0 = t_of[w] // 4 * 6 + 3
            for arr, ext, dst in ((xo, xe, x2), (go, ge, g2)):
                halves = []
                for dz in range(2):
                    z = (t_of[w] % 4 * 2 + dz + 1) % 8
                    own = arr[z, pl.ds(r0, 6)].astype(F32).reshape(144, C).astype(BF)
                    part = dot(so_ref[c_of[w]], own)
                    if with_east:
                        ex = ext[z, pl.ds(r0, 6)].astype(F32).reshape(48, C).astype(BF)
                        part = part + dot(se_ref[c_of[w]], ex)
                    halves.append(part)
                dst[w * WTOK:(w + 1) * WTOK] = jnp.concatenate(halves, axis=0).astype(BF)

    def scatter(s, gin):
        t_of, c_of = place(s)
        for w in range(2):
            r0 = t_of[w] // 4 * 6 + 3
            for dz in range(2):
                z = (t_of[w] % 4 * 2 + dz + 1) % 8
                lo = w * WTOK + dz * 72
                part = gin[lo:lo + 72].astype(BF)
                own = dot(to_ref[c_of[w]], part).reshape(6, 24, C)
                fo[z, pl.ds(r0, 6)] = (fo[z, pl.ds(r0, 6)].astype(F32) + own).astype(BF)
                ex = dot(te_ref[c_of[w]], part).reshape(6, 8, C)
                fe[z, pl.ds(r0, 6)] = (fe[z, pl.ds(r0, 6)].astype(F32) + ex).astype(BF)

    def step(s, _):
        @pl.when(s == FIRST_PAIRS)
        def _():
            for cp in halo("e"):
                cp.wait_recv()

        @pl.when(jnp.logical_and(s == 2 * FIRST_PAIRS, has_south))
        def _():
            for cp in halo("s"):
                cp.wait_recv()

        for k in (8, 7, 6, 5, 4, 3, 2):
            run_stage(k, s)
        for k in (7, 6, 5, 4, 3, 2):
            @pl.when(s == NT - 2 + k)
            def _(k=k):
                w_stage(k)

        @pl.when(s == 2 * FIRST_PAIRS)
        def _():
            for cp in strips(0):
                cp.start()

        @pl.when(s == NT)
        def _():
            for cp in strips(1):
                cp.start()

            @pl.when(has_south)
            def _():
                for cp in strips(2):
                    cp.start()

        @pl.when(s < FIRST_PAIRS)
        def _():
            gather(s, False)

        @pl.when(jnp.logical_and(s >= FIRST_PAIRS, s < NT))
        def _():
            gather(s, True)

        @pl.when(s < NT)
        def _():
            t_of, _c = place(s)
            gin = window_pair(s, x2, g2, t_of, wq_ref, wqt_ref, wpt_ref, bm_ref, bt_ref, penz_ref, penl_ref,
                              lat_last, gq, gp, gsum, gbuf)
            scatter(s, gin)

        run_stage(1, s)

        @pl.when(s == NT - 1)
        def _():
            w_stage(1)
        return 0

    lax.fori_loop(0, STEPS, step, 0)

    for cp in strips(0) + strips(1):
        cp.wait_recv()
        cp.wait_send()

    @pl.when(has_north)
    def _():
        for cp in strips(2):
            cp.wait_recv()

    @pl.when(has_south)
    def _():
        for cp in strips(2):
            cp.wait_send()

    def finish(z, _):
        out_ref[z] = fo[z, 0:24]
        out_ref[z, 0:3] = fs[z]
        out_ref[z, :, 0:8] = add(out_ref[z, :, 0:8], fw[z, 0:24])
        return 0

    lax.fori_loop(0, 8, finish, 0)

    for cp in halo("e"):
        cp.wait_send()

    @pl.when(has_north)
    def _():
        for cp in halo("s"):
            cp.wait_send()

    for k in range(1, 7):
        for cp in w_copies(k):
            cp.wait_send()

    def drain(t, _):
        for k in range(1, 8):
            for cp in stage_copies(k, t):
                cp.wait_send()
        pltpu.make_async_copy(fin.at[t], f_hbm.at[t], out_sem.at[t]).wait()
        return 0

    lax.fori_loop(0, NT, drain, 0)


def selectors():
    tok = jnp.arange(72, dtype=jnp.int32)
    i, j = tok // 12, tok % 12
    own = jnp.arange(144, dtype=jnp.int32)
    ext = jnp.arange(48, dtype=jnp.int32)
    so, se = [], []
    for c in range(2):
        col = 6 + 12 * c + j
        so.append((own[None, :] == (i * 24 + col)[:, None]) & (col < 24)[:, None])
        se.append((ext[None, :] == (i * 8 + col - 24)[:, None]) & (col >= 24)[:, None])
    so = jnp.stack(so).astype(BF)
    se = jnp.stack(se).astype(BF)
    return so, se, so.transpose(0, 2, 1), se.transpose(0, 2, 1)


def penalties():
    k = jnp.arange(WTOK, dtype=jnp.int32)
    lane = jnp.arange(PACK, dtype=jnp.int32)
    q = jnp.where(lane < 768, lane % 128, 128 + lane % 16)
    z = (k[:, None] // 72) != (q[None, :] // 72)
    l = ((k[:, None] // 12) % 6 >= 3) != ((q[None, :] // 12) % 6 >= 3)
    return jnp.where(z, -1e30, 0.0).astype(BF), jnp.where(l, -1e30, 0.0).astype(BF)


def fused(normed, cotangent, weight_qkv, weight_proj, bias_main, bias_tail):
    wq = weight_qkv.reshape(C, 3, C)
    wq_pad = jnp.pad(wq, ((0, 0), (0, 0), (0, 64))).reshape(C, 768)
    wqt = wq.transpose(1, 2, 0)
    wpt = weight_proj.T
    penz, penl = penalties()
    so, se, to, te = selectors()
    vm = pl.BlockSpec(memory_space=pltpu.VMEM)
    hbm = pl.BlockSpec(memory_space=pl.ANY)
    V = pltpu.VMEM
    return pl.pallas_call(
        fused_kernel,
        in_specs=[hbm, hbm] + [vm] * 11,
        out_specs=[vm, vm, hbm],
        out_shape=[
            jax.ShapeDtypeStruct(normed.shape, BF),
            jax.ShapeDtypeStruct((72, 16, 128), BF),
            jax.ShapeDtypeStruct((NT, 64, 16, 128), BF),
        ],
        scratch_shapes=[
            V((8, 27, 24, C), BF), V((8, 27, 24, C), BF), V((8, 27, 8, C), BF), V((8, 27, 8, C), BF),
            V((2 * WTOK, C), BF), V((2 * WTOK, C), BF),
            V((8, 27, 24, C), BF), V((8, 27, 8, C), BF), V((8, 27, 8, C), BF), V((8, 3, 24, C), BF),
            V((3, C, C), F32), V((C, C), F32), V((NT, WTOK, PACK), F32),
            V((NT, 64, 16, 128), BF), V((NT, 32, 16, 128), BF), V((NT, 32, 16, 128), BF),
            V((NT, 8, 16, 128), BF), V((NT, 16, 16, 128), BF), V((NT, 16, 16, 128), BF),
            V((NT, 8, 16, 128), BF), V((NT, 8, 16, 128), BF), V((NT, 64, 16, 128), BF),
            V((72, 16, 128), BF), V((36, 16, 128), BF), V((36, 16, 128), BF), V((3, 9, 16, 128), BF),
            V((4, 9, 16, 128), BF), V((4, 9, 16, 128), BF), V((72, 16, 128), BF),
            pltpu.SemaphoreType.DMA((2,)), pltpu.SemaphoreType.DMA((10,)), pltpu.SemaphoreType.DMA((10,)),
            pltpu.SemaphoreType.DMA((11, NT)), pltpu.SemaphoreType.DMA((11, NT)),
            pltpu.SemaphoreType.DMA((14,)), pltpu.SemaphoreType.DMA((14,)), pltpu.SemaphoreType.DMA((NT,)),
        ],
        compiler_params=pltpu.CompilerParams(collective_id=0, has_side_effects=True, vmem_limit_bytes=66_000_000),
        name="fused",
    )(normed, cotangent, wq_pad, wqt, wpt, bias_main, bias_tail, penz, penl, so, se, to, te)


def local(normed, cotangent, weight_qkv, weight_proj, bias_table):
    bias_main, bias_tail = pack(bias_table.transpose(1, 0, 2))
    input_grad, w, f = fused(normed, cotangent, weight_qkv, weight_proj, bias_main, bias_tail)
    bias_grad = unpack(f).transpose(1, 0, 2)
    w = w.reshape(3, 2, 12, 16, 128).transpose(2, 3, 0, 1, 4).reshape(C, 3, 256).astype(F32)
    return input_grad, w[:, :, :C].reshape(C, 3 * C), w[:, :, C:].reshape(C, C), bias_grad


def solution(mesh):
    in_specs = (P(None, "lat", "lon", None), P(None, "lat", "lon", None), P(), P(), P("lat", None, None))
    out_specs = (P(None, "lat", "lon", None), P(), P(), P("lat", None, None))
    return jax.shard_map(local, mesh=mesh, in_specs=in_specs, out_specs=out_specs, check_vma=False)
```

```python
import functools
import jax
import jax.numpy as jnp
from jax import lax
from jax.experimental import pallas as pl
from jax.experimental.pallas import tpu as pltpu
from jax.sharding import PartitionSpec as P

HEADS = 6
WTOK = 144
HD = 32
C = 192
MAIN = 128
TAIL = WTOK - MAIN
PACK = 896
NT = 16
SCALE = HD ** -0.5
LOG2E = 1.4426950408889634
BF = jnp.bfloat16
F32 = jnp.float32
MESH = pl.DeviceIdType.MESH
FIRST = 5
EDGE = 9
PAIRED = 14
STEPS = 23
ST = 17
MASKED = -1e30


def dot(a, b):
    return jnp.dot(a, b, preferred_element_type=F32)


def lane_head(shape):
    return lax.broadcasted_iota(jnp.int32, shape, 1) // HD


def pack_kernel(b_ref, main_ref, tail_ref, sc):
    lane = lax.broadcasted_iota(jnp.int32, (NT, 128), 1)

    def group(g, _):
        base = pl.multiple_of(g * 1152, 128)
        tiles = [b_ref[0, :, pl.ds(base + 128 * j, 128)].astype(F32) for j in range(9)]
        for j in range(8):
            if j == 0:
                main, sec = tiles[0], tiles[1]
            else:
                r = pltpu.roll(tiles[j], 128 - 16 * j, 1)
                sec = pltpu.roll(tiles[j + 1], 128 - 16 * j, 1)
                main = jnp.where(lane < 128 - 16 * j, r, sec)
            row = g * (8 * ST) + ST * j
            sc[0, pl.ds(row, NT), :] = main
            sc[1, pl.ds(row, NT), :] = sec
        return 0

    lax.fori_loop(0, 18, group, 0, unroll=9)
    last = (lax.axis_index("lat") == 7).astype(F32)

    def half(n):
        return jnp.logical_or(jnp.logical_and(n >= 36, n < 72), n >= 108)

    def masks(shape, k_axis, q_first):
        k = lax.broadcasted_iota(jnp.int32, shape, k_axis)
        q = lax.broadcasted_iota(jnp.int32, shape, 1 - k_axis)
        q = q if q_first == 0 else q * 0 + q_first
        z_no = jnp.logical_xor(k >= 72, q >= 72)
        l_no = jnp.logical_xor(half(k), half(q))
        return jnp.where(z_no, MASKED, 0.0), jnp.where(l_no, MASKED, 0.0) * last

    z_main, l_main = masks((WTOK, MAIN), 0, 0)
    z_tail, l_tail = masks((16, WTOK), 1, 128)

    def masked(x, t, z, l):
        if t % 4 != 3 and t // 4 != 3:
            return x
        y = x.astype(F32)
        if t % 4 == 3:
            y = y + z
        if t // 4 == 3:
            y = y + l
        return y.astype(BF)

    for t in range(NT):
        a = sc[0, pl.ds(t, WTOK, stride=ST), :].astype(BF)
        b = sc[1, pl.ds(t, WTOK, stride=ST), :].astype(BF)
        main_ref[t, 0:128, :] = masked(a[:MAIN].T, t, z_main[:128], l_main[:128])
        main_ref[t, 128:144, :] = masked(b[:MAIN].T[:16], t, z_main[128:], l_main[128:])
        tail_ref[t, :, 0:128] = masked(a[MAIN:], t, z_tail[:, :128], l_tail[:, :128])
        tail_ref[t, :, 128:144] = masked(b[MAIN:, 0:16], t, z_tail[:, 128:], l_tail[:, 128:])


def pack(bias_view):
    return pl.pallas_call(
        pack_kernel, grid=(6,),
        in_specs=[pl.BlockSpec((1, NT, WTOK * WTOK), lambda h: (h, 0, 0))],
        out_specs=[pl.BlockSpec((NT, WTOK, MAIN), lambda h: (0, 0, h)),
                   pl.BlockSpec((NT, 16, WTOK), lambda h: (0, h, 0))],
        out_shape=[jax.ShapeDtypeStruct((NT, WTOK, 6 * MAIN), BF), jax.ShapeDtypeStruct((NT, 96, WTOK), BF)],
        scratch_shapes=[pltpu.VMEM((2, WTOK * ST, 128), F32)], name="pack",
        cost_estimate=pl.CostEstimate(flops=10**9, bytes_accessed=8 * 2**20, transcendentals=0),
    )(bias_view)


def unpack_kernel(m_ref, t_ref, w_ref, out_ref, gq_ref, gp_ref, sc, tn):
    h = pl.program_id(0)

    @pl.when(h == 0)
    def _():
        for t in range(NT):
            tn[t] = t_ref[t].reshape(WTOK, 128).T
        for i in range(3):
            gq_ref[:, C * i:C * i + 128] = w_ref[24 * i:24 * i + 12].reshape(C, 128).astype(F32)
            rest = w_ref[24 * i + 12:24 * i + 24].reshape(C, 128).astype(F32)
            gq_ref[:, C * i + 128:C * i + C] = rest[:, :64]
            gp_ref[:, 64 * i:64 * i + 64] = rest[:, 64:]

    for t in range(NT):
        m = m_ref[t].reshape(WTOK, 128)
        sc[0, pl.ds(t, MAIN, stride=ST), :] = m[:MAIN].T.astype(F32)
        sc[1, pl.ds(t, MAIN, stride=ST), 0:16] = m[MAIN:].T.astype(F32)
        tl = tn[t, pl.ds(pl.multiple_of(h * 16, 16), 16), :].astype(F32)
        sc[0, pl.ds(MAIN * ST + t, 16, stride=ST), :] = tl[:, :128]
        sc[1, pl.ds(MAIN * ST + t, 16, stride=ST), 0:16] = tl[:, 128:]
    lane = lax.broadcasted_iota(jnp.int32, (NT, 128), 1)

    def group(g, _):
        base = pl.multiple_of(g * 1152, 128)
        r, s = [], []
        for j in range(8):
            row = g * (8 * ST) + ST * j
            m = sc[0, pl.ds(row, NT), :]
            t = sc[1, pl.ds(row, NT), :]
            r.append(pltpu.roll(m, 16 * j, 1) if j else m)
            s.append(pltpu.roll(t, 16 * j, 1) if j else t)
        for j in range(9):
            if j == 0:
                v = r[0]
            else:
                low = jnp.where(lane < 16 * (j - 1), r[j - 1], s[j - 1]) if j > 1 else s[0]
                v = jnp.where(lane < 16 * j, low, r[j]) if j < 8 else low
            out_ref[0, :, pl.ds(base + 128 * j, 128)] = v
        return 0

    lax.fori_loop(0, 18, group, 0, unroll=9)


def unpack(f, w):
    return pl.pallas_call(
        unpack_kernel, grid=(6,),
        in_specs=[pl.BlockSpec((NT, 9, 16, 128), lambda h: (0, h, 0, 0)),
                  pl.BlockSpec((NT, 9, 16, 128), lambda h: (0, 6, 0, 0)),
                  pl.BlockSpec((72, 16, 128), lambda h: (0, 0, 0))],
        out_specs=[pl.BlockSpec((1, NT, WTOK * WTOK), lambda h: (h, 0, 0)),
                   pl.BlockSpec((C, 3 * C), lambda h: (0, 0)), pl.BlockSpec((C, C), lambda h: (0, 0))],
        out_shape=[jax.ShapeDtypeStruct((6, NT, WTOK * WTOK), F32), jax.ShapeDtypeStruct((C, 3 * C), F32),
                   jax.ShapeDtypeStruct((C, C), F32)],
        scratch_shapes=[pltpu.VMEM((2, WTOK * ST, 128), F32), pltpu.VMEM((NT, 128, WTOK), BF)], name="unpack",
        cost_estimate=pl.CostEstimate(flops=10**9, bytes_accessed=12 * 2**20, transcendentals=0),
    )(f, f, w)


def add(*parts):
    total = parts[0].astype(F32)
    for part in parts[1:]:
        total = total + part.astype(F32)
    return total.astype(BF)


def window_pair(s, x2, g2, t_of, wq_ref, wqt_ref, wpt_ref, bm_ref, bt_ref,
                gq, gp, gsum, gbuf):
    x = x2[...]
    cot = g2[...]
    proj = dot(x, wq_ref[...]).astype(BF)
    dmix = dot(cot, wpt_ref[...]).astype(BF)
    xt = x.T
    dq_l, dk_l, dv_l, mixm, mixt, cott = [], [], [], [], [], []
    for c in range(2):
        t = t_of[c]
        rows = slice(c * WTOK, (c + 1) * WTOK)
        q = proj[rows, 0:192]
        k = proj[rows, 256:448]
        v = proj[rows, 512:704]
        dm = dmix[rows]
        ct = cot[rows]
        qt, kt, vt, dmt = q.T, k.T, v.T, dm.T
        hm = lane_head((MAIN, C))
        ht = lane_head((TAIL, C))
        zq = jnp.zeros((HD, MAIN), BF)

        def blk(at, p):
            top = jnp.concatenate([at[64 * p:64 * p + 32, :MAIN], zq], axis=1)
            bot = jnp.concatenate([zq, at[64 * p + 32:64 * p + 64, :MAIN]], axis=1)
            two = jnp.concatenate([top, bot], axis=0)
            if p == 2:
                return two
            z64 = jnp.zeros((64, 256), BF)
            return jnp.concatenate([two, z64] if p == 0 else [z64, two], axis=0)

        def nat(a, p):
            lanes = slice(0, 128) if p < 2 else slice(128, 192)
            am = a[:MAIN, lanes]
            hh = hm[:, lanes]
            z = jnp.zeros_like(am)
            return jnp.concatenate([jnp.where(hh == 2 * p, am, z), jnp.where(hh == 2 * p + 1, am, z)], axis=0)

        def nat_tail(a):
            am = a[MAIN:]
            z = jnp.zeros_like(am)
            return jnp.concatenate([jnp.where(ht == h, am, z) for h in range(HEADS)], axis=0)

        q_tail, dm_tail = nat_tail(q), nat_tail(dm)
        dn = (((1,), (1,)), ((), ()))
        dk_a = dk_b = dv_a = dv_b = None
        mix_parts, dq_parts = [], []
        for p in range(4):
            if p < 3:
                ln = slice(256 * p, 256 * p + 256)
                sub = slice(0, 128) if p < 2 else slice(128, 192)
                s_ = dot(k[:, sub], blk(qt, p))
                dp = dot(v[:, sub], blk(dmt, p))
                bias = bm_ref[t, :, ln].astype(F32)
            else:
                ln = slice(768, 864)
                s_ = lax.dot_general(k, q_tail, dn, preferred_element_type=F32)
                dp = lax.dot_general(v, dm_tail, dn, preferred_element_type=F32)
                bias = bt_ref[t].T.astype(F32)
            s_ = s_ * (SCALE * LOG2E) + bias * LOG2E
            m = jnp.max(s_, axis=0, keepdims=True)
            e = jnp.exp2(s_ - m)
            r = 1.0 / jnp.sum(e, axis=0, keepdims=True)
            pr = e * r
            pb = pr.astype(BF)
            d = jnp.sum(pr * dp, axis=0, keepdims=True)
            gs = pr * (dp - d)
            gb = gs.astype(BF)
            tot = gsum[t, :, ln] + gs
            gsum[t, :, ln] = tot
            tot = tot.astype(BF)
            if p < 3:
                gbuf[t, 18 * p:18 * p + 9] = tot[:, :128].reshape(9, 16, 128)
                gbuf[t, 18 * p + 9:18 * p + 18] = tot[:, 128:].reshape(9, 16, 128)
            else:
                gbuf[t, 54:63, :, 0:96] = tot.reshape(9, 16, 96)
            if p < 3:
                mo = dot(vt[64 * p:64 * p + 64], pb).astype(BF)
                do = dot(kt[64 * p:64 * p + 64], gb)
                mix_parts += [mo[:32, :MAIN], mo[32:, MAIN:]]
                dq_parts += [do[:32, :MAIN], do[32:, MAIN:]]
                dkp = dot(gb, nat(q, p))
                dvp = dot(pb, nat(dm, p))
                if p < 2:
                    dk_a = dkp if dk_a is None else dk_a + dkp
                    dv_a = dvp if dv_a is None else dv_a + dvp
                else:
                    dk_b, dv_b = dkp, dvp
            else:
                mo = dot(vt, pb).astype(BF)
                do = (dot(kt, gb) * SCALE).astype(BF)
                rh = lax.broadcasted_iota(jnp.int32, (C, 96), 0) // HD
                lh = lax.broadcasted_iota(jnp.int32, (C, 96), 1) // TAIL
                mixt.append(jnp.where(rh == lh, mo, jnp.zeros_like(mo)))
                dot_t = do.T
                dq_tail = jnp.zeros((TAIL, C), BF)
                for h in range(HEADS):
                    dq_tail = jnp.where(ht == h, dot_t[TAIL * h:TAIL * h + TAIL], dq_tail)
                dk_a = dk_a + dot(gb, q_tail[:, :128])
                dk_b = dk_b + dot(gb, q_tail[:, 128:])
                dv_a = dv_a + dot(pb, dm_tail[:, :128])
                dv_b = dv_b + dot(pb, dm_tail[:, 128:])
        mixm.append(jnp.concatenate(mix_parts, axis=0))
        dqt = (jnp.concatenate(dq_parts, axis=0) * SCALE).astype(BF)
        dq_l.append(jnp.concatenate([dqt.T, dq_tail], axis=0))
        dk_l.append((jnp.concatenate([dk_a, dk_b], axis=1) * SCALE).astype(BF))
        dv_l.append(jnp.concatenate([dv_a, dv_b], axis=1).astype(BF))
        cott.append(jnp.concatenate([ct[MAIN:]] * HEADS, axis=0))
    mm = jnp.concatenate(mixm, axis=1)
    cm = jnp.concatenate([cot[0:MAIN], cot[WTOK:WTOK + MAIN]], axis=0)
    gp[...] += dot(mm, cm) + dot(mixt[0], cott[0]) + dot(mixt[1], cott[1])
    dq = jnp.concatenate(dq_l, axis=0)
    dk = jnp.concatenate(dk_l, axis=0)
    dv = jnp.concatenate(dv_l, axis=0)
    gq[0] += dot(xt, dq)
    gq[1] += dot(xt, dk)
    gq[2] += dot(xt, dv)
    return dot(dq, wqt_ref[0]) + dot(dk, wqt_ref[1]) + dot(dv, wqt_ref[2])


def fused_kernel(x_hbm, g_hbm, wqkv_ref, wproj_ref, bm_ref, bt_ref, out_ref, w_ref, f_hbm,
                 xo, go, xe, ge, x2, g2, fo, fe, fw, fs, gq, gp, gsum, gbuf, rd, hb, xa, xs, xb, ys, yr, fin,
                 wb, wr, wh, wx, wy, wz, wf, wq_ref, wqt_ref, wpt_ref, so_ref, se_ref, to_ref, te_ref,
                 load_sem, halo_s, halo_r, ss, rs, ws, wrs, out_sem):
    lon = lax.axis_index("lon")
    lat = lax.axis_index("lat")
    n_lon = 16
    core = lon % 2
    yh = (lon // 2) % 2
    xx = lon // 4
    zz = lat % 4
    yl = lat // 4
    yy = yh * 2 + yl
    partner = lon + 1 - 2 * core
    right = (lon + 4) % n_lon
    left = (lon + 12) % n_lon
    ymate = lon + 2 - 4 * yh
    east = (lon + 1) % n_lon
    west = (lon + 15) % n_lon
    has_south = lat < 7
    has_north = lat > 0

    def peer(lon_, lat_):
        return {"lon": lon_, "lat": lat_}

    def xpeer(d):
        return peer((xx + d) % 4 * 4 + yh * 2 + core, lat)

    def ypeer(d):
        o = (yy + d) % 4
        return peer(xx * 4 + o // 2 * 2 + core, o % 2 * 4 + zz)

    def zpeer(d):
        return peer(lon, yl * 4 + (zz + d) % 4)

    def remote(src, dst, ssem, rsem, dev):
        return pltpu.make_async_remote_copy(src_ref=src, dst_ref=dst, send_sem=ssem, recv_sem=rsem,
                                            device_id=dev, device_id_type=MESH)

    own_loads = [pltpu.make_async_copy(x_hbm, xo.at[:, 0:24], load_sem.at[0]),
                 pltpu.make_async_copy(g_hbm, go.at[:, 0:24], load_sem.at[1])]
    for cp in own_loads:
        cp.start()
    for buf in (xe, ge):
        buf[...] = jnp.zeros_like(buf)
    for buf in (xo, go):
        buf[:, 24:27] = jnp.zeros((8, 3, 24, C), BF)
    for buf in (fw, fs):
        buf[...] = jnp.zeros_like(buf)

    for i in range(3):
        part = wqkv_ref[:, C * i:C * i + C]
        wq_ref[:, 256 * i:256 * i + C] = part
        wq_ref[:, 256 * i + C:256 * i + 256] = jnp.zeros((C, 64), BF)
        wqt_ref[i] = part.T
    wpt_ref[...] = wproj_ref[...].T
    for c in range(2):
        for ref, width, over, axis in ((so_ref, 24, False, 0), (se_ref, 8, True, 0), (to_ref, 24, False, 1),
                                       (te_ref, 8, True, 1)):
            shape = ref.shape[1:]
            tok = lax.broadcasted_iota(jnp.int32, shape, axis)
            at = lax.broadcasted_iota(jnp.int32, shape, 1 - axis)
            row = jnp.zeros(shape, jnp.int32)
            for m in range(1, 6):
                row = row + (tok >= 12 * m).astype(jnp.int32)
            col = tok - 12 * row + 6 + 12 * c
            hit = at == row * width + col - (24 if over else 0)
            hit = jnp.logical_and(hit, col >= 24 if over else col < 24)
            ref[c] = jnp.where(hit, 1.0, 0.0).astype(BF)

    barrier = pltpu.get_barrier_semaphore()
    greet = [peer(partner, lat), xpeer(1), xpeer(2), xpeer(3)] + [ypeer(d) for d in (1, 2, 3)] + [zpeer(d) for d in (1, 2, 3)]
    for dev in greet:
        pl.semaphore_signal(barrier, inc=1, device_id=dev, device_id_type=MESH)
    for dev in (peer(east, lat), peer(west, lat)):
        pl.semaphore_signal(barrier, inc=1, device_id=dev, device_id_type=MESH)

    @pl.when(has_north)
    def _():
        pl.semaphore_signal(barrier, inc=1, device_id=peer(lon, lat - 1), device_id_type=MESH)
        pl.semaphore_signal(barrier, inc=1, device_id=peer(west, lat - 1), device_id_type=MESH)

    @pl.when(has_south)
    def _():
        pl.semaphore_signal(barrier, inc=1, device_id=peer(lon, lat + 1), device_id_type=MESH)
        pl.semaphore_signal(barrier, inc=1, device_id=peer(east, lat + 1), device_id_type=MESH)

    pl.semaphore_wait(barrier, 12 + 2 * has_north.astype(jnp.int32) + 2 * has_south.astype(jnp.int32))

    def halo(which):
        out = []
        for n, (src, ext, own) in enumerate(((x_hbm, xe, xo), (g_hbm, ge, go))):
            if which == "e":
                out.append(remote(src.at[:, :, 0:8], ext.at[:, 0:24], halo_s.at[n], halo_r.at[n], peer(west, lat)))
            if which == "s":
                out.append(remote(src.at[:, 0:3], own.at[:, 24:27], halo_s.at[2 + n], halo_r.at[2 + n],
                                  peer(lon, lat - 1)))
                out.append(remote(src.at[:, 0:3, 0:8], ext.at[:, 24:27], halo_s.at[4 + n], halo_r.at[4 + n],
                                  peer(west, lat - 1)))
        return out

    for cp in halo("e"):
        cp.start()

    @pl.when(has_north)
    def _():
        for cp in halo("s"):
            cp.start()

    gq[...] = jnp.zeros_like(gq)
    gp[...] = jnp.zeros_like(gp)
    fe[...] = jnp.zeros_like(fe)

    def clear(t, _):
        gsum[t] = jnp.zeros((WTOK, PACK), F32)
        gbuf[t, 54:64] = jnp.zeros((10, 16, 128), BF)
        return 0

    lax.fori_loop(0, NT, clear, 0)

    def clear_out(z, _):
        fo[z] = jnp.zeros((27, 24, C), BF)
        return 0

    lax.fori_loop(0, 8, clear_out, 0)
    for cp in own_loads:
        cp.wait()

    mine = core * 32
    other = 32 - mine
    o8 = (xx + 2) % 4 * 8
    r8 = (xx + 1) % 4 * 8
    l8 = (xx + 3) % 4 * 8
    m8 = xx * 8

    def stage_copies(k, t):
        def rc(kind, src, dst, lon_):
            return remote(src, dst, ss.at[kind, t], rs.at[kind, t], peer(lon_, lat))
        if k == 1:
            return [rc(0, gbuf.at[t, pl.ds(other, 32)], rd.at[t], partner)]
        if k == 2:
            return [rc(1, hb.at[t, pl.ds(o8, 4)], xa.at[t, 0:4], right),
                    rc(2, hb.at[t, pl.ds(o8 + 4, 4)], xa.at[t, 4:8], left)]
        if k == 3:
            return [rc(3, xs.at[t, 0:8], xb.at[t, 0:8], right), rc(4, xs.at[t, 8:16], xb.at[t, 8:16], left)]
        if k == 4:
            return [rc(5, ys.at[t], yr.at[t], ymate)]
        if k == 5:
            here = fin.at[t, pl.ds(mine + m8, 8)]
            return [rc(6, here, here, right), rc(7, here, here, left)]
        if k == 6:
            a = fin.at[t, pl.ds(mine + l8, 4)]
            b = fin.at[t, pl.ds(mine + r8 + 4, 4)]
            return [rc(8, a, a, right), rc(9, b, b, left)]
        half = fin.at[t, pl.ds(mine, 32)]
        return [rc(10, half, half, partner)]

    def stage(k, t):
        if k > 1:
            for cp in stage_copies(k - 1, t):
                cp.wait_recv()
        if k == 2:
            hb[t] = add(gbuf[t, pl.ds(mine, 32)], rd[t])
        if k == 3:
            xs[t, 0:4] = add(hb[t, pl.ds(r8, 4)], xa[t, 0:4])
            xs[t, 4:8] = hb[t, pl.ds(r8 + 4, 4)]
            xs[t, 8:12] = hb[t, pl.ds(l8, 4)]
            xs[t, 12:16] = add(hb[t, pl.ds(l8 + 4, 4)], xa[t, 4:8])
        if k == 4:
            ys[t] = add(hb[t, pl.ds(m8, 8)], xb[t, 0:8], xb[t, 8:16])
        if k == 5:
            fin[t, pl.ds(mine + m8, 8)] = add(ys[t], yr[t])
        if k < 8:
            for cp in stage_copies(k, t):
                cp.start()
        else:
            pltpu.make_async_copy(fin.at[t], f_hbm.at[t], out_sem.at[t]).start()

    def run_stage(k, s):
        d = s - (k - 1)

        @pl.when(jnp.logical_and(d >= EDGE, d < PAIRED))
        def _():
            stage(k, 2 * (d - EDGE))
            stage(k, 2 * (d - EDGE) + 1)

        @pl.when(jnp.logical_or(jnp.logical_and(d >= FIRST, d < EDGE), jnp.logical_and(d >= PAIRED, d < NT)))
        def _():
            stage(k, jnp.where(d < EDGE, d + 12 - FIRST, d - 4))

    wm = core * 36
    wo = 36 - wm

    def w_copies(k):
        def rc(src, dst, i, j, dev):
            return remote(src, dst, ws.at[i], wrs.at[j], dev)
        if k == 1:
            return [rc(wb.at[pl.ds(wo, 36)], wr, 0, 0, peer(partner, lat))]
        if k == 2:
            return [rc(wh.at[pl.ds((xx + d) % 4 * 9, 9)], wx.at[d - 1], d, d, xpeer(d)) for d in (1, 2, 3)]
        if k == 3:
            return [rc(wy.at[yy], wy.at[yy], 3 + d, 3 + d, ypeer(d)) for d in (1, 2, 3)]
        if k == 4:
            return [rc(wz.at[zz], wz.at[zz], 6 + d, 6 + d, zpeer(d)) for d in (1, 2, 3)]
        if k == 5:
            here = wf.at[pl.ds(wm + xx * 9, 9)]
            return [rc(here, here, 9 + d, 9 + d, xpeer(d)) for d in (1, 2, 3)]
        half = wf.at[pl.ds(wm, 36)]
        return [rc(half, half, 13, 13, peer(partner, lat))]

    def w_stage(k):
        if k > 1:
            for cp in w_copies(k - 1):
                cp.wait_recv()
        if k == 1:
            for i in range(3):
                wb[24 * i:24 * i + 12] = gq[i, :, 0:128].astype(BF).reshape(12, 16, 128)
                wb[24 * i + 12:24 * i + 24, :, 0:64] = gq[i, :, 128:192].astype(BF).reshape(12, 16, 64)
                wb[24 * i + 12:24 * i + 24, :, 64:128] = gp[:, 64 * i:64 * i + 64].astype(BF).reshape(12, 16, 64)
        if k == 2:
            wh[...] = add(wb[pl.ds(wm, 36)], wr[...])
        if k == 3:
            wy[yy] = add(wh[pl.ds(xx * 9, 9)], wx[0], wx[1], wx[2])
        if k == 4:
            wz[zz] = add(wy[0], wy[1], wy[2], wy[3])
        if k == 5:
            wf[pl.ds(wm + xx * 9, 9)] = add(wz[0], wz[1], wz[2], wz[3])
        if k < 7:
            for cp in w_copies(k):
                cp.start()
        else:
            w_ref[...] = wf[...]

    def strips(part):
        if part < 4:
            r = (21, 3, 9, 15)[part]
            n = 3 if part == 0 else 6
            return [remote(fe.at[:, r:r + n], fw.at[:, r:r + n], halo_s.at[6 + part], halo_r.at[6 + part], peer(east, lat))]
        return [remote(fe.at[:, 24:27], fw.at[:, 0:3], halo_s.at[10], halo_r.at[10], peer(east, lat + 1)),
                remote(fo.at[:, 24:27], fs, halo_s.at[11], halo_r.at[11], peer(lon, lat + 1))]

    def place(s):
        early = s < FIRST
        paired = jnp.logical_and(s >= EDGE, s < PAIRED)
        both = jnp.logical_or(early, paired)
        base = jnp.where(early, 2 * s, jnp.where(paired, 2 * (s - EDGE), jnp.where(s < EDGE, s + 12 - FIRST, s - 4)))
        late = jnp.where(paired, 1, 0)
        return (base, base + jnp.where(both, 1, 0)), (late, jnp.where(early, 0, 1))

    def gather(s, with_east):
        t_of, c_of = place(s)
        for w in range(2):
            r0 = t_of[w] // 4 * 6 + 3
            for arr, ext, dst in ((xo, xe, x2), (go, ge, g2)):
                halves = []
                for dz in range(2):
                    z = (t_of[w] % 4 * 2 + dz + 1) % 8
                    own = arr[z, pl.ds(r0, 6)].astype(F32).reshape(144, C).astype(BF)
                    part = dot(so_ref[c_of[w]], own)
                    if with_east:
                        ex = ext[z, pl.ds(r0, 6)].astype(F32).reshape(48, C).astype(BF)
                        part = part + dot(se_ref[c_of[w]], ex)
                    halves.append(part)
                dst[w * WTOK:(w + 1) * WTOK] = jnp.concatenate(halves, axis=0).astype(BF)

    def scatter(s, gin):
        t_of, c_of = place(s)
        for w in range(2):
            r0 = t_of[w] // 4 * 6 + 3
            for dz in range(2):
                z = (t_of[w] % 4 * 2 + dz + 1) % 8
                lo = w * WTOK + dz * 72
                part = gin[lo:lo + 72].astype(BF)
                own = dot(to_ref[c_of[w]], part).reshape(6, 24, C)
                fo[z, pl.ds(r0, 6)] = (fo[z, pl.ds(r0, 6)].astype(F32) + own).astype(BF)
                ex = dot(te_ref[c_of[w]], part).reshape(6, 8, C)
                fe[z, pl.ds(r0, 6)] = (fe[z, pl.ds(r0, 6)].astype(F32) + ex).astype(BF)

    def step(s, _):
        @pl.when(s == FIRST)
        def _():
            for cp in halo("e"):
                cp.wait_recv()

        @pl.when(jnp.logical_and(s == FIRST, has_south))
        def _():
            for cp in halo("s"):
                cp.wait_recv()

        for k in (8, 7, 6, 5, 4, 3, 2):
            run_stage(k, s)
        for k in (7, 6, 5, 4, 3, 2):
            @pl.when(s == NT - 2 + k)
            def _(k=k):
                w_stage(k)

        for part, when in ((0, EDGE), (1, EDGE + 2), (2, EDGE + 4), (3, NT)):
            @pl.when(s == when)
            def _(part=part):
                for cp in strips(part):
                    cp.start()

        @pl.when(jnp.logical_and(s == EDGE, has_south))
        def _():
            for cp in strips(4):
                cp.start()

        @pl.when(s < FIRST)
        def _():
            gather(s, False)

        @pl.when(jnp.logical_and(s >= FIRST, s < NT))
        def _():
            gather(s, True)

        @pl.when(s < NT)
        def _():
            t_of, _c = place(s)
            gin = window_pair(s, x2, g2, t_of, wq_ref, wqt_ref, wpt_ref, bm_ref, bt_ref,
                              gq, gp, gsum, gbuf)
            scatter(s, gin)

        run_stage(1, s)

        @pl.when(s == NT - 1)
        def _():
            w_stage(1)
        return 0

    lax.fori_loop(0, STEPS, step, 0)

    for part in range(4):
        for cp in strips(part):
            cp.wait_recv()
            cp.wait_send()

    @pl.when(has_north)
    def _():
        for cp in strips(4):
            cp.wait_recv()

    @pl.when(has_south)
    def _():
        for cp in strips(4):
            cp.wait_send()

    def finish(z, _):
        out_ref[z] = fo[z, 0:24]
        out_ref[z, 0:3] = fs[z]
        out_ref[z, :, 0:8] = add(out_ref[z, :, 0:8], fw[z, 0:24])
        return 0

    lax.fori_loop(0, 8, finish, 0)

    for cp in halo("e"):
        cp.wait_send()

    @pl.when(has_north)
    def _():
        for cp in halo("s"):
            cp.wait_send()

    for k in range(1, 7):
        for cp in w_copies(k):
            cp.wait_send()

    def drain(t, _):
        for k in range(1, 8):
            for cp in stage_copies(k, t):
                cp.wait_send()
        pltpu.make_async_copy(fin.at[t], f_hbm.at[t], out_sem.at[t]).wait()
        return 0

    lax.fori_loop(0, NT, drain, 0)


def fused(normed, cotangent, weight_qkv, weight_proj, bias_main, bias_tail):
    vm = pl.BlockSpec(memory_space=pltpu.VMEM)
    hbm = pl.BlockSpec(memory_space=pl.ANY)
    V = pltpu.VMEM
    return pl.pallas_call(
        fused_kernel,
        in_specs=[hbm, hbm] + [vm] * 4,
        out_specs=[vm, vm, hbm],
        out_shape=[
            jax.ShapeDtypeStruct(normed.shape, BF),
            jax.ShapeDtypeStruct((72, 16, 128), BF),
            jax.ShapeDtypeStruct((NT, 64, 16, 128), BF),
        ],
        scratch_shapes=[
            V((8, 27, 24, C), BF), V((8, 27, 24, C), BF), V((8, 27, 8, C), BF), V((8, 27, 8, C), BF),
            V((2 * WTOK, C), BF), V((2 * WTOK, C), BF),
            V((8, 27, 24, C), BF), V((8, 27, 8, C), BF), V((8, 27, 8, C), BF), V((8, 3, 24, C), BF),
            V((3, C, C), F32), V((C, C), F32), V((NT, WTOK, PACK), F32),
            V((NT, 64, 16, 128), BF), V((NT, 32, 16, 128), BF), V((NT, 32, 16, 128), BF),
            V((NT, 8, 16, 128), BF), V((NT, 16, 16, 128), BF), V((NT, 16, 16, 128), BF),
            V((NT, 8, 16, 128), BF), V((NT, 8, 16, 128), BF), V((NT, 64, 16, 128), BF),
            V((72, 16, 128), BF), V((36, 16, 128), BF), V((36, 16, 128), BF), V((3, 9, 16, 128), BF),
            V((4, 9, 16, 128), BF), V((4, 9, 16, 128), BF), V((72, 16, 128), BF),
            V((C, 768), BF), V((3, C, C), BF), V((C, C), BF),
            V((2, 72, 144), BF), V((2, 72, 48), BF), V((2, 144, 72), BF), V((2, 48, 72), BF),
            pltpu.SemaphoreType.DMA((2,)), pltpu.SemaphoreType.DMA((12,)), pltpu.SemaphoreType.DMA((12,)),
            pltpu.SemaphoreType.DMA((11, NT)), pltpu.SemaphoreType.DMA((11, NT)),
            pltpu.SemaphoreType.DMA((14,)), pltpu.SemaphoreType.DMA((14,)), pltpu.SemaphoreType.DMA((NT,)),
        ],
        compiler_params=pltpu.CompilerParams(collective_id=0, has_side_effects=True, vmem_limit_bytes=66_000_000),
        name="fused",
    )(normed, cotangent, weight_qkv, weight_proj, bias_main, bias_tail)


def local(normed, cotangent, weight_qkv, weight_proj, bias_table):
    bias_main, bias_tail = pack(bias_table.transpose(1, 0, 2))
    input_grad, w, f = fused(normed, cotangent, weight_qkv, weight_proj, bias_main, bias_tail)
    bias_grad, qkv_grad, proj_grad = unpack(f, w)
    return input_grad, qkv_grad, proj_grad, bias_grad.transpose(1, 0, 2)


def solution(mesh):
    in_specs = (P(None, "lat", "lon", None), P(None, "lat", "lon", None), P(), P(), P("lat", None, None))
    out_specs = (P(None, "lat", "lon", None), P(), P(), P("lat", None, None))
    return jax.shard_map(local, mesh=mesh, in_specs=in_specs, out_specs=out_specs, check_vma=False)
```

```python
import functools
import jax
import jax.numpy as jnp
from jax import lax
from jax.experimental import pallas as pl
from jax.experimental.pallas import tpu as pltpu
from jax.sharding import PartitionSpec as P

HEADS = 6
WTOK = 144
HD = 32
C = 192
MAIN = 128
TAIL = WTOK - MAIN
PACK = 896
NT = 16
SCALE = HD ** -0.5
LOG2E = 1.4426950408889634
BF = jnp.bfloat16
F32 = jnp.float32
MESH = pl.DeviceIdType.MESH
FIRST = 6
EDGE = 10
STEPS = 23
ST = 17
MASKED = -1e30


def dot(a, b):
    return jnp.dot(a, b, preferred_element_type=F32)


def lane_head(shape):
    return lax.broadcasted_iota(jnp.int32, shape, 1) // HD


def pack_head(b_ref, main_ref, tail_ref, sc, lanes, rows):
    lane = lax.broadcasted_iota(jnp.int32, (NT, 128), 1)

    def group(g, _):
        base = pl.multiple_of(g * 1152, 128)
        tiles = [b_ref[:, pl.ds(base + 128 * j, 128)].astype(F32) for j in range(9)]
        for j in range(8):
            if j == 0:
                main, sec = tiles[0], tiles[1]
            else:
                r = pltpu.roll(tiles[j], 128 - 16 * j, 1)
                sec = pltpu.roll(tiles[j + 1], 128 - 16 * j, 1)
                main = jnp.where(lane < 128 - 16 * j, r, sec)
            row = g * (8 * ST) + ST * j
            sc[0, pl.ds(row, NT), :] = main
            sc[1, pl.ds(row, NT), :] = sec
        return 0

    lax.fori_loop(0, 18, group, 0, unroll=9)
    last = (lax.axis_index("lat") == 7).astype(F32)

    def half(n):
        return jnp.logical_or(jnp.logical_and(n >= 36, n < 72), n >= 108)

    def masks(shape, k_axis, q_first):
        k = lax.broadcasted_iota(jnp.int32, shape, k_axis)
        q = lax.broadcasted_iota(jnp.int32, shape, 1 - k_axis)
        q = q if q_first == 0 else q * 0 + q_first
        z_no = jnp.logical_xor(k >= 72, q >= 72)
        l_no = jnp.logical_xor(half(k), half(q))
        return jnp.where(z_no, MASKED, 0.0), jnp.where(l_no, MASKED, 0.0) * last

    z_main, l_main = masks((WTOK, MAIN), 0, 0)
    z_tail, l_tail = masks((16, WTOK), 1, 128)

    def masked(x, t, z, l):
        if t % 4 != 3 and t // 4 != 3:
            return x
        y = x.astype(F32)
        if t % 4 == 3:
            y = y + z
        if t // 4 == 3:
            y = y + l
        return y.astype(BF)

    for t in range(NT):
        a = sc[0, pl.ds(t, WTOK, stride=ST), :].astype(BF)
        b = sc[1, pl.ds(t, WTOK, stride=ST), :].astype(BF)
        main_ref[t, 0:128, lanes] = masked(a[:MAIN].T, t, z_main[:128], l_main[:128])
        main_ref[t, 128:144, lanes] = masked(b[:MAIN].T[:16], t, z_main[128:], l_main[128:])
        tail_ref[t, rows, 0:128] = masked(a[MAIN:], t, z_tail[:, :128], l_tail[:, :128])
        tail_ref[t, rows, 128:144] = masked(b[MAIN:, 0:16], t, z_tail[:, 128:], l_tail[:, 128:])


def unpack_kernel(m_ref, t_ref, w_ref, out_ref, gq_ref, gp_ref, sc, tn):
    h = pl.program_id(0)

    @pl.when(h == 0)
    def _():
        for t in range(NT):
            tn[t] = t_ref[t].reshape(WTOK, 128).T
        for i in range(3):
            gq_ref[:, C * i:C * i + 128] = w_ref[24 * i:24 * i + 12].reshape(C, 128).astype(F32)
            rest = w_ref[24 * i + 12:24 * i + 24].reshape(C, 128).astype(F32)
            gq_ref[:, C * i + 128:C * i + C] = rest[:, :64]
            gp_ref[:, 64 * i:64 * i + 64] = rest[:, 64:]

    for t in range(NT):
        m = m_ref[t].reshape(WTOK, 128)
        sc[0, pl.ds(t, MAIN, stride=ST), :] = m[:MAIN].T.astype(F32)
        sc[1, pl.ds(t, MAIN, stride=ST), 0:16] = m[MAIN:].T.astype(F32)
        tl = tn[t, pl.ds(pl.multiple_of(h * 16, 16), 16), :].astype(F32)
        sc[0, pl.ds(MAIN * ST + t, 16, stride=ST), :] = tl[:, :128]
        sc[1, pl.ds(MAIN * ST + t, 16, stride=ST), 0:16] = tl[:, 128:]
    lane = lax.broadcasted_iota(jnp.int32, (NT, 128), 1)

    def group(g, _):
        base = pl.multiple_of(g * 1152, 128)
        r, s = [], []
        for j in range(8):
            row = g * (8 * ST) + ST * j
            m = sc[0, pl.ds(row, NT), :]
            t = sc[1, pl.ds(row, NT), :]
            r.append(pltpu.roll(m, 16 * j, 1) if j else m)
            s.append(pltpu.roll(t, 16 * j, 1) if j else t)
        for j in range(9):
            if j == 0:
                v = r[0]
            else:
                low = jnp.where(lane < 16 * (j - 1), r[j - 1], s[j - 1]) if j > 1 else s[0]
                v = jnp.where(lane < 16 * j, low, r[j]) if j < 8 else low
            out_ref[0, :, pl.ds(base + 128 * j, 128)] = v
        return 0

    lax.fori_loop(0, 18, group, 0, unroll=9)


def unpack(f, w):
    return pl.pallas_call(
        unpack_kernel, grid=(6,),
        in_specs=[pl.BlockSpec((NT, 9, 16, 128), lambda h: (0, h, 0, 0)),
                  pl.BlockSpec((NT, 9, 16, 128), lambda h: (0, 6, 0, 0)),
                  pl.BlockSpec((72, 16, 128), lambda h: (0, 0, 0))],
        out_specs=[pl.BlockSpec((1, NT, WTOK * WTOK), lambda h: (h, 0, 0)),
                   pl.BlockSpec((C, 3 * C), lambda h: (0, 0)), pl.BlockSpec((C, C), lambda h: (0, 0))],
        out_shape=[jax.ShapeDtypeStruct((6, NT, WTOK * WTOK), F32), jax.ShapeDtypeStruct((C, 3 * C), F32),
                   jax.ShapeDtypeStruct((C, C), F32)],
        scratch_shapes=[pltpu.VMEM((2, WTOK * ST, 128), F32), pltpu.VMEM((NT, 128, WTOK), BF)], name="unpack",
        cost_estimate=pl.CostEstimate(flops=10**9, bytes_accessed=12 * 2**20, transcendentals=0),
    )(f, f, w)


def add(*parts):
    total = parts[0].astype(F32)
    for part in parts[1:]:
        total = total + part.astype(F32)
    return total.astype(BF)


def window_pair(s, x2, g2, t_of, wq_ref, wqt_ref, wpt_ref, bm_ref, bt_ref,
                gq, gp, gsum, gbuf):
    x = x2[...]
    cot = g2[...]
    proj = dot(x, wq_ref[...]).astype(BF)
    dmix = dot(cot, wpt_ref[...]).astype(BF)
    xt = x.T
    dq_l, dk_l, dv_l, mixm, mixt, cott = [], [], [], [], [], []
    for c in range(2):
        t = t_of[c]
        rows = slice(c * WTOK, (c + 1) * WTOK)
        q = proj[rows, 0:192]
        k = proj[rows, 256:448]
        v = proj[rows, 512:704]
        dm = dmix[rows]
        ct = cot[rows]
        qt, kt, vt, dmt = q.T, k.T, v.T, dm.T
        hm = lane_head((MAIN, C))
        ht = lane_head((TAIL, C))
        zq = jnp.zeros((HD, MAIN), BF)

        def blk(at, p):
            top = jnp.concatenate([at[64 * p:64 * p + 32, :MAIN], zq], axis=1)
            bot = jnp.concatenate([zq, at[64 * p + 32:64 * p + 64, :MAIN]], axis=1)
            two = jnp.concatenate([top, bot], axis=0)
            if p == 2:
                return two
            z64 = jnp.zeros((64, 256), BF)
            return jnp.concatenate([two, z64] if p == 0 else [z64, two], axis=0)

        def nat(a, p):
            lanes = slice(0, 128) if p < 2 else slice(128, 192)
            am = a[:MAIN, lanes]
            hh = hm[:, lanes]
            z = jnp.zeros_like(am)
            return jnp.concatenate([jnp.where(hh == 2 * p, am, z), jnp.where(hh == 2 * p + 1, am, z)], axis=0)

        def nat_tail(a):
            am = a[MAIN:]
            z = jnp.zeros_like(am)
            return jnp.concatenate([jnp.where(ht == h, am, z) for h in range(HEADS)], axis=0)

        q_tail, dm_tail = nat_tail(q), nat_tail(dm)
        dn = (((1,), (1,)), ((), ()))
        dk_a = dk_b = dv_a = dv_b = None
        mix_parts, dq_parts = [], []
        for p in range(4):
            if p < 3:
                ln = slice(256 * p, 256 * p + 256)
                sub = slice(0, 128) if p < 2 else slice(128, 192)
                s_ = dot(k[:, sub], blk(qt, p))
                dp = dot(v[:, sub], blk(dmt, p))
                bias = bm_ref[t, :, ln].astype(F32)
            else:
                ln = slice(768, 864)
                s_ = lax.dot_general(k, q_tail, dn, preferred_element_type=F32)
                dp = lax.dot_general(v, dm_tail, dn, preferred_element_type=F32)
                bias = bt_ref[t].T.astype(F32)
            s_ = s_ * (SCALE * LOG2E) + bias * LOG2E
            m = jnp.max(s_, axis=0, keepdims=True)
            e = jnp.exp2(s_ - m)
            r = 1.0 / jnp.sum(e, axis=0, keepdims=True)
            pr = e * r
            pb = pr.astype(BF)
            d = jnp.sum(pr * dp, axis=0, keepdims=True)
            gs = pr * (dp - d)
            gb = gs.astype(BF)
            tot = gsum[t, :, ln] + gs
            gsum[t, :, ln] = tot
            tot = tot.astype(BF)
            if p < 3:
                gbuf[t, 18 * p:18 * p + 9] = tot[:, :128].reshape(9, 16, 128)
                gbuf[t, 18 * p + 9:18 * p + 18] = tot[:, 128:].reshape(9, 16, 128)
            else:
                gbuf[t, 54:63, :, 0:96] = tot.reshape(9, 16, 96)
            if p < 3:
                mo = dot(vt[64 * p:64 * p + 64], pb).astype(BF)
                do = dot(kt[64 * p:64 * p + 64], gb)
                mix_parts += [mo[:32, :MAIN], mo[32:, MAIN:]]
                dq_parts += [do[:32, :MAIN], do[32:, MAIN:]]
                dkp = dot(gb, nat(q, p))
                dvp = dot(pb, nat(dm, p))
                if p < 2:
                    dk_a = dkp if dk_a is None else dk_a + dkp
                    dv_a = dvp if dv_a is None else dv_a + dvp
                else:
                    dk_b, dv_b = dkp, dvp
            else:
                mo = dot(vt, pb).astype(BF)
                do = (dot(kt, gb) * SCALE).astype(BF)
                rh = lax.broadcasted_iota(jnp.int32, (C, 96), 0) // HD
                lh = lax.broadcasted_iota(jnp.int32, (C, 96), 1) // TAIL
                mixt.append(jnp.where(rh == lh, mo, jnp.zeros_like(mo)))
                dot_t = do.T
                dq_tail = jnp.zeros((TAIL, C), BF)
                for h in range(HEADS):
                    dq_tail = jnp.where(ht == h, dot_t[TAIL * h:TAIL * h + TAIL], dq_tail)
                dk_a = dk_a + dot(gb, q_tail[:, :128])
                dk_b = dk_b + dot(gb, q_tail[:, 128:])
                dv_a = dv_a + dot(pb, dm_tail[:, :128])
                dv_b = dv_b + dot(pb, dm_tail[:, 128:])
        mixm.append(jnp.concatenate(mix_parts, axis=0))
        dqt = (jnp.concatenate(dq_parts, axis=0) * SCALE).astype(BF)
        dq_l.append(jnp.concatenate([dqt.T, dq_tail], axis=0))
        dk_l.append((jnp.concatenate([dk_a, dk_b], axis=1) * SCALE).astype(BF))
        dv_l.append(jnp.concatenate([dv_a, dv_b], axis=1).astype(BF))
        cott.append(jnp.concatenate([ct[MAIN:]] * HEADS, axis=0))
    mm = jnp.concatenate(mixm, axis=1)
    cm = jnp.concatenate([cot[0:MAIN], cot[WTOK:WTOK + MAIN]], axis=0)
    gp[...] += dot(mm, cm) + dot(mixt[0], cott[0]) + dot(mixt[1], cott[1])
    dq = jnp.concatenate(dq_l, axis=0)
    dk = jnp.concatenate(dk_l, axis=0)
    dv = jnp.concatenate(dv_l, axis=0)
    gq[0] += dot(xt, dq)
    gq[1] += dot(xt, dk)
    gq[2] += dot(xt, dv)
    return dot(dq, wqt_ref[0]) + dot(dk, wqt_ref[1]) + dot(dv, wqt_ref[2])


def fused_kernel(x_hbm, g_hbm, wqkv_ref, wproj_ref, bias_hbm, out_ref, w_ref, f_hbm,
                 xo, go, xe, ge, x2, g2, fo, fe, fw, fs, gq, gp, gsum, gbuf, rd, hb, xa, xs, xb, ys, yr, fin,
                 wb, wr, wh, wx, wy, wz, wf, wq_ref, wqt_ref, wpt_ref, so_ref, se_ref, to_ref, te_ref,
                 bm_ref, bt_ref, bias_in, psc,
                 bias_sem, load_sem, halo_s, halo_r, ss, rs, ws, wrs, out_sem):
    lon = lax.axis_index("lon")
    lat = lax.axis_index("lat")
    n_lon = 16
    core = lon % 2
    yh = (lon // 2) % 2
    xx = lon // 4
    zz = lat % 4
    yl = lat // 4
    yy = yh * 2 + yl
    partner = lon + 1 - 2 * core
    right = (lon + 4) % n_lon
    left = (lon + 12) % n_lon
    ymate = lon + 2 - 4 * yh
    east = (lon + 1) % n_lon
    west = (lon + 15) % n_lon
    has_south = lat < 7
    has_north = lat > 0

    def peer(lon_, lat_):
        return {"lon": lon_, "lat": lat_}

    def xpeer(d):
        return peer((xx + d) % 4 * 4 + yh * 2 + core, lat)

    def ypeer(d):
        o = (yy + d) % 4
        return peer(xx * 4 + o // 2 * 2 + core, o % 2 * 4 + zz)

    def zpeer(d):
        return peer(lon, yl * 4 + (zz + d) % 4)

    def remote(src, dst, ssem, rsem, dev):
        return pltpu.make_async_remote_copy(src_ref=src, dst_ref=dst, send_sem=ssem, recv_sem=rsem,
                                            device_id=dev, device_id_type=MESH)

    own_loads = [pltpu.make_async_copy(x_hbm, xo.at[:, 0:24], load_sem.at[0]),
                 pltpu.make_async_copy(g_hbm, go.at[:, 0:24], load_sem.at[1])]
    for cp in own_loads:
        cp.start()
    for buf in (xe, ge):
        buf[...] = jnp.zeros_like(buf)
    for buf in (xo, go):
        buf[:, 24:27] = jnp.zeros((8, 3, 24, C), BF)
    for buf in (fw, fs):
        buf[...] = jnp.zeros_like(buf)

    for i in range(3):
        part = wqkv_ref[:, C * i:C * i + C]
        wq_ref[:, 256 * i:256 * i + C] = part
        wq_ref[:, 256 * i + C:256 * i + 256] = jnp.zeros((C, 64), BF)
        wqt_ref[i] = part.T
    wpt_ref[...] = wproj_ref[...].T
    for c in range(2):
        for ref, width, over, axis in ((so_ref, 24, False, 0), (se_ref, 8, True, 0), (to_ref, 24, False, 1),
                                       (te_ref, 8, True, 1)):
            shape = ref.shape[1:]
            tok = lax.broadcasted_iota(jnp.int32, shape, axis)
            at = lax.broadcasted_iota(jnp.int32, shape, 1 - axis)
            row = jnp.zeros(shape, jnp.int32)
            for m in range(1, 6):
                row = row + (tok >= 12 * m).astype(jnp.int32)
            col = tok - 12 * row + 6 + 12 * c
            hit = at == row * width + col - (24 if over else 0)
            hit = jnp.logical_and(hit, col >= 24 if over else col < 24)
            ref[c] = jnp.where(hit, 1.0, 0.0).astype(BF)

    barrier = pltpu.get_barrier_semaphore()
    greet = [peer(partner, lat), xpeer(1), xpeer(2), xpeer(3)] + [ypeer(d) for d in (1, 2, 3)] + [zpeer(d) for d in (1, 2, 3)]
    for dev in greet:
        pl.semaphore_signal(barrier, inc=1, device_id=dev, device_id_type=MESH)
    for dev in (peer(east, lat), peer(west, lat)):
        pl.semaphore_signal(barrier, inc=1, device_id=dev, device_id_type=MESH)

    @pl.when(has_north)
    def _():
        pl.semaphore_signal(barrier, inc=1, device_id=peer(lon, lat - 1), device_id_type=MESH)
        pl.semaphore_signal(barrier, inc=1, device_id=peer(west, lat - 1), device_id_type=MESH)

    @pl.when(has_south)
    def _():
        pl.semaphore_signal(barrier, inc=1, device_id=peer(lon, lat + 1), device_id_type=MESH)
        pl.semaphore_signal(barrier, inc=1, device_id=peer(east, lat + 1), device_id_type=MESH)

    pl.semaphore_wait(barrier, 12 + 2 * has_north.astype(jnp.int32) + 2 * has_south.astype(jnp.int32))

    def halo(which):
        out = []
        for n, (src, ext, own) in enumerate(((x_hbm, xe, xo), (g_hbm, ge, go))):
            if which == "e":
                out.append(remote(src.at[:, 3:24, 0:8], ext.at[:, 3:24], halo_s.at[n], halo_r.at[n], peer(west, lat)))
            if which == "s":
                out.append(remote(src.at[:, 0:3], own.at[:, 24:27], halo_s.at[2 + n], halo_r.at[2 + n],
                                  peer(lon, lat - 1)))
                out.append(remote(src.at[:, 0:3, 0:8], ext.at[:, 24:27], halo_s.at[4 + n], halo_r.at[4 + n],
                                  peer(west, lat - 1)))
        return out

    for cp in halo("e"):
        cp.start()

    @pl.when(has_north)
    def _():
        for cp in halo("s"):
            cp.start()

    def bias_load(h):
        return pltpu.make_async_copy(bias_hbm.at[h], bias_in.at[h % 2], bias_sem.at[h % 2])

    bias_load(0).start()
    gq[...] = jnp.zeros_like(gq)
    gp[...] = jnp.zeros_like(gp)
    fe[...] = jnp.zeros_like(fe)

    def clear(t, _):
        gsum[t] = jnp.zeros((WTOK, PACK), F32)
        gbuf[t, 54:64] = jnp.zeros((10, 16, 128), BF)
        return 0

    lax.fori_loop(0, NT, clear, 0)

    def clear_out(z, _):
        fo[z] = jnp.zeros((27, 24, C), BF)
        return 0

    lax.fori_loop(0, 8, clear_out, 0)
    def pack_one(h, _):
        @pl.when(h < HEADS - 1)
        def _():
            bias_load(h + 1).start()
        bias_load(h).wait()
        pack_head(bias_in.at[h % 2], bm_ref, bt_ref, psc, pl.ds(pl.multiple_of(h * MAIN, MAIN), MAIN),
                  pl.ds(pl.multiple_of(h * TAIL, TAIL), TAIL))
        return 0

    lax.fori_loop(0, HEADS, pack_one, 0)
    for cp in own_loads:
        cp.wait()

    mine = core * 32
    other = 32 - mine
    o8 = (xx + 2) % 4 * 8
    r8 = (xx + 1) % 4 * 8
    l8 = (xx + 3) % 4 * 8
    m8 = xx * 8

    def stage_copies(k, t):
        def rc(src, dst, lon_):
            return remote(src, dst, ss.at[k - 1], rs.at[k - 1, t], peer(lon_, lat))
        if k == 1:
            return [rc(gbuf.at[t, pl.ds(other, 32)], rd.at[t], partner)]
        if k == 2:
            return [rc(hb.at[t, pl.ds(o8, 4)], xa.at[t, 0:4], right),
                    rc(hb.at[t, pl.ds(o8 + 4, 4)], xa.at[t, 4:8], left)]
        if k == 3:
            return [rc(xs.at[t, 0:8], xb.at[t, 0:8], right), rc(xs.at[t, 8:16], xb.at[t, 8:16], left)]
        if k == 4:
            return [rc(ys.at[t], yr.at[t], ymate)]
        if k == 5:
            here = fin.at[t, pl.ds(mine + m8, 8)]
            return [rc(here, here, right), rc(here, here, left)]
        if k == 6:
            a = fin.at[t, pl.ds(mine + l8, 4)]
            b = fin.at[t, pl.ds(mine + r8 + 4, 4)]
            return [rc(a, a, right), rc(b, b, left)]
        half = fin.at[t, pl.ds(mine, 32)]
        return [rc(half, half, partner)]

    volume = (rd, xa, xb, yr, xb, xa, rd)

    def stage_arrived(k, t):
        ref = volume[k - 1].at[t]
        remote(ref, ref, ss.at[k - 1], rs.at[k - 1, t], peer(partner, lat)).wait_recv()

    def stage(k, t):
        if k > 1:
            stage_arrived(k - 1, t)
        if k == 2:
            hb[t] = add(gbuf[t, pl.ds(mine, 32)], rd[t])
        if k == 3:
            xs[t, 0:4] = add(hb[t, pl.ds(r8, 4)], xa[t, 0:4])
            xs[t, 4:8] = hb[t, pl.ds(r8 + 4, 4)]
            xs[t, 8:12] = hb[t, pl.ds(l8, 4)]
            xs[t, 12:16] = add(hb[t, pl.ds(l8 + 4, 4)], xa[t, 4:8])
        if k == 4:
            ys[t] = add(hb[t, pl.ds(m8, 8)], xb[t, 0:8], xb[t, 8:16])
        if k == 5:
            fin[t, pl.ds(mine + m8, 8)] = add(ys[t], yr[t])
        if k < 8:
            for cp in stage_copies(k, t):
                cp.start()
        else:
            pltpu.make_async_copy(fin.at[t], f_hbm.at[t], out_sem).start()

    def run_stage(k, s):
        d = s - (k - 1)

        @pl.when(jnp.logical_and(d >= EDGE, d < NT))
        def _():
            stage(k, 2 * (d - EDGE))
            stage(k, 2 * (d - EDGE) + 1)

        @pl.when(jnp.logical_and(d >= FIRST, d < EDGE))
        def _():
            stage(k, d + 12 - FIRST)

    wm = core * 36
    wo = 36 - wm

    def w_copies(k):
        def rc(src, dst, dev):
            return remote(src, dst, ws.at[0 if k in (1, 6) else 1], wrs.at[k - 1], dev)
        if k == 1:
            return [rc(wb.at[pl.ds(wo, 36)], wr, peer(partner, lat))]
        if k == 2:
            return [rc(wh.at[pl.ds((xx + d) % 4 * 9, 9)], wx.at[d - 1], xpeer(d)) for d in (1, 2, 3)]
        if k == 3:
            return [rc(wy.at[yy], wy.at[yy], ypeer(d)) for d in (1, 2, 3)]
        if k == 4:
            return [rc(wz.at[zz], wz.at[zz], zpeer(d)) for d in (1, 2, 3)]
        if k == 5:
            here = wf.at[pl.ds(wm + xx * 9, 9)]
            return [rc(here, here, xpeer(d)) for d in (1, 2, 3)]
        half = wf.at[pl.ds(wm, 36)]
        return [rc(half, half, peer(partner, lat))]

    def w_done(k, ref):
        return remote(ref, ref, ws.at[0 if k in (1, 6) else 1], wrs.at[k - 1], peer(partner, lat))

    def w_stage(k):
        if k > 1:
            w_done(k - 1, wr if k in (2, 7) else wx).wait_recv()
        if k == 1:
            for i in range(3):
                wb[24 * i:24 * i + 12] = gq[i, :, 0:128].astype(BF).reshape(12, 16, 128)
                wb[24 * i + 12:24 * i + 24, :, 0:64] = gq[i, :, 128:192].astype(BF).reshape(12, 16, 64)
                wb[24 * i + 12:24 * i + 24, :, 64:128] = gp[:, 64 * i:64 * i + 64].astype(BF).reshape(12, 16, 64)
        if k == 2:
            wh[...] = add(wb[pl.ds(wm, 36)], wr[...])
        if k == 3:
            wy[yy] = add(wh[pl.ds(xx * 9, 9)], wx[0], wx[1], wx[2])
        if k == 4:
            wz[zz] = add(wy[0], wy[1], wy[2], wy[3])
        if k == 5:
            wf[pl.ds(wm + xx * 9, 9)] = add(wz[0], wz[1], wz[2], wz[3])
        if k < 7:
            for cp in w_copies(k):
                cp.start()
        else:
            w_ref[...] = wf[...]

    def strips(part):
        if part < 4:
            r = (21, 3, 9, 15)[part]
            n = 3 if part == 0 else 6
            return [remote(fe.at[:, r:r + n], fw.at[:, r:r + n], halo_s.at[6 + part], halo_r.at[6 + part], peer(east, lat))]
        return [remote(fe.at[:, 24:27], fw.at[:, 0:3], halo_s.at[10], halo_r.at[10], peer(east, lat + 1)),
                remote(fo.at[:, 24:27], fs, halo_s.at[11], halo_r.at[11], peer(lon, lat + 1))]

    def place(s):
        early = s < FIRST
        paired = s >= EDGE
        both = jnp.logical_or(early, paired)
        base = jnp.where(early, 2 * s, jnp.where(paired, 2 * (s - EDGE), s + 12 - FIRST))
        late = jnp.where(paired, 1, 0)
        return (base, base + jnp.where(both, 1, 0)), (late, jnp.where(early, 0, 1))

    def gather(s, with_east):
        t_of, c_of = place(s)
        for w in range(2):
            r0 = t_of[w] // 4 * 6 + 3
            for arr, ext, dst in ((xo, xe, x2), (go, ge, g2)):
                halves = []
                for dz in range(2):
                    z = (t_of[w] % 4 * 2 + dz + 1) % 8
                    own = arr[z, pl.ds(r0, 6)].astype(F32).reshape(144, C).astype(BF)
                    part = dot(so_ref[c_of[w]], own)
                    if with_east:
                        ex = ext[z, pl.ds(r0, 6)].astype(F32).reshape(48, C).astype(BF)
                        part = part + dot(se_ref[c_of[w]], ex)
                    halves.append(part)
                dst[w * WTOK:(w + 1) * WTOK] = jnp.concatenate(halves, axis=0).astype(BF)

    def scatter(s, gin):
        t_of, c_of = place(s)
        for w in range(2):
            r0 = t_of[w] // 4 * 6 + 3
            for dz in range(2):
                z = (t_of[w] % 4 * 2 + dz + 1) % 8
                lo = w * WTOK + dz * 72
                part = gin[lo:lo + 72].astype(BF)
                own = dot(to_ref[c_of[w]], part).reshape(6, 24, C)
                fo[z, pl.ds(r0, 6)] = (fo[z, pl.ds(r0, 6)].astype(F32) + own).astype(BF)
                ex = dot(te_ref[c_of[w]], part).reshape(6, 8, C)
                fe[z, pl.ds(r0, 6)] = (fe[z, pl.ds(r0, 6)].astype(F32) + ex).astype(BF)

    def step(s, _):
        @pl.when(s == FIRST)
        def _():
            for cp in halo("e"):
                cp.wait_recv()

        @pl.when(jnp.logical_and(s == FIRST, has_south))
        def _():
            for cp in halo("s"):
                cp.wait_recv()

        for k in (8, 7, 6, 5, 4, 3, 2):
            run_stage(k, s)
        for k in (7, 6, 5, 4, 3, 2):
            @pl.when(s == NT - 2 + k)
            def _(k=k):
                w_stage(k)

        for part, when in ((0, EDGE), (1, EDGE + 2), (2, EDGE + 4), (3, NT)):
            @pl.when(s == when)
            def _(part=part):
                for cp in strips(part):
                    cp.start()

        @pl.when(jnp.logical_and(s == EDGE, has_south))
        def _():
            for cp in strips(4):
                cp.start()

        @pl.when(s < FIRST)
        def _():
            gather(s, False)

        @pl.when(jnp.logical_and(s >= FIRST, s < NT))
        def _():
            gather(s, True)

        @pl.when(s < NT)
        def _():
            t_of, _c = place(s)
            gin = window_pair(s, x2, g2, t_of, wq_ref, wqt_ref, wpt_ref, bm_ref, bt_ref,
                              gq, gp, gsum, gbuf)
            scatter(s, gin)

        run_stage(1, s)

        @pl.when(s == NT - 1)
        def _():
            w_stage(1)
        return 0

    lax.fori_loop(0, STEPS, step, 0)

    for part in range(4):
        for cp in strips(part):
            cp.wait_recv()
            cp.wait_send()

    @pl.when(has_north)
    def _():
        for cp in strips(4):
            cp.wait_recv()

    @pl.when(has_south)
    def _():
        for cp in strips(4):
            cp.wait_send()

    def finish(z, _):
        out_ref[z] = fo[z, 0:24]
        out_ref[z, 0:3] = fs[z]
        out_ref[z, :, 0:8] = add(out_ref[z, :, 0:8], fw[z, 0:24])
        return 0

    lax.fori_loop(0, 8, finish, 0)

    for cp in halo("e"):
        cp.wait_send()

    @pl.when(has_north)
    def _():
        for cp in halo("s"):
            cp.wait_send()

    w_done(1, wf).wait_send()
    for _ in range(4):
        w_done(2, wx).wait_send()
    for k in range(1, 8):
        ref = volume[k - 1]
        remote(ref, ref, ss.at[k - 1], rs.at[k - 1, 0], peer(partner, lat)).wait_send()
    pltpu.make_async_copy(fin, f_hbm, out_sem).wait()


def fused(normed, cotangent, weight_qkv, weight_proj, bias_view):
    vm = pl.BlockSpec(memory_space=pltpu.VMEM)
    hbm = pl.BlockSpec(memory_space=pl.ANY)
    V = pltpu.VMEM
    return pl.pallas_call(
        fused_kernel,
        in_specs=[hbm, hbm, vm, vm, hbm],
        out_specs=[vm, vm, hbm],
        out_shape=[
            jax.ShapeDtypeStruct(normed.shape, BF),
            jax.ShapeDtypeStruct((72, 16, 128), BF),
            jax.ShapeDtypeStruct((NT, 64, 16, 128), BF),
        ],
        scratch_shapes=[
            V((8, 27, 24, C), BF), V((8, 27, 24, C), BF), V((8, 27, 8, C), BF), V((8, 27, 8, C), BF),
            V((2 * WTOK, C), BF), V((2 * WTOK, C), BF),
            V((8, 27, 24, C), BF), V((8, 27, 8, C), BF), V((8, 27, 8, C), BF), V((8, 3, 24, C), BF),
            V((3, C, C), F32), V((C, C), F32), V((NT, WTOK, PACK), F32),
            V((NT, 64, 16, 128), BF), V((NT, 32, 16, 128), BF), V((NT, 32, 16, 128), BF),
            V((NT, 8, 16, 128), BF), V((NT, 16, 16, 128), BF), V((NT, 16, 16, 128), BF),
            V((NT, 8, 16, 128), BF), V((NT, 8, 16, 128), BF), V((NT, 64, 16, 128), BF),
            V((72, 16, 128), BF), V((36, 16, 128), BF), V((36, 16, 128), BF), V((3, 9, 16, 128), BF),
            V((4, 9, 16, 128), BF), V((4, 9, 16, 128), BF), V((72, 16, 128), BF),
            V((C, 768), BF), V((3, C, C), BF), V((C, C), BF),
            V((2, 72, 144), BF), V((2, 72, 48), BF), V((2, 144, 72), BF), V((2, 48, 72), BF),
            V((NT, WTOK, 6 * MAIN), BF), V((NT, 96, WTOK), BF), V((2, NT, WTOK * WTOK), BF),
            V((2, WTOK * ST, 128), F32), pltpu.SemaphoreType.DMA((2,)),
            pltpu.SemaphoreType.DMA((2,)), pltpu.SemaphoreType.DMA((12,)), pltpu.SemaphoreType.DMA((12,)),
            pltpu.SemaphoreType.DMA((7,)), pltpu.SemaphoreType.DMA((7, NT)),
            pltpu.SemaphoreType.DMA((2,)), pltpu.SemaphoreType.DMA((6,)), pltpu.SemaphoreType.DMA,
        ],
        compiler_params=pltpu.CompilerParams(collective_id=0, has_side_effects=True, vmem_limit_bytes=66_000_000),
        name="fused",
    )(normed, cotangent, weight_qkv, weight_proj, bias_view)


def local(normed, cotangent, weight_qkv, weight_proj, bias_table):
    input_grad, w, f = fused(normed, cotangent, weight_qkv, weight_proj, bias_table.transpose(1, 0, 2))
    bias_grad, qkv_grad, proj_grad = unpack(f, w)
    return input_grad, qkv_grad, proj_grad, bias_grad.transpose(1, 0, 2)


def solution(mesh):
    in_specs = (P(None, "lat", "lon", None), P(None, "lat", "lon", None), P(), P(), P("lat", None, None))
    out_specs = (P(None, "lat", "lon", None), P(), P(), P("lat", None, None))
    return jax.shard_map(local, mesh=mesh, in_specs=in_specs, out_specs=out_specs, check_vma=False)
```

```python
import functools
import jax
import jax.numpy as jnp
from jax import lax
from jax.experimental import pallas as pl
from jax.experimental.pallas import tpu as pltpu
from jax.sharding import PartitionSpec as P

HEADS = 6
WTOK = 144
HD = 32
C = 192
MAIN = 128
TAIL = WTOK - MAIN
PACK = 896
NT = 16
SCALE = HD ** -0.5
LOG2E = 1.4426950408889634
BF = jnp.bfloat16
F32 = jnp.float32
MESH = pl.DeviceIdType.MESH
FIRST = 6
EDGE = 10
STEPS = 23
ST = 17
MASKED = -1e30


def dot(a, b):
    return jnp.dot(a, b, preferred_element_type=F32)


def lane_head(shape):
    return lax.broadcasted_iota(jnp.int32, shape, 1) // HD


def pack_head(b_ref, main_ref, tail_ref, sc, lanes, rows):
    lane = lax.broadcasted_iota(jnp.int32, (NT, 128), 1)

    def group(g, _):
        base = pl.multiple_of(g * 1152, 128)
        tiles = [b_ref[:, pl.ds(base + 128 * j, 128)].astype(F32) for j in range(9)]
        for j in range(8):
            if j == 0:
                main, sec = tiles[0], tiles[1]
            else:
                r = pltpu.roll(tiles[j], 128 - 16 * j, 1)
                sec = pltpu.roll(tiles[j + 1], 128 - 16 * j, 1)
                main = jnp.where(lane < 128 - 16 * j, r, sec)
            row = g * (8 * ST) + ST * j
            sc[0, pl.ds(row, NT), :] = main
            sc[1, pl.ds(row, NT), :] = sec
        return 0

    lax.fori_loop(0, 18, group, 0, unroll=9)
    last = (lax.axis_index("lat") == 7).astype(F32)

    def half(n):
        return jnp.logical_or(jnp.logical_and(n >= 36, n < 72), n >= 108)

    def masks(shape, k_axis, q_first):
        k = lax.broadcasted_iota(jnp.int32, shape, k_axis)
        q = lax.broadcasted_iota(jnp.int32, shape, 1 - k_axis)
        q = q if q_first == 0 else q * 0 + q_first
        z_no = jnp.logical_xor(k >= 72, q >= 72)
        l_no = jnp.logical_xor(half(k), half(q))
        return jnp.where(z_no, MASKED, 0.0), jnp.where(l_no, MASKED, 0.0) * last

    z_main, l_main = masks((WTOK, MAIN), 0, 0)
    z_tail, l_tail = masks((16, WTOK), 1, 128)

    def masked(x, t, z, l):
        if t % 4 != 3 and t // 4 != 3:
            return x
        y = x.astype(F32)
        if t % 4 == 3:
            y = y + z
        if t // 4 == 3:
            y = y + l
        return y.astype(BF)

    for t in range(NT):
        a = sc[0, pl.ds(t, WTOK, stride=ST), :].astype(BF)
        b = sc[1, pl.ds(t, WTOK, stride=ST), :].astype(BF)
        main_ref[t, 0:128, lanes] = masked(a[:MAIN].T, t, z_main[:128], l_main[:128])
        main_ref[t, 128:144, lanes] = masked(b[:MAIN].T[:16], t, z_main[128:], l_main[128:])
        tail_ref[t, rows, 0:128] = masked(a[MAIN:], t, z_tail[:, :128], l_tail[:, :128])
        tail_ref[t, rows, 128:144] = masked(b[MAIN:, 0:16], t, z_tail[:, 128:], l_tail[:, 128:])


def unpack_kernel(m_ref, t_ref, w_ref, out_ref, gq_ref, gp_ref, sc, tn):
    h = pl.program_id(0)

    @pl.when(h == 0)
    def _():
        for t in range(NT):
            tn[t] = t_ref[t].reshape(WTOK, 128).T
        for i in range(3):
            gq_ref[:, C * i:C * i + 128] = w_ref[24 * i:24 * i + 12].reshape(C, 128).astype(F32)
            rest = w_ref[24 * i + 12:24 * i + 24].reshape(C, 128).astype(F32)
            gq_ref[:, C * i + 128:C * i + C] = rest[:, :64]
            gp_ref[:, 64 * i:64 * i + 64] = rest[:, 64:]

    for t in range(NT):
        m = m_ref[t].reshape(WTOK, 128)
        sc[0, pl.ds(t, MAIN, stride=ST), :] = m[:MAIN].T.astype(F32)
        sc[1, pl.ds(t, MAIN, stride=ST), 0:16] = m[MAIN:].T.astype(F32)
        tl = tn[t, pl.ds(pl.multiple_of(h * 16, 16), 16), :].astype(F32)
        sc[0, pl.ds(MAIN * ST + t, 16, stride=ST), :] = tl[:, :128]
        sc[1, pl.ds(MAIN * ST + t, 16, stride=ST), 0:16] = tl[:, 128:]
    lane = lax.broadcasted_iota(jnp.int32, (NT, 128), 1)

    def group(g, _):
        base = pl.multiple_of(g * 1152, 128)
        r, s = [], []
        for j in range(8):
            row = g * (8 * ST) + ST * j
            m = sc[0, pl.ds(row, NT), :]
            t = sc[1, pl.ds(row, NT), :]
            r.append(pltpu.roll(m, 16 * j, 1) if j else m)
            s.append(pltpu.roll(t, 16 * j, 1) if j else t)
        for j in range(9):
            if j == 0:
                v = r[0]
            else:
                low = jnp.where(lane < 16 * (j - 1), r[j - 1], s[j - 1]) if j > 1 else s[0]
                v = jnp.where(lane < 16 * j, low, r[j]) if j < 8 else low
            out_ref[0, :, pl.ds(base + 128 * j, 128)] = v
        return 0

    lax.fori_loop(0, 18, group, 0, unroll=9)


def unpack(f, w):
    return pl.pallas_call(
        unpack_kernel, grid=(6,),
        in_specs=[pl.BlockSpec((NT, 9, 16, 128), lambda h: (0, h, 0, 0)),
                  pl.BlockSpec((NT, 9, 16, 128), lambda h: (0, 6, 0, 0)),
                  pl.BlockSpec((72, 16, 128), lambda h: (0, 0, 0))],
        out_specs=[pl.BlockSpec((1, NT, WTOK * WTOK), lambda h: (h, 0, 0)),
                   pl.BlockSpec((C, 3 * C), lambda h: (0, 0)), pl.BlockSpec((C, C), lambda h: (0, 0))],
        out_shape=[jax.ShapeDtypeStruct((6, NT, WTOK * WTOK), F32), jax.ShapeDtypeStruct((C, 3 * C), F32),
                   jax.ShapeDtypeStruct((C, C), F32)],
        scratch_shapes=[pltpu.VMEM((2, WTOK * ST, 128), F32), pltpu.VMEM((NT, 128, WTOK), BF)], name="unpack",
        cost_estimate=pl.CostEstimate(flops=10**9, bytes_accessed=12 * 2**20, transcendentals=0),
    )(f, f, w)


def add(*parts):
    total = parts[0].astype(F32)
    for part in parts[1:]:
        total = total + part.astype(F32)
    return total.astype(BF)


def blk(at, p):
    zq = jnp.zeros((HD, MAIN), BF)
    top = jnp.concatenate([at[64 * p:64 * p + 32, :MAIN], zq], axis=1)
    bot = jnp.concatenate([zq, at[64 * p + 32:64 * p + 64, :MAIN]], axis=1)
    two = jnp.concatenate([top, bot], axis=0)
    if p == 2:
        return two
    z64 = jnp.zeros((64, 256), BF)
    return jnp.concatenate([two, z64] if p == 0 else [z64, two], axis=0)


def nat(a, p):
    lanes = slice(0, 128) if p < 2 else slice(128, 192)
    am = a[:MAIN, lanes]
    hh = lane_head((MAIN, C))[:, lanes]
    z = jnp.zeros_like(am)
    return jnp.concatenate([jnp.where(hh == 2 * p, am, z), jnp.where(hh == 2 * p + 1, am, z)], axis=0)


def nat_tail(a):
    am = a[MAIN:]
    ht = lane_head((TAIL, C))
    z = jnp.zeros_like(am)
    return jnp.concatenate([jnp.where(ht == h, am, z) for h in range(HEADS)], axis=0)


def score_part(x2, g2, pr, dmx, sc, dpc, wq_ref, wpt_ref):
    proj = dot(x2[...], wq_ref[...]).astype(BF)
    dmix = dot(g2[...], wpt_ref[...]).astype(BF)
    pr[...] = proj
    dmx[...] = dmix
    dn = (((1,), (1,)), ((), ()))
    for w in range(2):
        rows = slice(w * WTOK, (w + 1) * WTOK)
        q, k, v, dm = proj[rows, 0:192], proj[rows, 256:448], proj[rows, 512:704], dmix[rows]
        qt, dmt = q.T, dm.T
        for p in range(3):
            sub = slice(0, 128) if p < 2 else slice(128, 192)
            ln = slice(256 * p, 256 * p + 256)
            sc[w, :, ln] = dot(k[:, sub], blk(qt, p))
            dpc[w, :, ln] = dot(v[:, sub], blk(dmt, p))
        sc[w, :, 768:864] = lax.dot_general(k, nat_tail(q), dn, preferred_element_type=F32)
        dpc[w, :, 768:864] = lax.dot_general(v, nat_tail(dm), dn, preferred_element_type=F32)


def softmax_part(t_of, sc, dpc, pbs, gbs, bm_ref, bt_ref, gsum, gbuf):
    for w in range(2):
        t = t_of[w]
        for j in range(7):
            width = 128 if j < 6 else 96
            ln = slice(128 * j, 128 * j + width)
            bias = (bm_ref[t, :, ln] if j < 6 else bt_ref[t].T).astype(F32)
            z = sc[w, :, ln] * (SCALE * LOG2E) + bias * LOG2E
            m = jnp.max(z, axis=0, keepdims=True)
            e = jnp.exp2(z - m)
            r = 1.0 / jnp.sum(e, axis=0, keepdims=True)
            prob = e * r
            pbs[w, :, ln] = prob.astype(BF)
            dp = dpc[w, :, ln]
            d = jnp.sum(prob * dp, axis=0, keepdims=True)
            gs = prob * (dp - d)
            gbs[w, :, ln] = gs.astype(BF)
            tot = gsum[t, :, ln] + gs
            gsum[t, :, ln] = tot
            gbuf[t, 9 * j:9 * j + 9, :, 0:width] = tot.astype(BF).reshape(9, 16, width)


def closing_part(x2, g2, pr, dmx, pbs, gbs, wqt_ref, gq, gp):
    x = x2[...]
    cot = g2[...]
    proj = pr[...]
    xt = x.T
    ht = lane_head((TAIL, C))
    dq_l, dk_l, dv_l, mixm, mixt, cott = [], [], [], [], [], []
    for w in range(2):
        rows = slice(w * WTOK, (w + 1) * WTOK)
        q, k, v = proj[rows, 0:192], proj[rows, 256:448], proj[rows, 512:704]
        dm = dmx[rows]
        kt, vt = k.T, v.T
        q_tail, dm_tail = nat_tail(q), nat_tail(dm)
        mix_parts, dq_parts, dkp, dvp = [], [], [], []
        for p in range(3):
            pb = pbs[w, :, 256 * p:256 * p + 256]
            gb = gbs[w, :, 256 * p:256 * p + 256]
            mo = dot(vt[64 * p:64 * p + 64], pb).astype(BF)
            do = dot(kt[64 * p:64 * p + 64], gb)
            mix_parts += [mo[:32, :MAIN], mo[32:, MAIN:]]
            dq_parts += [do[:32, :MAIN], do[32:, MAIN:]]
            dkp.append(dot(gb, nat(q, p)))
            dvp.append(dot(pb, nat(dm, p)))
        pb = pbs[w, :, 768:864]
        gb = gbs[w, :, 768:864]
        mo = dot(vt, pb).astype(BF)
        do = (dot(kt, gb) * SCALE).astype(BF)
        rh = lax.broadcasted_iota(jnp.int32, (C, 96), 0) // HD
        lh = lax.broadcasted_iota(jnp.int32, (C, 96), 1) // TAIL
        mixt.append(jnp.where(rh == lh, mo, jnp.zeros_like(mo)))
        dot_t = do.T
        dq_tail = jnp.zeros((TAIL, C), BF)
        for h in range(HEADS):
            dq_tail = jnp.where(ht == h, dot_t[TAIL * h:TAIL * h + TAIL], dq_tail)
        dk_a = dkp[0] + dkp[1] + dot(gb, q_tail[:, :128])
        dk_b = dkp[2] + dot(gb, q_tail[:, 128:])
        dv_a = dvp[0] + dvp[1] + dot(pb, dm_tail[:, :128])
        dv_b = dvp[2] + dot(pb, dm_tail[:, 128:])
        mixm.append(jnp.concatenate(mix_parts, axis=0))
        dqt = (jnp.concatenate(dq_parts, axis=0) * SCALE).astype(BF)
        dq_l.append(jnp.concatenate([dqt.T, dq_tail], axis=0))
        dk_l.append((jnp.concatenate([dk_a, dk_b], axis=1) * SCALE).astype(BF))
        dv_l.append(jnp.concatenate([dv_a, dv_b], axis=1).astype(BF))
        cott.append(jnp.concatenate([cot[rows][MAIN:]] * HEADS, axis=0))
    mm = jnp.concatenate(mixm, axis=1)
    cm = jnp.concatenate([cot[0:MAIN], cot[WTOK:WTOK + MAIN]], axis=0)
    gp[...] += dot(mm, cm) + dot(mixt[0], cott[0]) + dot(mixt[1], cott[1])
    dq = jnp.concatenate(dq_l, axis=0)
    dk = jnp.concatenate(dk_l, axis=0)
    dv = jnp.concatenate(dv_l, axis=0)
    gq[0] += dot(xt, dq)
    gq[1] += dot(xt, dk)
    gq[2] += dot(xt, dv)
    return dot(dq, wqt_ref[0]) + dot(dk, wqt_ref[1]) + dot(dv, wqt_ref[2])


def fused_kernel(x_hbm, g_hbm, wqkv_ref, wproj_ref, bias_hbm, out_ref, w_ref, f_hbm,
                 xo, go, xe, ge, x2, g2, pr, dmx, sc, dpc, x2b, g2b, prb, dmxb, scb, dpcb, pbs, gbs, fo, fe, fw, fs, gq, gp, gsum, gbuf, rd, hb, xa, xs, xb, ys, yr, fin,
                 wb, wr, wh, wx, wy, wz, wf, wq_ref, wqt_ref, wpt_ref, so_ref, se_ref, to_ref, te_ref,
                 bm_ref, bt_ref, bias_in, psc,
                 bias_sem, load_sem, halo_s, halo_r, ss, rs, ws, wrs, out_sem):
    lon = lax.axis_index("lon")
    lat = lax.axis_index("lat")
    n_lon = 16
    core = lon % 2
    yh = (lon // 2) % 2
    xx = lon // 4
    zz = lat % 4
    yl = lat // 4
    yy = yh * 2 + yl
    partner = lon + 1 - 2 * core
    right = (lon + 4) % n_lon
    left = (lon + 12) % n_lon
    ymate = lon + 2 - 4 * yh
    east = (lon + 1) % n_lon
    west = (lon + 15) % n_lon
    has_south = lat < 7
    has_north = lat > 0

    def peer(lon_, lat_):
        return {"lon": lon_, "lat": lat_}

    def xpeer(d):
        return peer((xx + d) % 4 * 4 + yh * 2 + core, lat)

    def ypeer(d):
        o = (yy + d) % 4
        return peer(xx * 4 + o // 2 * 2 + core, o % 2 * 4 + zz)

    def zpeer(d):
        return peer(lon, yl * 4 + (zz + d) % 4)

    def remote(src, dst, ssem, rsem, dev):
        return pltpu.make_async_remote_copy(src_ref=src, dst_ref=dst, send_sem=ssem, recv_sem=rsem,
                                            device_id=dev, device_id_type=MESH)

    own_loads = [pltpu.make_async_copy(x_hbm, xo.at[:, 0:24], load_sem.at[0]),
                 pltpu.make_async_copy(g_hbm, go.at[:, 0:24], load_sem.at[1])]
    for cp in own_loads:
        cp.start()
    for buf in (xe, ge):
        buf[...] = jnp.zeros_like(buf)
    for buf in (xo, go):
        buf[:, 24:27] = jnp.zeros((8, 3, 24, C), BF)
    for buf in (fw, fs):
        buf[...] = jnp.zeros_like(buf)

    for i in range(3):
        part = wqkv_ref[:, C * i:C * i + C]
        wq_ref[:, 256 * i:256 * i + C] = part
        wq_ref[:, 256 * i + C:256 * i + 256] = jnp.zeros((C, 64), BF)
        wqt_ref[i] = part.T
    wpt_ref[...] = wproj_ref[...].T
    for c in range(2):
        for ref, width, over, axis in ((so_ref, 24, False, 0), (se_ref, 8, True, 0), (to_ref, 24, False, 1),
                                       (te_ref, 8, True, 1)):
            shape = ref.shape[1:]
            tok = lax.broadcasted_iota(jnp.int32, shape, axis)
            at = lax.broadcasted_iota(jnp.int32, shape, 1 - axis)
            row = jnp.zeros(shape, jnp.int32)
            for m in range(1, 6):
                row = row + (tok >= 12 * m).astype(jnp.int32)
            col = tok - 12 * row + 6 + 12 * c
            hit = at == row * width + col - (24 if over else 0)
            hit = jnp.logical_and(hit, col >= 24 if over else col < 24)
            ref[c] = jnp.where(hit, 1.0, 0.0).astype(BF)

    barrier = pltpu.get_barrier_semaphore()
    greet = [peer(partner, lat), xpeer(1), xpeer(2), xpeer(3)] + [ypeer(d) for d in (1, 2, 3)] + [zpeer(d) for d in (1, 2, 3)]
    for dev in greet:
        pl.semaphore_signal(barrier, inc=1, device_id=dev, device_id_type=MESH)
    for dev in (peer(east, lat), peer(west, lat)):
        pl.semaphore_signal(barrier, inc=1, device_id=dev, device_id_type=MESH)

    @pl.when(has_north)
    def _():
        pl.semaphore_signal(barrier, inc=1, device_id=peer(lon, lat - 1), device_id_type=MESH)
        pl.semaphore_signal(barrier, inc=1, device_id=peer(west, lat - 1), device_id_type=MESH)

    @pl.when(has_south)
    def _():
        pl.semaphore_signal(barrier, inc=1, device_id=peer(lon, lat + 1), device_id_type=MESH)
        pl.semaphore_signal(barrier, inc=1, device_id=peer(east, lat + 1), device_id_type=MESH)

    pl.semaphore_wait(barrier, 12 + 2 * has_north.astype(jnp.int32) + 2 * has_south.astype(jnp.int32))

    def halo(which):
        out = []
        for n, (src, ext, own) in enumerate(((x_hbm, xe, xo), (g_hbm, ge, go))):
            if which == "e":
                out.append(remote(src.at[:, 3:24, 0:8], ext.at[0:8, 3:24], halo_s.at[n], halo_r.at[n], peer(west, lat)))
            if which == "s":
                out.append(remote(src.at[:, 0:3], own.at[:, 24:27], halo_s.at[2 + n], halo_r.at[2 + n],
                                  peer(lon, lat - 1)))
                out.append(remote(src.at[:, 0:3, 0:8], ext.at[0:8, 24:27], halo_s.at[4 + n], halo_r.at[4 + n],
                                  peer(west, lat - 1)))
        return out

    for cp in halo("e"):
        cp.start()

    @pl.when(has_north)
    def _():
        for cp in halo("s"):
            cp.start()

    def bias_load(h):
        return pltpu.make_async_copy(bias_hbm.at[h], bias_in.at[h % 2], bias_sem.at[h % 2])

    bias_load(0).start()
    gq[...] = jnp.zeros_like(gq)
    gp[...] = jnp.zeros_like(gp)
    fe[...] = jnp.zeros_like(fe)

    def clear(t, _):
        gsum[t] = jnp.zeros((WTOK, PACK), F32)
        gbuf[t, 54:64] = jnp.zeros((10, 16, 128), BF)
        return 0

    lax.fori_loop(0, NT, clear, 0)

    def clear_out(z, _):
        fo[z] = jnp.zeros((27, 24, C), BF)
        return 0

    lax.fori_loop(0, 8, clear_out, 0)
    def pack_one(h, _):
        @pl.when(h < HEADS - 1)
        def _():
            bias_load(h + 1).start()
        bias_load(h).wait()
        pack_head(bias_in.at[h % 2], bm_ref, bt_ref, psc, pl.ds(pl.multiple_of(h * MAIN, MAIN), MAIN),
                  pl.ds(pl.multiple_of(h * TAIL, TAIL), TAIL))
        return 0

    lax.fori_loop(0, HEADS, pack_one, 0)
    for cp in own_loads:
        cp.wait()

    mine = core * 32
    other = 32 - mine
    o8 = (xx + 2) % 4 * 8
    r8 = (xx + 1) % 4 * 8
    l8 = (xx + 3) % 4 * 8
    m8 = xx * 8

    def stage_copies(k, t):
        def rc(src, dst, lon_):
            return remote(src, dst, ss.at[k - 1], rs.at[k - 1, t], peer(lon_, lat))
        if k == 1:
            return [rc(gbuf.at[t, pl.ds(other, 32)], rd.at[t], partner)]
        if k == 2:
            return [rc(hb.at[t, pl.ds(o8, 4)], xa.at[t, 0:4], right),
                    rc(hb.at[t, pl.ds(o8 + 4, 4)], xa.at[t, 4:8], left)]
        if k == 3:
            return [rc(xs.at[t, 0:8], xb.at[t, 0:8], right), rc(xs.at[t, 8:16], xb.at[t, 8:16], left)]
        if k == 4:
            return [rc(ys.at[t], yr.at[t], ymate)]
        if k == 5:
            here = fin.at[t, pl.ds(mine + m8, 8)]
            return [rc(here, here, right), rc(here, here, left)]
        if k == 6:
            a = fin.at[t, pl.ds(mine + l8, 4)]
            b = fin.at[t, pl.ds(mine + r8 + 4, 4)]
            return [rc(a, a, right), rc(b, b, left)]
        half = fin.at[t, pl.ds(mine, 32)]
        return [rc(half, half, partner)]

    volume = (rd, xa, xb, yr, xb, xa, rd)

    def stage_arrived(k, t):
        ref = volume[k - 1].at[t]
        remote(ref, ref, ss.at[k - 1], rs.at[k - 1, t], peer(partner, lat)).wait_recv()

    def stage(k, t):
        if k > 1:
            stage_arrived(k - 1, t)
        if k == 2:
            hb[t] = add(gbuf[t, pl.ds(mine, 32)], rd[t])
        if k == 3:
            xs[t, 0:4] = add(hb[t, pl.ds(r8, 4)], xa[t, 0:4])
            xs[t, 4:8] = hb[t, pl.ds(r8 + 4, 4)]
            xs[t, 8:12] = hb[t, pl.ds(l8, 4)]
            xs[t, 12:16] = add(hb[t, pl.ds(l8 + 4, 4)], xa[t, 4:8])
        if k == 4:
            ys[t] = add(hb[t, pl.ds(m8, 8)], xb[t, 0:8], xb[t, 8:16])
        if k == 5:
            fin[t, pl.ds(mine + m8, 8)] = add(ys[t], yr[t])
        if k < 8:
            for cp in stage_copies(k, t):
                cp.start()
        else:
            pltpu.make_async_copy(fin.at[t], f_hbm.at[t], out_sem).start()

    def run_stage(k, s):
        d = s - (k - 1)

        @pl.when(jnp.logical_and(d >= EDGE, d < NT))
        def _():
            stage(k, 2 * (d - EDGE))
            stage(k, 2 * (d - EDGE) + 1)

        @pl.when(jnp.logical_and(d >= FIRST, d < EDGE))
        def _():
            stage(k, d + 12 - FIRST)

    wm = core * 36
    wo = 36 - wm

    def w_copies(k):
        def rc(src, dst, dev):
            return remote(src, dst, ws.at[0 if k in (1, 6) else 1], wrs.at[k - 1], dev)
        if k == 1:
            return [rc(wb.at[pl.ds(wo, 36)], wr, peer(partner, lat))]
        if k == 2:
            return [rc(wh.at[pl.ds((xx + d) % 4 * 9, 9)], wx.at[d - 1], xpeer(d)) for d in (1, 2, 3)]
        if k == 3:
            return [rc(wy.at[yy], wy.at[yy], ypeer(d)) for d in (1, 2, 3)]
        if k == 4:
            return [rc(wz.at[zz], wz.at[zz], zpeer(d)) for d in (1, 2, 3)]
        if k == 5:
            here = wf.at[pl.ds(wm + xx * 9, 9)]
            return [rc(here, here, xpeer(d)) for d in (1, 2, 3)]
        half = wf.at[pl.ds(wm, 36)]
        return [rc(half, half, peer(partner, lat))]

    def w_done(k, ref):
        return remote(ref, ref, ws.at[0 if k in (1, 6) else 1], wrs.at[k - 1], peer(partner, lat))

    def w_stage(k):
        if k > 1:
            w_done(k - 1, wr if k in (2, 7) else wx).wait_recv()
        if k == 1:
            for i in range(3):
                wb[24 * i:24 * i + 12] = gq[i, :, 0:128].astype(BF).reshape(12, 16, 128)
                wb[24 * i + 12:24 * i + 24, :, 0:64] = gq[i, :, 128:192].astype(BF).reshape(12, 16, 64)
                wb[24 * i + 12:24 * i + 24, :, 64:128] = gp[:, 64 * i:64 * i + 64].astype(BF).reshape(12, 16, 64)
        if k == 2:
            wh[...] = add(wb[pl.ds(wm, 36)], wr[...])
        if k == 3:
            wy[yy] = add(wh[pl.ds(xx * 9, 9)], wx[0], wx[1], wx[2])
        if k == 4:
            wz[zz] = add(wy[0], wy[1], wy[2], wy[3])
        if k == 5:
            wf[pl.ds(wm + xx * 9, 9)] = add(wz[0], wz[1], wz[2], wz[3])
        if k < 7:
            for cp in w_copies(k):
                cp.start()
        else:
            w_ref[...] = wf[...]

    def strips(part):
        if part < 4:
            r = (21, 3, 9, 15)[part]
            n = 3 if part == 0 else 6
            return [remote(fe.at[:, r:r + n], fw.at[:, r:r + n], halo_s.at[6 + part], halo_r.at[6 + part], peer(east, lat))]
        return [remote(fe.at[:, 24:27], fw.at[:, 0:3], halo_s.at[10], halo_r.at[10], peer(east, lat + 1)),
                remote(fo.at[:, 24:27], fs, halo_s.at[11], halo_r.at[11], peer(lon, lat + 1))]

    def place(s):
        early = s < FIRST
        paired = s >= EDGE
        both = jnp.logical_or(early, paired)
        base = jnp.where(early, 2 * s, jnp.where(paired, 2 * (s - EDGE), s + 12 - FIRST))
        late = jnp.where(paired, 1, 0)
        return (base, base + jnp.where(both, 1, 0)), (late, jnp.where(early, 0, 1))

    def gather(s, x2, g2):
        t_of, c_of = place(s)
        for w in range(2):
            r0 = t_of[w] // 4 * 6 + 3
            for arr, ext, dst in ((xo, xe, x2), (go, ge, g2)):
                halves = []
                for dz in range(2):
                    z = (t_of[w] % 4 * 2 + dz + 1) % 8
                    ze = jnp.where(s < FIRST, 8, z)
                    own = arr[z, pl.ds(r0, 6)].astype(F32).reshape(144, C).astype(BF)
                    ex = ext[ze, pl.ds(r0, 6)].astype(F32).reshape(48, C).astype(BF)
                    halves.append(dot(so_ref[c_of[w]], own) + dot(se_ref[c_of[w]], ex))
                dst[w * WTOK:(w + 1) * WTOK] = jnp.concatenate(halves, axis=0).astype(BF)

    def scatter(s, gin):
        t_of, c_of = place(s)
        for w in range(2):
            r0 = t_of[w] // 4 * 6 + 3
            for dz in range(2):
                z = (t_of[w] % 4 * 2 + dz + 1) % 8
                lo = w * WTOK + dz * 72
                part = gin[lo:lo + 72].astype(BF)
                own = dot(to_ref[c_of[w]], part).reshape(6, 24, C)
                fo[z, pl.ds(r0, 6)] = (fo[z, pl.ds(r0, 6)].astype(F32) + own).astype(BF)
                ex = dot(te_ref[c_of[w]], part).reshape(6, 8, C)
                fe[z, pl.ds(r0, 6)] = (fe[z, pl.ds(r0, 6)].astype(F32) + ex).astype(BF)

    sets = ((x2, g2, pr, dmx, sc, dpc), (x2b, g2b, prb, dmxb, scb, dpcb))

    def comm(s):
        @pl.when(s == FIRST - 1)
        def _():
            for cp in halo("e"):
                cp.wait_recv()

        @pl.when(jnp.logical_and(s == FIRST - 1, has_south))
        def _():
            for cp in halo("s"):
                cp.wait_recv()

        for k in (8, 7, 6, 5, 4, 3, 2):
            run_stage(k, s)

        for part, when in ((0, EDGE), (1, EDGE + 2), (2, EDGE + 4), (3, NT)):
            @pl.when(s == when)
            def _(part=part):
                for cp in strips(part):
                    cp.start()

        @pl.when(jnp.logical_and(s == EDGE, has_south))
        def _():
            for cp in strips(4):
                cp.start()

    def begin(s, buf):
        gather(s, buf[0], buf[1])
        score_part(*buf, wq_ref, wpt_ref)

    def work(s, buf, after):
        t_of, _c = place(s)
        softmax_part(t_of, buf[4], buf[5], pbs, gbs, bm_ref, bt_ref, gsum, gbuf)
        if after is not None:
            begin(s + 1, after)
        scatter(s, closing_part(*buf[:4], pbs, gbs, wqt_ref, gq, gp))

    def two_steps(i, last):
        comm(2 * i)
        work(2 * i, sets[0], sets[1])
        run_stage(1, 2 * i)
        comm(2 * i + 1)
        work(2 * i + 1, sets[1], None if last else sets[0])
        run_stage(1, 2 * i + 1)

    def looped(i, _):
        two_steps(i, False)
        return 0

    begin(0, sets[0])
    lax.fori_loop(0, NT // 2 - 1, looped, 0)
    two_steps(NT // 2 - 1, True)
    w_stage(1)

    def tail(s, _):
        comm(s)
        for k in (7, 6, 5, 4, 3, 2):
            @pl.when(s == NT - 2 + k)
            def _(k=k):
                w_stage(k)
        return 0

    lax.fori_loop(NT, STEPS, tail, 0)

    for part in range(4):
        for cp in strips(part):
            cp.wait_recv()
            cp.wait_send()

    @pl.when(has_north)
    def _():
        for cp in strips(4):
            cp.wait_recv()

    @pl.when(has_south)
    def _():
        for cp in strips(4):
            cp.wait_send()

    def finish(z, _):
        out_ref[z] = fo[z, 0:24]
        out_ref[z, 0:3] = fs[z]
        out_ref[z, :, 0:8] = add(out_ref[z, :, 0:8], fw[z, 0:24])
        return 0

    lax.fori_loop(0, 8, finish, 0)

    for cp in halo("e"):
        cp.wait_send()

    @pl.when(has_north)
    def _():
        for cp in halo("s"):
            cp.wait_send()

    w_done(1, wf).wait_send()
    for _ in range(4):
        w_done(2, wx).wait_send()
    for k in range(1, 8):
        ref = volume[k - 1]
        remote(ref, ref, ss.at[k - 1], rs.at[k - 1, 0], peer(partner, lat)).wait_send()
    pltpu.make_async_copy(fin, f_hbm, out_sem).wait()


def fused(normed, cotangent, weight_qkv, weight_proj, bias_view):
    vm = pl.BlockSpec(memory_space=pltpu.VMEM)
    hbm = pl.BlockSpec(memory_space=pl.ANY)
    V = pltpu.VMEM
    return pl.pallas_call(
        fused_kernel,
        in_specs=[hbm, hbm, vm, vm, hbm],
        out_specs=[vm, vm, hbm],
        out_shape=[
            jax.ShapeDtypeStruct(normed.shape, BF),
            jax.ShapeDtypeStruct((72, 16, 128), BF),
            jax.ShapeDtypeStruct((NT, 64, 16, 128), BF),
        ],
        scratch_shapes=[
            V((8, 27, 24, C), BF), V((8, 27, 24, C), BF), V((9, 27, 8, C), BF), V((9, 27, 8, C), BF),
            V((2 * WTOK, C), BF), V((2 * WTOK, C), BF), V((2 * WTOK, 768), BF), V((2 * WTOK, C), BF),
            V((2, WTOK, PACK), F32), V((2, WTOK, PACK), F32),
            V((2 * WTOK, C), BF), V((2 * WTOK, C), BF), V((2 * WTOK, 768), BF), V((2 * WTOK, C), BF),
            V((2, WTOK, PACK), F32), V((2, WTOK, PACK), F32),
            V((2, WTOK, PACK), BF), V((2, WTOK, PACK), BF),
            V((8, 27, 24, C), BF), V((8, 27, 8, C), BF), V((8, 27, 8, C), BF), V((8, 3, 24, C), BF),
            V((3, C, C), F32), V((C, C), F32), V((NT, WTOK, PACK), F32),
            V((NT, 64, 16, 128), BF), V((NT, 32, 16, 128), BF), V((NT, 32, 16, 128), BF),
            V((NT, 8, 16, 128), BF), V((NT, 16, 16, 128), BF), V((NT, 16, 16, 128), BF),
            V((NT, 8, 16, 128), BF), V((NT, 8, 16, 128), BF), V((NT, 64, 16, 128), BF),
            V((72, 16, 128), BF), V((36, 16, 128), BF), V((36, 16, 128), BF), V((3, 9, 16, 128), BF),
            V((4, 9, 16, 128), BF), V((4, 9, 16, 128), BF), V((72, 16, 128), BF),
            V((C, 768), BF), V((3, C, C), BF), V((C, C), BF),
            V((2, 72, 144), BF), V((2, 72, 48), BF), V((2, 144, 72), BF), V((2, 48, 72), BF),
            V((NT, WTOK, 6 * MAIN), BF), V((NT, 96, WTOK), BF), V((2, NT, WTOK * WTOK), BF),
            V((2, WTOK * ST, 128), F32), pltpu.SemaphoreType.DMA((2,)),
            pltpu.SemaphoreType.DMA((2,)), pltpu.SemaphoreType.DMA((12,)), pltpu.SemaphoreType.DMA((12,)),
            pltpu.SemaphoreType.DMA((7,)), pltpu.SemaphoreType.DMA((7, NT)),
            pltpu.SemaphoreType.DMA((2,)), pltpu.SemaphoreType.DMA((6,)), pltpu.SemaphoreType.DMA,
        ],
        compiler_params=pltpu.CompilerParams(collective_id=0, has_side_effects=True, vmem_limit_bytes=66_000_000),
        name="fused",
    )(normed, cotangent, weight_qkv, weight_proj, bias_view)


def local(normed, cotangent, weight_qkv, weight_proj, bias_table):
    input_grad, w, f = fused(normed, cotangent, weight_qkv, weight_proj, bias_table.transpose(1, 0, 2))
    bias_grad, qkv_grad, proj_grad = unpack(f, w)
    return input_grad, qkv_grad, proj_grad, bias_grad.transpose(1, 0, 2)


def solution(mesh):
    in_specs = (P(None, "lat", "lon", None), P(None, "lat", "lon", None), P(), P(), P("lat", None, None))
    out_specs = (P(None, "lat", "lon", None), P(), P(), P("lat", None, None))
    return jax.shard_map(local, mesh=mesh, in_specs=in_specs, out_specs=out_specs, check_vma=False)
```

```python
import functools
import jax
import jax.numpy as jnp
from jax import lax
from jax.experimental import pallas as pl
from jax.experimental.pallas import tpu as pltpu
from jax.sharding import PartitionSpec as P

HEADS = 6
WTOK = 144
HD = 32
C = 192
MAIN = 128
TAIL = WTOK - MAIN
PACK = 896
NT = 16
SCALE = HD ** -0.5
LOG2E = 1.4426950408889634
BF = jnp.bfloat16
F32 = jnp.float32
MESH = pl.DeviceIdType.MESH
FIRST = 5
EDGE = 9
PAIRED = 14
STEPS = 28
OFFSET = (0, 0, 1, 3, 5, 7, 9, 11, 12)
W_AT = (0, 0, 16, 18, 20, 22, 24, 25)
ST = 17
MASKED = -1e30


def dot(a, b):
    return jnp.dot(a, b, preferred_element_type=F32)


def lane_head(shape):
    return lax.broadcasted_iota(jnp.int32, shape, 1) // HD


def pack_head(b_ref, main_ref, tail_ref, sc, lanes, rows):
    lane = lax.broadcasted_iota(jnp.int32, (NT, 128), 1)

    def group(g, _):
        base = pl.multiple_of(g * 1152, 128)
        tiles = [b_ref[:, pl.ds(base + 128 * j, 128)].astype(F32) for j in range(9)]
        for j in range(8):
            if j == 0:
                main, sec = tiles[0], tiles[1]
            else:
                r = pltpu.roll(tiles[j], 128 - 16 * j, 1)
                sec = pltpu.roll(tiles[j + 1], 128 - 16 * j, 1)
                main = jnp.where(lane < 128 - 16 * j, r, sec)
            row = g * (8 * ST) + ST * j
            sc[0, pl.ds(row, NT), :] = main
            sc[1, pl.ds(row, NT), :] = sec
        return 0

    lax.fori_loop(0, 18, group, 0, unroll=9)
    last = (lax.axis_index("lat") == 7).astype(F32)

    def half(n):
        return jnp.logical_or(jnp.logical_and(n >= 36, n < 72), n >= 108)

    def masks(shape, k_axis, q_first):
        k = lax.broadcasted_iota(jnp.int32, shape, k_axis)
        q = lax.broadcasted_iota(jnp.int32, shape, 1 - k_axis)
        q = q if q_first == 0 else q * 0 + q_first
        z_no = jnp.logical_xor(k >= 72, q >= 72)
        l_no = jnp.logical_xor(half(k), half(q))
        return jnp.where(z_no, MASKED, 0.0), jnp.where(l_no, MASKED, 0.0) * last

    z_main, l_main = masks((WTOK, MAIN), 0, 0)
    z_tail, l_tail = masks((16, WTOK), 1, 128)

    def masked(x, t, z, l):
        if t % 4 != 3 and t // 4 != 3:
            return x
        y = x.astype(F32)
        if t % 4 == 3:
            y = y + z
        if t // 4 == 3:
            y = y + l
        return y.astype(BF)

    for t in range(NT):
        a = sc[0, pl.ds(t, WTOK, stride=ST), :].astype(BF)
        b = sc[1, pl.ds(t, WTOK, stride=ST), :].astype(BF)
        main_ref[t, 0:128, lanes] = masked(a[:MAIN].T, t, z_main[:128], l_main[:128])
        main_ref[t, 128:144, lanes] = masked(b[:MAIN].T[:16], t, z_main[128:], l_main[128:])
        tail_ref[t, rows, 0:128] = masked(a[MAIN:], t, z_tail[:, :128], l_tail[:, :128])
        tail_ref[t, rows, 128:144] = masked(b[MAIN:, 0:16], t, z_tail[:, 128:], l_tail[:, 128:])


def unpack_kernel(m_ref, t_ref, w_ref, out_ref, gq_ref, gp_ref, sc, tn):
    h = pl.program_id(0)

    @pl.when(h == 0)
    def _():
        for t in range(NT):
            tn[t] = t_ref[t].reshape(WTOK, 128).T
        for i in range(3):
            gq_ref[:, C * i:C * i + 128] = w_ref[24 * i:24 * i + 12].reshape(C, 128).astype(F32)
            rest = w_ref[24 * i + 12:24 * i + 24].reshape(C, 128).astype(F32)
            gq_ref[:, C * i + 128:C * i + C] = rest[:, :64]
            gp_ref[:, 64 * i:64 * i + 64] = rest[:, 64:]

    for t in range(NT):
        m = m_ref[t].reshape(WTOK, 128)
        sc[0, pl.ds(t, MAIN, stride=ST), :] = m[:MAIN].T.astype(F32)
        sc[1, pl.ds(t, MAIN, stride=ST), 0:16] = m[MAIN:].T.astype(F32)
        tl = tn[t, pl.ds(pl.multiple_of(h * 16, 16), 16), :].astype(F32)
        sc[0, pl.ds(MAIN * ST + t, 16, stride=ST), :] = tl[:, :128]
        sc[1, pl.ds(MAIN * ST + t, 16, stride=ST), 0:16] = tl[:, 128:]
    lane = lax.broadcasted_iota(jnp.int32, (NT, 128), 1)

    def group(g, _):
        base = pl.multiple_of(g * 1152, 128)
        r, s = [], []
        for j in range(8):
            row = g * (8 * ST) + ST * j
            m = sc[0, pl.ds(row, NT), :]
            t = sc[1, pl.ds(row, NT), :]
            r.append(pltpu.roll(m, 16 * j, 1) if j else m)
            s.append(pltpu.roll(t, 16 * j, 1) if j else t)
        for j in range(9):
            if j == 0:
                v = r[0]
            else:
                low = jnp.where(lane < 16 * (j - 1), r[j - 1], s[j - 1]) if j > 1 else s[0]
                v = jnp.where(lane < 16 * j, low, r[j]) if j < 8 else low
            out_ref[0, :, pl.ds(base + 128 * j, 128)] = v
        return 0

    lax.fori_loop(0, 18, group, 0, unroll=9)


def unpack(f, w):
    return pl.pallas_call(
        unpack_kernel, grid=(6,),
        in_specs=[pl.BlockSpec((NT, 9, 16, 128), lambda h: (0, h, 0, 0)),
                  pl.BlockSpec((NT, 9, 16, 128), lambda h: (0, 6, 0, 0)),
                  pl.BlockSpec((72, 16, 128), lambda h: (0, 0, 0))],
        out_specs=[pl.BlockSpec((1, NT, WTOK * WTOK), lambda h: (h, 0, 0)),
                   pl.BlockSpec((C, 3 * C), lambda h: (0, 0)), pl.BlockSpec((C, C), lambda h: (0, 0))],
        out_shape=[jax.ShapeDtypeStruct((6, NT, WTOK * WTOK), F32), jax.ShapeDtypeStruct((C, 3 * C), F32),
                   jax.ShapeDtypeStruct((C, C), F32)],
        scratch_shapes=[pltpu.VMEM((2, WTOK * ST, 128), F32), pltpu.VMEM((NT, 128, WTOK), BF)], name="unpack",
        cost_estimate=pl.CostEstimate(flops=10**9, bytes_accessed=12 * 2**20, transcendentals=0),
    )(f, f, w)


def add(*parts):
    total = parts[0].astype(F32)
    for part in parts[1:]:
        total = total + part.astype(F32)
    return total.astype(BF)


def blk(at, p):
    zq = jnp.zeros((HD, MAIN), BF)
    top = jnp.concatenate([at[64 * p:64 * p + 32, :MAIN], zq], axis=1)
    bot = jnp.concatenate([zq, at[64 * p + 32:64 * p + 64, :MAIN]], axis=1)
    two = jnp.concatenate([top, bot], axis=0)
    if p == 2:
        return two
    z64 = jnp.zeros((64, 256), BF)
    return jnp.concatenate([two, z64] if p == 0 else [z64, two], axis=0)


def nat(a, p):
    lanes = slice(0, 128) if p < 2 else slice(128, 192)
    am = a[:MAIN, lanes]
    hh = lane_head((MAIN, C))[:, lanes]
    z = jnp.zeros_like(am)
    return jnp.concatenate([jnp.where(hh == 2 * p, am, z), jnp.where(hh == 2 * p + 1, am, z)], axis=0)


def nat_tail(a):
    am = a[MAIN:]
    ht = lane_head((TAIL, C))
    z = jnp.zeros_like(am)
    return jnp.concatenate([jnp.where(ht == h, am, z) for h in range(HEADS)], axis=0)


def score_part(x2, g2, pr, dmx, sc, dpc, wq_ref, wpt_ref):
    proj = dot(x2[...], wq_ref[...]).astype(BF)
    dmix = dot(g2[...], wpt_ref[...]).astype(BF)
    pr[...] = proj
    dmx[...] = dmix
    dn = (((1,), (1,)), ((), ()))
    for w in range(2):
        rows = slice(w * WTOK, (w + 1) * WTOK)
        q, k, v, dm = proj[rows, 0:192], proj[rows, 256:448], proj[rows, 512:704], dmix[rows]
        qt, dmt = q.T, dm.T
        for p in range(3):
            sub = slice(0, 128) if p < 2 else slice(128, 192)
            ln = slice(256 * p, 256 * p + 256)
            sc[w, :, ln] = dot(k[:, sub], blk(qt, p))
            dpc[w, :, ln] = dot(v[:, sub], blk(dmt, p))
        sc[w, :, 768:864] = lax.dot_general(k, nat_tail(q), dn, preferred_element_type=F32)
        dpc[w, :, 768:864] = lax.dot_general(v, nat_tail(dm), dn, preferred_element_type=F32)


def softmax_part(t_of, sc, dpc, pbs, gbs, bm_ref, bt_ref, gsum, gbuf):
    for w in range(2):
        t = t_of[w]
        for j in range(7):
            width = 128 if j < 6 else 96
            ln = slice(128 * j, 128 * j + width)
            bias = (bm_ref[t, :, ln] if j < 6 else bt_ref[t].T).astype(F32)
            z = sc[w, :, ln] * (SCALE * LOG2E) + bias * LOG2E
            m = jnp.max(z, axis=0, keepdims=True)
            e = jnp.exp2(z - m)
            r = 1.0 / jnp.sum(e, axis=0, keepdims=True)
            prob = e * r
            pbs[w, :, ln] = prob.astype(BF)
            dp = dpc[w, :, ln]
            d = jnp.sum(prob * dp, axis=0, keepdims=True)
            gs = prob * (dp - d)
            gbs[w, :, ln] = gs.astype(BF)
            tot = gsum[t, :, ln] + gs
            gsum[t, :, ln] = tot
            gbuf[t, 9 * j:9 * j + 9, :, 0:width] = tot.astype(BF).reshape(9, 16, width)


def closing_part(x2, g2, pr, dmx, pbs, gbs, wqt_ref, gq, gp):
    x = x2[...]
    cot = g2[...]
    proj = pr[...]
    xt = x.T
    ht = lane_head((TAIL, C))
    dq_l, dk_l, dv_l, mixm, mixt, cott = [], [], [], [], [], []
    for w in range(2):
        rows = slice(w * WTOK, (w + 1) * WTOK)
        q, k, v = proj[rows, 0:192], proj[rows, 256:448], proj[rows, 512:704]
        dm = dmx[rows]
        kt, vt = k.T, v.T
        q_tail, dm_tail = nat_tail(q), nat_tail(dm)
        mix_parts, dq_parts, dkp, dvp = [], [], [], []
        for p in range(3):
            pb = pbs[w, :, 256 * p:256 * p + 256]
            gb = gbs[w, :, 256 * p:256 * p + 256]
            mo = dot(vt[64 * p:64 * p + 64], pb).astype(BF)
            do = dot(kt[64 * p:64 * p + 64], gb)
            mix_parts += [mo[:32, :MAIN], mo[32:, MAIN:]]
            dq_parts += [do[:32, :MAIN], do[32:, MAIN:]]
            dkp.append(dot(gb, nat(q, p)))
            dvp.append(dot(pb, nat(dm, p)))
        pb = pbs[w, :, 768:864]
        gb = gbs[w, :, 768:864]
        mo = dot(vt, pb).astype(BF)
        do = (dot(kt, gb) * SCALE).astype(BF)
        rh = lax.broadcasted_iota(jnp.int32, (C, 96), 0) // HD
        lh = lax.broadcasted_iota(jnp.int32, (C, 96), 1) // TAIL
        mixt.append(jnp.where(rh == lh, mo, jnp.zeros_like(mo)))
        dot_t = do.T
        dq_tail = jnp.zeros((TAIL, C), BF)
        for h in range(HEADS):
            dq_tail = jnp.where(ht == h, dot_t[TAIL * h:TAIL * h + TAIL], dq_tail)
        dk_a = dkp[0] + dkp[1] + dot(gb, q_tail[:, :128])
        dk_b = dkp[2] + dot(gb, q_tail[:, 128:])
        dv_a = dvp[0] + dvp[1] + dot(pb, dm_tail[:, :128])
        dv_b = dvp[2] + dot(pb, dm_tail[:, 128:])
        mixm.append(jnp.concatenate(mix_parts, axis=0))
        dqt = (jnp.concatenate(dq_parts, axis=0) * SCALE).astype(BF)
        dq_l.append(jnp.concatenate([dqt.T, dq_tail], axis=0))
        dk_l.append((jnp.concatenate([dk_a, dk_b], axis=1) * SCALE).astype(BF))
        dv_l.append(jnp.concatenate([dv_a, dv_b], axis=1).astype(BF))
        cott.append(jnp.concatenate([cot[rows][MAIN:]] * HEADS, axis=0))
    mm = jnp.concatenate(mixm, axis=1)
    cm = jnp.concatenate([cot[0:MAIN], cot[WTOK:WTOK + MAIN]], axis=0)
    gp[...] += dot(mm, cm) + dot(mixt[0], cott[0]) + dot(mixt[1], cott[1])
    dq = jnp.concatenate(dq_l, axis=0)
    dk = jnp.concatenate(dk_l, axis=0)
    dv = jnp.concatenate(dv_l, axis=0)
    gq[0] += dot(xt, dq)
    gq[1] += dot(xt, dk)
    gq[2] += dot(xt, dv)
    return dot(dq, wqt_ref[0]) + dot(dk, wqt_ref[1]) + dot(dv, wqt_ref[2])


def fused_kernel(x_hbm, g_hbm, wqkv_ref, wproj_ref, bias_hbm, out_ref, w_ref, f_hbm,
                 xo, go, xe, ge, x2, g2, pr, dmx, sc, dpc, x2b, g2b, prb, dmxb, scb, dpcb, pbs, gbs, fo, fe, fw, fs, gq, gp, gsum, gbuf, rd, hb, xa, xs, xb, ys, yr, fin,
                 wb, wr, wh, wx, wy, wz, wf, wq_ref, wqt_ref, wpt_ref, so_ref, se_ref, to_ref, te_ref,
                 bm_ref, bt_ref, bias_in, psc, hs, hx, cs_ref, sse_ref,
                 bias_sem, load_sem, halo_s, halo_r, ss, rs, ws, wrs, out_sem):
    lon = lax.axis_index("lon")
    lat = lax.axis_index("lat")
    n_lon = 16
    core = lon % 2
    yh = (lon // 2) % 2
    xx = lon // 4
    zz = lat % 4
    yl = lat // 4
    yy = yh * 2 + yl
    partner = lon + 1 - 2 * core
    right = (lon + 4) % n_lon
    left = (lon + 12) % n_lon
    ymate = lon + 2 - 4 * yh
    east = (lon + 1) % n_lon
    west = (lon + 15) % n_lon
    has_south = lat < 7
    has_north = lat > 0

    def peer(lon_, lat_):
        return {"lon": lon_, "lat": lat_}

    def xpeer(d):
        return peer((xx + d) % 4 * 4 + yh * 2 + core, lat)

    def ypeer(d):
        o = (yy + d) % 4
        return peer(xx * 4 + o // 2 * 2 + core, o % 2 * 4 + zz)

    def zpeer(d):
        return peer(lon, yl * 4 + (zz + d) % 4)

    def remote(src, dst, ssem, rsem, dev):
        return pltpu.make_async_remote_copy(src_ref=src, dst_ref=dst, send_sem=ssem, recv_sem=rsem,
                                            device_id=dev, device_id_type=MESH)

    own_loads = [pltpu.make_async_copy(x_hbm, xo.at[:, 0:24], load_sem.at[0]),
                 pltpu.make_async_copy(g_hbm, go.at[:, 0:24], load_sem.at[1])]
    for cp in own_loads:
        cp.start()
    for buf in (xe, ge):
        buf[...] = jnp.zeros_like(buf)
    for buf in (xo, go):
        buf[:, 24:27] = jnp.zeros((8, 3, 24, C), BF)
    for buf in (fw, fs):
        buf[...] = jnp.zeros_like(buf)

    for i in range(3):
        part = wqkv_ref[:, C * i:C * i + C]
        wq_ref[:, 256 * i:256 * i + C] = part
        wq_ref[:, 256 * i + C:256 * i + 256] = jnp.zeros((C, 64), BF)
        wqt_ref[i] = part.T
    wpt_ref[...] = wproj_ref[...].T
    def token(shape, axis):
        tok = lax.broadcasted_iota(jnp.int32, shape, axis)
        row = jnp.zeros(shape, jnp.int32)
        for m in range(1, 6):
            row = row + (tok >= 12 * m).astype(jnp.int32)
        return row, tok - 12 * row, lax.broadcasted_iota(jnp.int32, shape, 1 - axis)

    def one_hot(hit):
        return jnp.where(hit, 1.0, 0.0).astype(BF)

    for c in range(2):
        for ref, width, over, axis in ((so_ref, 24, False, 0), (to_ref, 24, False, 1), (te_ref, 8, True, 1)):
            row, col, at = token(ref.shape[1:], axis)
            col = col + 6 + 12 * c
            hit = at == row * width + col - (24 if over else 0)
            ref[c] = one_hot(jnp.logical_and(hit, col >= 24 if over else col < 24))
    for b in range(4):
        row, col, at = token((72, 128), 0)
        hit = jnp.logical_and(at == 36 * b + 6 * row + col - 6, col >= 6)
        se_ref[b] = one_hot(jnp.logical_and(hit, row < 3) if b == 3 else hit)
    se_ref[4] = jnp.zeros((72, 128), BF)
    row, col, at = token((72, 24), 0)
    sse_ref[0] = jnp.zeros((72, 24), BF)
    sse_ref[1] = one_hot(jnp.logical_and(at == 8 * row - 24 + col - 6, jnp.logical_and(row >= 3, col >= 6)))
    kept_row = lax.broadcasted_iota(jnp.int32, (128, 168), 0)
    group = jnp.zeros((128, 168), jnp.int32)
    for m in range(1, 21):
        group = group + (kept_row >= 6 * m).astype(jnp.int32)
    at = lax.broadcasted_iota(jnp.int32, (128, 168), 1)
    cs_ref[...] = one_hot(jnp.logical_and(at == kept_row + 2 * group, kept_row < 126))
    hx[:, 4] = jnp.zeros((2, 3, 128, 128), BF)

    barrier = pltpu.get_barrier_semaphore()
    greet = [peer(partner, lat), xpeer(1), xpeer(2), xpeer(3)] + [ypeer(d) for d in (1, 2, 3)] + [zpeer(d) for d in (1, 2, 3)]
    for dev in greet:
        pl.semaphore_signal(barrier, inc=1, device_id=dev, device_id_type=MESH)
    for dev in (peer(east, lat), peer(west, lat)):
        pl.semaphore_signal(barrier, inc=1, device_id=dev, device_id_type=MESH)

    @pl.when(has_north)
    def _():
        pl.semaphore_signal(barrier, inc=1, device_id=peer(lon, lat - 1), device_id_type=MESH)
        pl.semaphore_signal(barrier, inc=1, device_id=peer(west, lat - 1), device_id_type=MESH)

    @pl.when(has_south)
    def _():
        pl.semaphore_signal(barrier, inc=1, device_id=peer(lon, lat + 1), device_id_type=MESH)
        pl.semaphore_signal(barrier, inc=1, device_id=peer(east, lat + 1), device_id_type=MESH)

    pl.semaphore_wait(barrier, 12 + 2 * has_north.astype(jnp.int32) + 2 * has_south.astype(jnp.int32))

    def halo(which):
        out = []
        for n, (src, ext, own) in enumerate(((x_hbm, xe, xo), (g_hbm, ge, go))):
            if which == "e":
                out.append(remote(hs.at[n], hx.at[n, 0:4], halo_s.at[n], halo_r.at[n], peer(west, lat)))
            if which == "s":
                out.append(remote(src.at[:, 0:3], own.at[:, 24:27], halo_s.at[2 + n], halo_r.at[2 + n],
                                  peer(lon, lat - 1)))
                out.append(remote(src.at[:, 0:3, 0:8], ext.at[0:8], halo_s.at[4 + n], halo_r.at[4 + n],
                                  peer(west, lat - 1)))
        return out

    @pl.when(has_north)
    def _():
        for cp in halo("s"):
            cp.start()

    for cp in own_loads:
        cp.wait()
    for n, arr in enumerate((xo, go)):
        for zp in range(4):
            kept = []
            for dz in range(2):
                edge = arr[2 * zp + dz, 3:24, 0:8].astype(F32).reshape(168, C).astype(BF)
                kept.append(dot(cs_ref[...], edge).astype(BF))
            hs[n, zp, 0] = kept[0][:, :128]
            hs[n, zp, 1] = kept[1][:, :128]
            hs[n, zp, 2] = jnp.concatenate([kept[0][:, 128:], kept[1][:, 128:]], axis=1)
    for cp in halo("e"):
        cp.start()

    def bias_load(h):
        return pltpu.make_async_copy(bias_hbm.at[h], bias_in.at[h % 2], bias_sem.at[h % 2])

    bias_load(0).start()
    gq[...] = jnp.zeros_like(gq)
    gp[...] = jnp.zeros_like(gp)
    fe[...] = jnp.zeros_like(fe)

    def clear(t, _):
        gsum[t] = jnp.zeros((WTOK, PACK), F32)
        gbuf[t, 54:64] = jnp.zeros((10, 16, 128), BF)
        return 0

    lax.fori_loop(0, NT, clear, 0)

    def clear_out(z, _):
        fo[z] = jnp.zeros((27, 24, C), BF)
        return 0

    lax.fori_loop(0, 8, clear_out, 0)
    def pack_one(h, _):
        @pl.when(h < HEADS - 1)
        def _():
            bias_load(h + 1).start()
        bias_load(h).wait()
        pack_head(bias_in.at[h % 2], bm_ref, bt_ref, psc, pl.ds(pl.multiple_of(h * MAIN, MAIN), MAIN),
                  pl.ds(pl.multiple_of(h * TAIL, TAIL), TAIL))
        return 0

    lax.fori_loop(0, HEADS, pack_one, 0)

    mine = core * 32
    other = 32 - mine
    o8 = (xx + 2) % 4 * 8
    r8 = (xx + 1) % 4 * 8
    l8 = (xx + 3) % 4 * 8
    m8 = xx * 8

    def stage_copies(k, t):
        def rc(src, dst, lon_):
            return remote(src, dst, ss.at[k - 1], rs.at[k - 1, t], peer(lon_, lat))
        if k == 1:
            return [rc(gbuf.at[t, pl.ds(other, 32)], rd.at[t], partner)]
        if k == 2:
            return [rc(hb.at[t, pl.ds(o8, 4)], xa.at[t, 0:4], right),
                    rc(hb.at[t, pl.ds(o8 + 4, 4)], xa.at[t, 4:8], left)]
        if k == 3:
            return [rc(xs.at[t, 0:8], xb.at[t, 0:8], right), rc(xs.at[t, 8:16], xb.at[t, 8:16], left)]
        if k == 4:
            return [rc(ys.at[t], yr.at[t], ymate)]
        if k == 5:
            here = fin.at[t, pl.ds(mine + m8, 8)]
            return [rc(here, here, right), rc(here, here, left)]
        if k == 6:
            a = fin.at[t, pl.ds(mine + l8, 4)]
            b = fin.at[t, pl.ds(mine + r8 + 4, 4)]
            return [rc(a, a, right), rc(b, b, left)]
        half = fin.at[t, pl.ds(mine, 32)]
        return [rc(half, half, partner)]

    volume = (rd, xa, xb, yr, xb, xa, rd)

    def stage_arrived(k, t):
        ref = volume[k - 1].at[t]
        remote(ref, ref, ss.at[k - 1], rs.at[k - 1, t], peer(partner, lat)).wait_recv()

    def stage(k, t):
        if k > 1:
            stage_arrived(k - 1, t)
        if k == 2:
            hb[t] = add(gbuf[t, pl.ds(mine, 32)], rd[t])
        if k == 3:
            xs[t, 0:4] = add(hb[t, pl.ds(r8, 4)], xa[t, 0:4])
            xs[t, 4:8] = hb[t, pl.ds(r8 + 4, 4)]
            xs[t, 8:12] = hb[t, pl.ds(l8, 4)]
            xs[t, 12:16] = add(hb[t, pl.ds(l8 + 4, 4)], xa[t, 4:8])
        if k == 4:
            ys[t] = add(hb[t, pl.ds(m8, 8)], xb[t, 0:8], xb[t, 8:16])
        if k == 5:
            fin[t, pl.ds(mine + m8, 8)] = add(ys[t], yr[t])
        if k < 8:
            for cp in stage_copies(k, t):
                cp.start()
        else:
            pltpu.make_async_copy(fin.at[t], f_hbm.at[t], out_sem).start()

    def run_stage(k, s):
        d = s - OFFSET[k]

        @pl.when(jnp.logical_and(d >= EDGE, d < PAIRED))
        def _():
            stage(k, 2 * (d - EDGE))
            stage(k, 2 * (d - EDGE) + 1)

        @pl.when(jnp.logical_or(jnp.logical_and(d >= FIRST, d < EDGE), jnp.logical_and(d >= PAIRED, d < NT)))
        def _():
            stage(k, jnp.where(d < EDGE, d + 12 - FIRST, d - 4))

    wm = core * 36
    wo = 36 - wm

    def w_copies(k):
        def rc(src, dst, dev):
            return remote(src, dst, ws.at[0 if k in (1, 6) else 1], wrs.at[k - 1], dev)
        if k == 1:
            return [rc(wb.at[pl.ds(wo, 36)], wr, peer(partner, lat))]
        if k == 2:
            return [rc(wh.at[pl.ds((xx + d) % 4 * 9, 9)], wx.at[d - 1], xpeer(d)) for d in (1, 2, 3)]
        if k == 3:
            return [rc(wy.at[yy], wy.at[yy], ypeer(d)) for d in (1, 2, 3)]
        if k == 4:
            return [rc(wz.at[zz], wz.at[zz], zpeer(d)) for d in (1, 2, 3)]
        if k == 5:
            here = wf.at[pl.ds(wm + xx * 9, 9)]
            return [rc(here, here, xpeer(d)) for d in (1, 2, 3)]
        half = wf.at[pl.ds(wm, 36)]
        return [rc(half, half, peer(partner, lat))]

    def w_done(k, ref):
        return remote(ref, ref, ws.at[0 if k in (1, 6) else 1], wrs.at[k - 1], peer(partner, lat))

    def w_stage(k):
        if k > 1:
            w_done(k - 1, wr if k in (2, 7) else wx).wait_recv()
        if k == 1:
            for i in range(3):
                wb[24 * i:24 * i + 12] = gq[i, :, 0:128].astype(BF).reshape(12, 16, 128)
                wb[24 * i + 12:24 * i + 24, :, 0:64] = gq[i, :, 128:192].astype(BF).reshape(12, 16, 64)
                wb[24 * i + 12:24 * i + 24, :, 64:128] = gp[:, 64 * i:64 * i + 64].astype(BF).reshape(12, 16, 64)
        if k == 2:
            wh[...] = add(wb[pl.ds(wm, 36)], wr[...])
        if k == 3:
            wy[yy] = add(wh[pl.ds(xx * 9, 9)], wx[0], wx[1], wx[2])
        if k == 4:
            wz[zz] = add(wy[0], wy[1], wy[2], wy[3])
        if k == 5:
            wf[pl.ds(wm + xx * 9, 9)] = add(wz[0], wz[1], wz[2], wz[3])
        if k < 7:
            for cp in w_copies(k):
                cp.start()
        else:
            w_ref[...] = wf[...]

    def strips(part):
        if part < 4:
            r = (21, 3, 9, 15)[part]
            n = 3 if part == 0 else 6
            return [remote(fe.at[:, r:r + n], fw.at[:, r:r + n], halo_s.at[6 + part], halo_r.at[6 + part], peer(east, lat))]
        return [remote(fe.at[:, 24:27], fw.at[:, 0:3], halo_s.at[10], halo_r.at[10], peer(east, lat + 1)),
                remote(fo.at[:, 24:27], fs, halo_s.at[11], halo_r.at[11], peer(lon, lat + 1))]

    def place(s):
        early = s < FIRST
        paired = jnp.logical_and(s >= EDGE, s < PAIRED)
        both = jnp.logical_or(early, paired)
        base = jnp.where(early, 2 * s, jnp.where(paired, 2 * (s - EDGE), jnp.where(s < EDGE, s + 12 - FIRST, s - 4)))
        late = jnp.where(paired, 1, 0)
        return (base, base + jnp.where(both, 1, 0)), (late, jnp.where(early, 0, 1))

    def gather(s, x2, g2):
        t_of, c_of = place(s)
        for w in range(2):
            b = t_of[w] // 4
            r0 = b * 6 + 3
            pick = jnp.where(c_of[w] == 1, b, 4)
            corner = jnp.where(jnp.logical_and(c_of[w] == 1, b == 3), 1, 0)
            for n, (arr, ext, dst) in enumerate(((xo, xe, x2), (go, ge, g2))):
                halves = []
                for dz in range(2):
                    z = (t_of[w] % 4 * 2 + dz + 1) % 8
                    ze = jnp.where(s < FIRST, 8, z)
                    zp = jnp.where(s < FIRST, 4, z // 2)
                    own = arr[z, pl.ds(r0, 6)].astype(F32).reshape(144, C).astype(BF)
                    rest = hx[n, zp, 2].astype(F32)
                    rest = jnp.where(z % 2 == 1, rest[:, 64:], rest[:, :64]).astype(BF)
                    east_cols = jnp.concatenate([hx[n, zp, z % 2], rest], axis=1)
                    ex = ext[ze].astype(F32).reshape(24, C).astype(BF)
                    halves.append(dot(so_ref[c_of[w]], own) + dot(se_ref[pick], east_cols) + dot(sse_ref[corner], ex))
                dst[w * WTOK:(w + 1) * WTOK] = jnp.concatenate(halves, axis=0).astype(BF)

    def scatter(s, gin):
        t_of, c_of = place(s)
        for w in range(2):
            r0 = t_of[w] // 4 * 6 + 3
            for dz in range(2):
                z = (t_of[w] % 4 * 2 + dz + 1) % 8
                lo = w * WTOK + dz * 72
                part = gin[lo:lo + 72].astype(BF)
                own = dot(to_ref[c_of[w]], part).reshape(6, 24, C)
                fo[z, pl.ds(r0, 6)] = (fo[z, pl.ds(r0, 6)].astype(F32) + own).astype(BF)
                ex = dot(te_ref[c_of[w]], part).reshape(6, 8, C)
                fe[z, pl.ds(r0, 6)] = (fe[z, pl.ds(r0, 6)].astype(F32) + ex).astype(BF)

    sets = ((x2, g2, pr, dmx, sc, dpc), (x2b, g2b, prb, dmxb, scb, dpcb))

    def comm(s):
        @pl.when(s == FIRST - 1)
        def _():
            for cp in halo("e"):
                cp.wait_recv()

        @pl.when(jnp.logical_and(s == FIRST - 1, has_south))
        def _():
            for cp in halo("s"):
                cp.wait_recv()

        for k in (8, 7, 6, 5, 4, 3, 2):
            run_stage(k, s)

        for part, when in ((0, EDGE), (1, EDGE + 2), (2, EDGE + 4), (3, NT)):
            @pl.when(s == when)
            def _(part=part):
                for cp in strips(part):
                    cp.start()

        @pl.when(jnp.logical_and(s == EDGE, has_south))
        def _():
            for cp in strips(4):
                cp.start()

    def begin(s, buf):
        gather(s, buf[0], buf[1])
        score_part(*buf, wq_ref, wpt_ref)

    def work(s, buf, after):
        t_of, _c = place(s)
        softmax_part(t_of, buf[4], buf[5], pbs, gbs, bm_ref, bt_ref, gsum, gbuf)
        if after is not None:
            begin(s + 1, after)
        scatter(s, closing_part(*buf[:4], pbs, gbs, wqt_ref, gq, gp))

    def two_steps(i, last):
        comm(2 * i)
        work(2 * i, sets[0], sets[1])
        run_stage(1, 2 * i)
        comm(2 * i + 1)
        work(2 * i + 1, sets[1], None if last else sets[0])
        run_stage(1, 2 * i + 1)

    def looped(i, _):
        two_steps(i, False)
        return 0

    begin(0, sets[0])
    lax.fori_loop(0, NT // 2 - 1, looped, 0)
    two_steps(NT // 2 - 1, True)
    w_stage(1)

    def tail(s, _):
        comm(s)
        for k in (7, 6, 5, 4, 3, 2):
            @pl.when(s == W_AT[k])
            def _(k=k):
                w_stage(k)
        return 0

    lax.fori_loop(NT, STEPS, tail, 0)

    for part in range(4):
        for cp in strips(part):
            cp.wait_recv()
            cp.wait_send()

    @pl.when(has_north)
    def _():
        for cp in strips(4):
            cp.wait_recv()

    @pl.when(has_south)
    def _():
        for cp in strips(4):
            cp.wait_send()

    def finish(z, _):
        out_ref[z] = fo[z, 0:24]
        out_ref[z, 0:3] = fs[z]
        out_ref[z, :, 0:8] = add(out_ref[z, :, 0:8], fw[z, 0:24])
        return 0

    lax.fori_loop(0, 8, finish, 0)

    for cp in halo("e"):
        cp.wait_send()

    @pl.when(has_north)
    def _():
        for cp in halo("s"):
            cp.wait_send()

    w_done(1, wf).wait_send()
    for _ in range(4):
        w_done(2, wx).wait_send()
    for k in range(1, 8):
        ref = volume[k - 1]
        remote(ref, ref, ss.at[k - 1], rs.at[k - 1, 0], peer(partner, lat)).wait_send()
    pltpu.make_async_copy(fin, f_hbm, out_sem).wait()


def fused(normed, cotangent, weight_qkv, weight_proj, bias_view):
    vm = pl.BlockSpec(memory_space=pltpu.VMEM)
    hbm = pl.BlockSpec(memory_space=pl.ANY)
    V = pltpu.VMEM
    return pl.pallas_call(
        fused_kernel,
        in_specs=[hbm, hbm, vm, vm, hbm],
        out_specs=[vm, vm, hbm],
        out_shape=[
            jax.ShapeDtypeStruct(normed.shape, BF),
            jax.ShapeDtypeStruct((72, 16, 128), BF),
            jax.ShapeDtypeStruct((NT, 64, 16, 128), BF),
        ],
        scratch_shapes=[
            V((8, 27, 24, C), BF), V((8, 27, 24, C), BF), V((9, 3, 8, C), BF), V((9, 3, 8, C), BF),
            V((2 * WTOK, C), BF), V((2 * WTOK, C), BF), V((2 * WTOK, 768), BF), V((2 * WTOK, C), BF),
            V((2, WTOK, PACK), F32), V((2, WTOK, PACK), F32),
            V((2 * WTOK, C), BF), V((2 * WTOK, C), BF), V((2 * WTOK, 768), BF), V((2 * WTOK, C), BF),
            V((2, WTOK, PACK), F32), V((2, WTOK, PACK), F32),
            V((2, WTOK, PACK), BF), V((2, WTOK, PACK), BF),
            V((8, 27, 24, C), BF), V((8, 27, 8, C), BF), V((8, 27, 8, C), BF), V((8, 3, 24, C), BF),
            V((3, C, C), F32), V((C, C), F32), V((NT, WTOK, PACK), F32),
            V((NT, 64, 16, 128), BF), V((NT, 32, 16, 128), BF), V((NT, 32, 16, 128), BF),
            V((NT, 8, 16, 128), BF), V((NT, 16, 16, 128), BF), V((NT, 16, 16, 128), BF),
            V((NT, 8, 16, 128), BF), V((NT, 8, 16, 128), BF), V((NT, 64, 16, 128), BF),
            V((72, 16, 128), BF), V((36, 16, 128), BF), V((36, 16, 128), BF), V((3, 9, 16, 128), BF),
            V((4, 9, 16, 128), BF), V((4, 9, 16, 128), BF), V((72, 16, 128), BF),
            V((C, 768), BF), V((3, C, C), BF), V((C, C), BF),
            V((2, 72, 144), BF), V((5, 72, 128), BF), V((2, 144, 72), BF), V((2, 48, 72), BF),
            V((NT, WTOK, 6 * MAIN), BF), V((NT, 96, WTOK), BF), V((2, NT, WTOK * WTOK), BF),
            V((2, WTOK * ST, 128), F32), V((2, 4, 3, 128, 128), BF), V((2, 5, 3, 128, 128), BF),
            V((128, 168), BF), V((2, 72, 24), BF), pltpu.SemaphoreType.DMA((2,)),
            pltpu.SemaphoreType.DMA((2,)), pltpu.SemaphoreType.DMA((12,)), pltpu.SemaphoreType.DMA((12,)),
            pltpu.SemaphoreType.DMA((7,)), pltpu.SemaphoreType.DMA((7, NT)),
            pltpu.SemaphoreType.DMA((2,)), pltpu.SemaphoreType.DMA((6,)), pltpu.SemaphoreType.DMA,
        ],
        compiler_params=pltpu.CompilerParams(collective_id=0, has_side_effects=True, vmem_limit_bytes=66_000_000),
        name="fused",
    )(normed, cotangent, weight_qkv, weight_proj, bias_view)


def local(normed, cotangent, weight_qkv, weight_proj, bias_table):
    input_grad, w, f = fused(normed, cotangent, weight_qkv, weight_proj, bias_table.transpose(1, 0, 2))
    bias_grad, qkv_grad, proj_grad = unpack(f, w)
    return input_grad, qkv_grad, proj_grad, bias_grad.transpose(1, 0, 2)


def solution(mesh):
    in_specs = (P(None, "lat", "lon", None), P(None, "lat", "lon", None), P(), P(), P("lat", None, None))
    out_specs = (P(None, "lat", "lon", None), P(), P(), P("lat", None, None))
    return jax.shard_map(local, mesh=mesh, in_specs=in_specs, out_specs=out_specs, check_vma=False)
```

```python
import functools
import jax
import jax.numpy as jnp
from jax import lax
from jax.experimental import pallas as pl
from jax.experimental.pallas import tpu as pltpu
from jax.sharding import PartitionSpec as P

HEADS = 6
WTOK = 144
HD = 32
C = 192
MAIN = 128
TAIL = WTOK - MAIN
PACK = 896
NT = 16
SCALE = HD ** -0.5
LOG2E = 1.4426950408889634
BF = jnp.bfloat16
F32 = jnp.float32
MESH = pl.DeviceIdType.MESH
FIRST = 5
EDGE = 9
PAIRED = 14
STEPS = 35
OFFSET = (0, 0, 2, 5, 8, 11, 14, 17, 19)
W_AT = (0, 0, 17, 20, 23, 26, 29, 31)
ST = 17
MASKED = -1e30


def dot(a, b):
    return jnp.dot(a, b, preferred_element_type=F32)


def lane_head(shape):
    return lax.broadcasted_iota(jnp.int32, shape, 1) // HD


def pack_head(b_ref, main_ref, tail_ref, sc, lanes, rows):
    lane = lax.broadcasted_iota(jnp.int32, (NT, 128), 1)

    def group(g, _):
        base = pl.multiple_of(g * 1152, 128)
        tiles = [b_ref[:, pl.ds(base + 128 * j, 128)].astype(F32) for j in range(9)]
        for j in range(8):
            if j == 0:
                main, sec = tiles[0], tiles[1]
            else:
                r = pltpu.roll(tiles[j], 128 - 16 * j, 1)
                sec = pltpu.roll(tiles[j + 1], 128 - 16 * j, 1)
                main = jnp.where(lane < 128 - 16 * j, r, sec)
            row = g * (8 * ST) + ST * j
            sc[0, pl.ds(row, NT), :] = main
            sc[1, pl.ds(row, NT), :] = sec
        return 0

    lax.fori_loop(0, 18, group, 0, unroll=9)
    last = (lax.axis_index("lat") == 7).astype(F32)

    def half(n):
        return jnp.logical_or(jnp.logical_and(n >= 36, n < 72), n >= 108)

    def masks(shape, k_axis, q_first):
        k = lax.broadcasted_iota(jnp.int32, shape, k_axis)
        q = lax.broadcasted_iota(jnp.int32, shape, 1 - k_axis)
        q = q if q_first == 0 else q * 0 + q_first
        z_no = jnp.logical_xor(k >= 72, q >= 72)
        l_no = jnp.logical_xor(half(k), half(q))
        return jnp.where(z_no, MASKED, 0.0), jnp.where(l_no, MASKED, 0.0) * last

    z_main, l_main = masks((WTOK, MAIN), 0, 0)
    z_tail, l_tail = masks((16, WTOK), 1, 128)

    def masked(x, t, z, l):
        if t % 4 != 3 and t // 4 != 3:
            return x
        y = x.astype(F32)
        if t % 4 == 3:
            y = y + z
        if t // 4 == 3:
            y = y + l
        return y.astype(BF)

    for t in range(NT):
        a = sc[0, pl.ds(t, WTOK, stride=ST), :].astype(BF)
        b = sc[1, pl.ds(t, WTOK, stride=ST), :].astype(BF)
        main_ref[t, 0:128, lanes] = masked(a[:MAIN].T, t, z_main[:128], l_main[:128])
        main_ref[t, 128:144, lanes] = masked(b[:MAIN].T[:16], t, z_main[128:], l_main[128:])
        tail_ref[t, rows, 0:128] = masked(a[MAIN:], t, z_tail[:, :128], l_tail[:, :128])
        tail_ref[t, rows, 128:144] = masked(b[MAIN:, 0:16], t, z_tail[:, 128:], l_tail[:, 128:])


def unpack_kernel(m_ref, t_ref, w_ref, out_ref, gq_ref, gp_ref, sc, tn):
    h = pl.program_id(0)

    @pl.when(h == 0)
    def _():
        for t in range(NT):
            tn[t] = t_ref[t].reshape(WTOK, 128).T
        for i in range(3):
            gq_ref[:, C * i:C * i + 128] = w_ref[24 * i:24 * i + 12].reshape(C, 128).astype(F32)
            rest = w_ref[24 * i + 12:24 * i + 24].reshape(C, 128).astype(F32)
            gq_ref[:, C * i + 128:C * i + C] = rest[:, :64]
            gp_ref[:, 64 * i:64 * i + 64] = rest[:, 64:]

    for t in range(NT):
        m = m_ref[t].reshape(WTOK, 128)
        sc[0, pl.ds(t, MAIN, stride=ST), :] = m[:MAIN].T.astype(F32)
        sc[1, pl.ds(t, MAIN, stride=ST), 0:16] = m[MAIN:].T.astype(F32)
        tl = tn[t, pl.ds(pl.multiple_of(h * 16, 16), 16), :].astype(F32)
        sc[0, pl.ds(MAIN * ST + t, 16, stride=ST), :] = tl[:, :128]
        sc[1, pl.ds(MAIN * ST + t, 16, stride=ST), 0:16] = tl[:, 128:]
    lane = lax.broadcasted_iota(jnp.int32, (NT, 128), 1)

    def group(g, _):
        base = pl.multiple_of(g * 1152, 128)
        r, s = [], []
        for j in range(8):
            row = g * (8 * ST) + ST * j
            m = sc[0, pl.ds(row, NT), :]
            t = sc[1, pl.ds(row, NT), :]
            r.append(pltpu.roll(m, 16 * j, 1) if j else m)
            s.append(pltpu.roll(t, 16 * j, 1) if j else t)
        for j in range(9):
            if j == 0:
                v = r[0]
            else:
                low = jnp.where(lane < 16 * (j - 1), r[j - 1], s[j - 1]) if j > 1 else s[0]
                v = jnp.where(lane < 16 * j, low, r[j]) if j < 8 else low
            out_ref[0, :, pl.ds(base + 128 * j, 128)] = v
        return 0

    lax.fori_loop(0, 18, group, 0, unroll=9)


def unpack(f, w):
    return pl.pallas_call(
        unpack_kernel, grid=(6,),
        in_specs=[pl.BlockSpec((NT, 9, 16, 128), lambda h: (0, h, 0, 0)),
                  pl.BlockSpec((NT, 9, 16, 128), lambda h: (0, 6, 0, 0)),
                  pl.BlockSpec((72, 16, 128), lambda h: (0, 0, 0))],
        out_specs=[pl.BlockSpec((1, NT, WTOK * WTOK), lambda h: (h, 0, 0)),
                   pl.BlockSpec((C, 3 * C), lambda h: (0, 0)), pl.BlockSpec((C, C), lambda h: (0, 0))],
        out_shape=[jax.ShapeDtypeStruct((6, NT, WTOK * WTOK), F32), jax.ShapeDtypeStruct((C, 3 * C), F32),
                   jax.ShapeDtypeStruct((C, C), F32)],
        scratch_shapes=[pltpu.VMEM((2, WTOK * ST, 128), F32), pltpu.VMEM((NT, 128, WTOK), BF)], name="unpack",
        cost_estimate=pl.CostEstimate(flops=10**9, bytes_accessed=12 * 2**20, transcendentals=0),
    )(f, f, w)


def add(*parts):
    total = parts[0].astype(F32)
    for part in parts[1:]:
        total = total + part.astype(F32)
    return total.astype(BF)


def blk(at, p):
    zq = jnp.zeros((HD, MAIN), BF)
    top = jnp.concatenate([at[64 * p:64 * p + 32, :MAIN], zq], axis=1)
    bot = jnp.concatenate([zq, at[64 * p + 32:64 * p + 64, :MAIN]], axis=1)
    two = jnp.concatenate([top, bot], axis=0)
    if p == 2:
        return two
    z64 = jnp.zeros((64, 256), BF)
    return jnp.concatenate([two, z64] if p == 0 else [z64, two], axis=0)


def nat(a, p):
    lanes = slice(0, 128) if p < 2 else slice(128, 192)
    am = a[:MAIN, lanes]
    hh = lane_head((MAIN, C))[:, lanes]
    z = jnp.zeros_like(am)
    return jnp.concatenate([jnp.where(hh == 2 * p, am, z), jnp.where(hh == 2 * p + 1, am, z)], axis=0)


def nat_tail(a):
    am = a[MAIN:]
    ht = lane_head((TAIL, C))
    z = jnp.zeros_like(am)
    return jnp.concatenate([jnp.where(ht == h, am, z) for h in range(HEADS)], axis=0)


def score_part(x2, g2, pr, dmx, sc, dpc, wq_ref, wpt_ref):
    proj = dot(x2[...], wq_ref[...]).astype(BF)
    dmix = dot(g2[...], wpt_ref[...]).astype(BF)
    pr[...] = proj
    dmx[...] = dmix
    dn = (((1,), (1,)), ((), ()))
    for w in range(2):
        rows = slice(w * WTOK, (w + 1) * WTOK)
        q, k, v, dm = proj[rows, 0:192], proj[rows, 256:448], proj[rows, 512:704], dmix[rows]
        qt, dmt = q.T, dm.T
        for p in range(3):
            sub = slice(0, 128) if p < 2 else slice(128, 192)
            ln = slice(256 * p, 256 * p + 256)
            sc[w, :, ln] = dot(k[:, sub], blk(qt, p))
            dpc[w, :, ln] = dot(v[:, sub], blk(dmt, p))
        sc[w, :, 768:864] = lax.dot_general(k, nat_tail(q), dn, preferred_element_type=F32)
        dpc[w, :, 768:864] = lax.dot_general(v, nat_tail(dm), dn, preferred_element_type=F32)


def softmax_part(t_of, sc, dpc, pbs, gbs, bm_ref, bt_ref, gsum, gbuf):
    for w in range(2):
        t = t_of[w]
        for j in range(7):
            width = 128 if j < 6 else 96
            ln = slice(128 * j, 128 * j + width)
            bias = (bm_ref[t, :, ln] if j < 6 else bt_ref[t].T).astype(F32)
            z = sc[w, :, ln] * (SCALE * LOG2E) + bias * LOG2E
            m = jnp.max(z, axis=0, keepdims=True)
            e = jnp.exp2(z - m)
            r = 1.0 / jnp.sum(e, axis=0, keepdims=True)
            prob = e * r
            pbs[w, :, ln] = prob.astype(BF)
            dp = dpc[w, :, ln]
            d = jnp.sum(prob * dp, axis=0, keepdims=True)
            gs = prob * (dp - d)
            gbs[w, :, ln] = gs.astype(BF)
            tot = gsum[t, :, ln] + gs
            gsum[t, :, ln] = tot
            gbuf[t, 9 * j:9 * j + 9, :, 0:width] = tot.astype(BF).reshape(9, 16, width)


def closing_part(x2, g2, pr, dmx, pbs, gbs, wqt_ref, gq, gp):
    x = x2[...]
    cot = g2[...]
    proj = pr[...]
    xt = x.T
    ht = lane_head((TAIL, C))
    dq_l, dk_l, dv_l, mixm, mixt, cott = [], [], [], [], [], []
    for w in range(2):
        rows = slice(w * WTOK, (w + 1) * WTOK)
        q, k, v = proj[rows, 0:192], proj[rows, 256:448], proj[rows, 512:704]
        dm = dmx[rows]
        kt, vt = k.T, v.T
        q_tail, dm_tail = nat_tail(q), nat_tail(dm)
        mix_parts, dq_parts, dkp, dvp = [], [], [], []
        for p in range(3):
            pb = pbs[w, :, 256 * p:256 * p + 256]
            gb = gbs[w, :, 256 * p:256 * p + 256]
            mo = dot(vt[64 * p:64 * p + 64], pb).astype(BF)
            do = dot(kt[64 * p:64 * p + 64], gb)
            mix_parts += [mo[:32, :MAIN], mo[32:, MAIN:]]
            dq_parts += [do[:32, :MAIN], do[32:, MAIN:]]
            dkp.append(dot(gb, nat(q, p)))
            dvp.append(dot(pb, nat(dm, p)))
        pb = pbs[w, :, 768:864]
        gb = gbs[w, :, 768:864]
        mo = dot(vt, pb).astype(BF)
        do = (dot(kt, gb) * SCALE).astype(BF)
        rh = lax.broadcasted_iota(jnp.int32, (C, 96), 0) // HD
        lh = lax.broadcasted_iota(jnp.int32, (C, 96), 1) // TAIL
        mixt.append(jnp.where(rh == lh, mo, jnp.zeros_like(mo)))
        dot_t = do.T
        dq_tail = jnp.zeros((TAIL, C), BF)
        for h in range(HEADS):
            dq_tail = jnp.where(ht == h, dot_t[TAIL * h:TAIL * h + TAIL], dq_tail)
        dk_a = dkp[0] + dkp[1] + dot(gb, q_tail[:, :128])
        dk_b = dkp[2] + dot(gb, q_tail[:, 128:])
        dv_a = dvp[0] + dvp[1] + dot(pb, dm_tail[:, :128])
        dv_b = dvp[2] + dot(pb, dm_tail[:, 128:])
        mixm.append(jnp.concatenate(mix_parts, axis=0))
        dqt = (jnp.concatenate(dq_parts, axis=0) * SCALE).astype(BF)
        dq_l.append(jnp.concatenate([dqt.T, dq_tail], axis=0))
        dk_l.append((jnp.concatenate([dk_a, dk_b], axis=1) * SCALE).astype(BF))
        dv_l.append(jnp.concatenate([dv_a, dv_b], axis=1).astype(BF))
        cott.append(jnp.concatenate([cot[rows][MAIN:]] * HEADS, axis=0))
    mm = jnp.concatenate(mixm, axis=1)
    cm = jnp.concatenate([cot[0:MAIN], cot[WTOK:WTOK + MAIN]], axis=0)
    gp[...] += dot(mm, cm) + dot(mixt[0], cott[0]) + dot(mixt[1], cott[1])
    dq = jnp.concatenate(dq_l, axis=0)
    dk = jnp.concatenate(dk_l, axis=0)
    dv = jnp.concatenate(dv_l, axis=0)
    gq[0] += dot(xt, dq)
    gq[1] += dot(xt, dk)
    gq[2] += dot(xt, dv)
    return dot(dq, wqt_ref[0]) + dot(dk, wqt_ref[1]) + dot(dv, wqt_ref[2])


def fused_kernel(x_hbm, g_hbm, wqkv_ref, wproj_ref, bias_hbm, out_ref, w_ref, f_hbm,
                 xo, go, xe, ge, x2, g2, pr, dmx, sc, dpc, x2b, g2b, prb, dmxb, scb, dpcb, pbs, gbs, fo, fe, fw, fs, gq, gp, gsum, gbuf, rd, hb, xa, xs, xb, ys, yr, fin,
                 wb, wr, wh, wx, wy, wz, wf, wq_ref, wqt_ref, wpt_ref, so_ref, se_ref, to_ref, te_ref,
                 bm_ref, bt_ref, bias_in, psc, hs, hx, cs_ref, sse_ref,
                 bias_sem, load_sem, halo_s, halo_r, ss, rs, ws, wrs, out_sem):
    lon = lax.axis_index("lon")
    lat = lax.axis_index("lat")
    n_lon = 16
    core = lon % 2
    yh = (lon // 2) % 2
    xx = lon // 4
    zz = lat % 4
    yl = lat // 4
    yy = yh * 2 + yl
    partner = lon + 1 - 2 * core
    right = (lon + 4) % n_lon
    left = (lon + 12) % n_lon
    ymate = lon + 2 - 4 * yh
    east = (lon + 1) % n_lon
    west = (lon + 15) % n_lon
    has_south = lat < 7
    has_north = lat > 0

    def peer(lon_, lat_):
        return {"lon": lon_, "lat": lat_}

    def xpeer(d):
        return peer((xx + d) % 4 * 4 + yh * 2 + core, lat)

    def ypeer(d):
        o = (yy + d) % 4
        return peer(xx * 4 + o // 2 * 2 + core, o % 2 * 4 + zz)

    def zpeer(d):
        return peer(lon, yl * 4 + (zz + d) % 4)

    def remote(src, dst, ssem, rsem, dev):
        return pltpu.make_async_remote_copy(src_ref=src, dst_ref=dst, send_sem=ssem, recv_sem=rsem,
                                            device_id=dev, device_id_type=MESH)

    own_loads = [pltpu.make_async_copy(x_hbm, xo.at[:, 0:24], load_sem.at[0]),
                 pltpu.make_async_copy(g_hbm, go.at[:, 0:24], load_sem.at[1])]
    for cp in own_loads:
        cp.start()
    for buf in (xe, ge):
        buf[...] = jnp.zeros_like(buf)
    for buf in (xo, go):
        buf[:, 24:27] = jnp.zeros((8, 3, 24, C), BF)
    for buf in (fw, fs):
        buf[...] = jnp.zeros_like(buf)

    for i in range(3):
        part = wqkv_ref[:, C * i:C * i + C]
        wq_ref[:, 256 * i:256 * i + C] = part
        wq_ref[:, 256 * i + C:256 * i + 256] = jnp.zeros((C, 64), BF)
        wqt_ref[i] = part.T
    wpt_ref[...] = wproj_ref[...].T
    def token(shape, axis):
        tok = lax.broadcasted_iota(jnp.int32, shape, axis)
        row = jnp.zeros(shape, jnp.int32)
        for m in range(1, 6):
            row = row + (tok >= 12 * m).astype(jnp.int32)
        return row, tok - 12 * row, lax.broadcasted_iota(jnp.int32, shape, 1 - axis)

    def one_hot(hit):
        return jnp.where(hit, 1.0, 0.0).astype(BF)

    for c in range(2):
        for ref, width, over, axis in ((so_ref, 24, False, 0), (to_ref, 24, False, 1), (te_ref, 8, True, 1)):
            row, col, at = token(ref.shape[1:], axis)
            col = col + 6 + 12 * c
            hit = at == row * width + col - (24 if over else 0)
            ref[c] = one_hot(jnp.logical_and(hit, col >= 24 if over else col < 24))
    for b in range(4):
        row, col, at = token((72, 128), 0)
        hit = jnp.logical_and(at == 36 * b + 6 * row + col - 6, col >= 6)
        se_ref[b] = one_hot(jnp.logical_and(hit, row < 3) if b == 3 else hit)
    se_ref[4] = jnp.zeros((72, 128), BF)
    row, col, at = token((72, 24), 0)
    sse_ref[0] = jnp.zeros((72, 24), BF)
    sse_ref[1] = one_hot(jnp.logical_and(at == 8 * row - 24 + col - 6, jnp.logical_and(row >= 3, col >= 6)))
    kept_row = lax.broadcasted_iota(jnp.int32, (128, 168), 0)
    group = jnp.zeros((128, 168), jnp.int32)
    for m in range(1, 21):
        group = group + (kept_row >= 6 * m).astype(jnp.int32)
    at = lax.broadcasted_iota(jnp.int32, (128, 168), 1)
    cs_ref[...] = one_hot(jnp.logical_and(at == kept_row + 2 * group, kept_row < 126))
    hx[:, 4] = jnp.zeros((2, 3, 128, 128), BF)

    barrier = pltpu.get_barrier_semaphore()
    greet = [peer(partner, lat), xpeer(1), xpeer(2), xpeer(3)] + [ypeer(d) for d in (1, 2, 3)] + [zpeer(d) for d in (1, 2, 3)]
    for dev in greet:
        pl.semaphore_signal(barrier, inc=1, device_id=dev, device_id_type=MESH)
    for dev in (peer(east, lat), peer(west, lat)):
        pl.semaphore_signal(barrier, inc=1, device_id=dev, device_id_type=MESH)

    @pl.when(has_north)
    def _():
        pl.semaphore_signal(barrier, inc=1, device_id=peer(lon, lat - 1), device_id_type=MESH)
        pl.semaphore_signal(barrier, inc=1, device_id=peer(west, lat - 1), device_id_type=MESH)

    @pl.when(has_south)
    def _():
        pl.semaphore_signal(barrier, inc=1, device_id=peer(lon, lat + 1), device_id_type=MESH)
        pl.semaphore_signal(barrier, inc=1, device_id=peer(east, lat + 1), device_id_type=MESH)

    pl.semaphore_wait(barrier, 12 + 2 * has_north.astype(jnp.int32) + 2 * has_south.astype(jnp.int32))

    def halo(which):
        out = []
        for n, (src, ext, own) in enumerate(((x_hbm, xe, xo), (g_hbm, ge, go))):
            if which == "e":
                out.append(remote(hs.at[n], hx.at[n, 0:4], halo_s.at[n], halo_r.at[n], peer(west, lat)))
            if which == "s":
                out.append(remote(src.at[:, 0:3], own.at[:, 24:27], halo_s.at[2 + n], halo_r.at[2 + n],
                                  peer(lon, lat - 1)))
                out.append(remote(src.at[:, 0:3, 0:8], ext.at[0:8], halo_s.at[4 + n], halo_r.at[4 + n],
                                  peer(west, lat - 1)))
        return out

    @pl.when(has_north)
    def _():
        for cp in halo("s"):
            cp.start()

    for cp in own_loads:
        cp.wait()
    for n, arr in enumerate((xo, go)):
        for zp in range(4):
            kept = []
            for dz in range(2):
                edge = arr[2 * zp + dz, 3:24, 0:8].astype(F32).reshape(168, C).astype(BF)
                kept.append(dot(cs_ref[...], edge).astype(BF))
            hs[n, zp, 0] = kept[0][:, :128]
            hs[n, zp, 1] = kept[1][:, :128]
            hs[n, zp, 2] = jnp.concatenate([kept[0][:, 128:], kept[1][:, 128:]], axis=1)
    for cp in halo("e"):
        cp.start()

    def bias_load(h):
        return pltpu.make_async_copy(bias_hbm.at[h], bias_in.at[h % 2], bias_sem.at[h % 2])

    bias_load(0).start()
    gq[...] = jnp.zeros_like(gq)
    gp[...] = jnp.zeros_like(gp)
    fe[...] = jnp.zeros_like(fe)

    def clear(t, _):
        gsum[t] = jnp.zeros((WTOK, PACK), F32)
        gbuf[t, 54:64] = jnp.zeros((10, 16, 128), BF)
        return 0

    lax.fori_loop(0, NT, clear, 0)

    def clear_out(z, _):
        fo[z] = jnp.zeros((27, 24, C), BF)
        return 0

    lax.fori_loop(0, 8, clear_out, 0)
    def pack_one(h, _):
        @pl.when(h < HEADS - 1)
        def _():
            bias_load(h + 1).start()
        bias_load(h).wait()
        pack_head(bias_in.at[h % 2], bm_ref, bt_ref, psc, pl.ds(pl.multiple_of(h * MAIN, MAIN), MAIN),
                  pl.ds(pl.multiple_of(h * TAIL, TAIL), TAIL))
        return 0

    lax.fori_loop(0, HEADS, pack_one, 0)

    mine = core * 32
    other = 32 - mine
    o8 = (xx + 2) % 4 * 8
    r8 = (xx + 1) % 4 * 8
    l8 = (xx + 3) % 4 * 8
    m8 = xx * 8

    def stage_copies(k, t):
        def rc(src, dst, lon_):
            return remote(src, dst, ss.at[k - 1], rs.at[k - 1, t], peer(lon_, lat))
        if k == 1:
            return [rc(gbuf.at[t, pl.ds(other, 32)], rd.at[t], partner)]
        if k == 2:
            return [rc(hb.at[t, pl.ds(o8, 4)], xa.at[t, 0:4], right),
                    rc(hb.at[t, pl.ds(o8 + 4, 4)], xa.at[t, 4:8], left)]
        if k == 3:
            return [rc(xs.at[t, 0:8], xb.at[t, 0:8], right), rc(xs.at[t, 8:16], xb.at[t, 8:16], left)]
        if k == 4:
            return [rc(ys.at[t], yr.at[t], ymate)]
        if k == 5:
            here = fin.at[t, pl.ds(mine + m8, 8)]
            return [rc(here, here, right), rc(here, here, left)]
        if k == 6:
            a = fin.at[t, pl.ds(mine + l8, 4)]
            b = fin.at[t, pl.ds(mine + r8 + 4, 4)]
            return [rc(a, a, right), rc(b, b, left)]
        half = fin.at[t, pl.ds(mine, 32)]
        return [rc(half, half, partner)]

    volume = (rd, xa, xb, yr, xb, xa, rd)

    def stage_arrived(k, t):
        ref = volume[k - 1].at[t]
        remote(ref, ref, ss.at[k - 1], rs.at[k - 1, t], peer(partner, lat)).wait_recv()

    def stage(k, t):
        if k > 1:
            stage_arrived(k - 1, t)
        if k == 2:
            hb[t] = add(gbuf[t, pl.ds(mine, 32)], rd[t])
        if k == 3:
            xs[t, 0:4] = add(hb[t, pl.ds(r8, 4)], xa[t, 0:4])
            xs[t, 4:8] = hb[t, pl.ds(r8 + 4, 4)]
            xs[t, 8:12] = hb[t, pl.ds(l8, 4)]
            xs[t, 12:16] = add(hb[t, pl.ds(l8 + 4, 4)], xa[t, 4:8])
        if k == 4:
            ys[t] = add(hb[t, pl.ds(m8, 8)], xb[t, 0:8], xb[t, 8:16])
        if k == 5:
            fin[t, pl.ds(mine + m8, 8)] = add(ys[t], yr[t])
        if k < 8:
            for cp in stage_copies(k, t):
                cp.start()
        else:
            pltpu.make_async_copy(fin.at[t], f_hbm.at[t], out_sem).start()

    def run_stage(k, s):
        d = s - OFFSET[k]

        @pl.when(jnp.logical_and(d >= EDGE, d < PAIRED))
        def _():
            stage(k, 2 * (d - EDGE))
            stage(k, 2 * (d - EDGE) + 1)

        @pl.when(jnp.logical_or(jnp.logical_and(d >= FIRST, d < EDGE), jnp.logical_and(d >= PAIRED, d < NT)))
        def _():
            stage(k, jnp.where(d < EDGE, d + 12 - FIRST, d - 4))

    wm = core * 36
    wo = 36 - wm

    def w_copies(k):
        def rc(src, dst, dev):
            return remote(src, dst, ws.at[0 if k in (1, 6) else 1], wrs.at[k - 1], dev)
        if k == 1:
            return [rc(wb.at[pl.ds(wo, 36)], wr, peer(partner, lat))]
        if k == 2:
            return [rc(wh.at[pl.ds((xx + d) % 4 * 9, 9)], wx.at[d - 1], xpeer(d)) for d in (1, 2, 3)]
        if k == 3:
            return [rc(wy.at[yy], wy.at[yy], ypeer(d)) for d in (1, 2, 3)]
        if k == 4:
            return [rc(wz.at[zz], wz.at[zz], zpeer(d)) for d in (1, 2, 3)]
        if k == 5:
            here = wf.at[pl.ds(wm + xx * 9, 9)]
            return [rc(here, here, xpeer(d)) for d in (1, 2, 3)]
        half = wf.at[pl.ds(wm, 36)]
        return [rc(half, half, peer(partner, lat))]

    def w_done(k, ref):
        return remote(ref, ref, ws.at[0 if k in (1, 6) else 1], wrs.at[k - 1], peer(partner, lat))

    def w_stage(k):
        if k > 1:
            w_done(k - 1, wr if k in (2, 7) else wx).wait_recv()
        if k == 1:
            for i in range(3):
                wb[24 * i:24 * i + 12] = gq[i, :, 0:128].astype(BF).reshape(12, 16, 128)
                wb[24 * i + 12:24 * i + 24, :, 0:64] = gq[i, :, 128:192].astype(BF).reshape(12, 16, 64)
                wb[24 * i + 12:24 * i + 24, :, 64:128] = gp[:, 64 * i:64 * i + 64].astype(BF).reshape(12, 16, 64)
        if k == 2:
            wh[...] = add(wb[pl.ds(wm, 36)], wr[...])
        if k == 3:
            wy[yy] = add(wh[pl.ds(xx * 9, 9)], wx[0], wx[1], wx[2])
        if k == 4:
            wz[zz] = add(wy[0], wy[1], wy[2], wy[3])
        if k == 5:
            wf[pl.ds(wm + xx * 9, 9)] = add(wz[0], wz[1], wz[2], wz[3])
        if k < 7:
            for cp in w_copies(k):
                cp.start()
        else:
            w_ref[...] = wf[...]

    def strips(part):
        if part < 4:
            r = (21, 3, 9, 15)[part]
            n = 3 if part == 0 else 6
            return [remote(fe.at[:, r:r + n], fw.at[:, r:r + n], halo_s.at[6 + part], halo_r.at[6 + part], peer(east, lat))]
        return [remote(fe.at[:, 24:27], fw.at[:, 0:3], halo_s.at[10], halo_r.at[10], peer(east, lat + 1)),
                remote(fo.at[:, 24:27], fs, halo_s.at[11], halo_r.at[11], peer(lon, lat + 1))]

    def place(s):
        early = s < FIRST
        paired = jnp.logical_and(s >= EDGE, s < PAIRED)
        both = jnp.logical_or(early, paired)
        base = jnp.where(early, 2 * s, jnp.where(paired, 2 * (s - EDGE), jnp.where(s < EDGE, s + 12 - FIRST, s - 4)))
        late = jnp.where(paired, 1, 0)
        return (base, base + jnp.where(both, 1, 0)), (late, jnp.where(early, 0, 1))

    def gather(s, x2, g2):
        t_of, c_of = place(s)
        for w in range(2):
            b = t_of[w] // 4
            r0 = b * 6 + 3
            pick = jnp.where(c_of[w] == 1, b, 4)
            corner = jnp.where(jnp.logical_and(c_of[w] == 1, b == 3), 1, 0)
            for n, (arr, ext, dst) in enumerate(((xo, xe, x2), (go, ge, g2))):
                halves = []
                for dz in range(2):
                    z = (t_of[w] % 4 * 2 + dz + 1) % 8
                    ze = jnp.where(s < FIRST, 8, z)
                    zp = jnp.where(s < FIRST, 4, z // 2)
                    own = arr[z, pl.ds(r0, 6)].astype(F32).reshape(144, C).astype(BF)
                    rest = hx[n, zp, 2].astype(F32)
                    rest = jnp.where(z % 2 == 1, rest[:, 64:], rest[:, :64]).astype(BF)
                    east_cols = jnp.concatenate([hx[n, zp, z % 2], rest], axis=1)
                    ex = ext[ze].astype(F32).reshape(24, C).astype(BF)
                    halves.append(dot(so_ref[c_of[w]], own) + dot(se_ref[pick], east_cols) + dot(sse_ref[corner], ex))
                dst[w * WTOK:(w + 1) * WTOK] = jnp.concatenate(halves, axis=0).astype(BF)

    def scatter(s, gin):
        t_of, c_of = place(s)
        for w in range(2):
            r0 = t_of[w] // 4 * 6 + 3
            for dz in range(2):
                z = (t_of[w] % 4 * 2 + dz + 1) % 8
                lo = w * WTOK + dz * 72
                part = gin[lo:lo + 72].astype(BF)
                own = dot(to_ref[c_of[w]], part).reshape(6, 24, C)
                fo[z, pl.ds(r0, 6)] = (fo[z, pl.ds(r0, 6)].astype(F32) + own).astype(BF)
                ex = dot(te_ref[c_of[w]], part).reshape(6, 8, C)
                fe[z, pl.ds(r0, 6)] = (fe[z, pl.ds(r0, 6)].astype(F32) + ex).astype(BF)

    sets = ((x2, g2, pr, dmx, sc, dpc), (x2b, g2b, prb, dmxb, scb, dpcb))

    def comm(s):
        @pl.when(s == FIRST - 1)
        def _():
            for cp in halo("e"):
                cp.wait_recv()

        @pl.when(jnp.logical_and(s == FIRST - 1, has_south))
        def _():
            for cp in halo("s"):
                cp.wait_recv()

        for k in (8, 7, 6, 5, 4, 3, 2):
            run_stage(k, s)

        for part, when in ((0, EDGE), (1, EDGE + 2), (2, EDGE + 4), (3, NT)):
            @pl.when(s == when)
            def _(part=part):
                for cp in strips(part):
                    cp.start()

        @pl.when(jnp.logical_and(s == EDGE, has_south))
        def _():
            for cp in strips(4):
                cp.start()

    def begin(s, buf):
        gather(s, buf[0], buf[1])
        score_part(*buf, wq_ref, wpt_ref)

    def work(s, buf, after):
        t_of, _c = place(s)
        softmax_part(t_of, buf[4], buf[5], pbs, gbs, bm_ref, bt_ref, gsum, gbuf)
        if after is not None:
            begin(s + 1, after)
        scatter(s, closing_part(*buf[:4], pbs, gbs, wqt_ref, gq, gp))

    def two_steps(i, last):
        comm(2 * i)
        work(2 * i, sets[0], sets[1])
        run_stage(1, 2 * i)
        comm(2 * i + 1)
        work(2 * i + 1, sets[1], None if last else sets[0])
        run_stage(1, 2 * i + 1)

    def looped(i, _):
        two_steps(i, False)
        return 0

    begin(0, sets[0])
    lax.fori_loop(0, NT // 2 - 1, looped, 0)
    two_steps(NT // 2 - 1, True)
    w_stage(1)

    def tail(s, _):
        comm(s)
        for k in (7, 6, 5, 4, 3, 2):
            @pl.when(s == W_AT[k])
            def _(k=k):
                w_stage(k)
        return 0

    lax.fori_loop(NT, STEPS, tail, 0)

    for part in range(4):
        for cp in strips(part):
            cp.wait_recv()
            cp.wait_send()

    @pl.when(has_north)
    def _():
        for cp in strips(4):
            cp.wait_recv()

    @pl.when(has_south)
    def _():
        for cp in strips(4):
            cp.wait_send()

    def finish(z, _):
        out_ref[z] = fo[z, 0:24]
        out_ref[z, 0:3] = fs[z]
        out_ref[z, :, 0:8] = add(out_ref[z, :, 0:8], fw[z, 0:24])
        return 0

    lax.fori_loop(0, 8, finish, 0)

    for cp in halo("e"):
        cp.wait_send()

    @pl.when(has_north)
    def _():
        for cp in halo("s"):
            cp.wait_send()

    w_done(1, wf).wait_send()
    for _ in range(4):
        w_done(2, wx).wait_send()
    for k in range(1, 8):
        ref = volume[k - 1]
        remote(ref, ref, ss.at[k - 1], rs.at[k - 1, 0], peer(partner, lat)).wait_send()
    pltpu.make_async_copy(fin, f_hbm, out_sem).wait()


def fused(normed, cotangent, weight_qkv, weight_proj, bias_view):
    vm = pl.BlockSpec(memory_space=pltpu.VMEM)
    hbm = pl.BlockSpec(memory_space=pl.ANY)
    V = pltpu.VMEM
    return pl.pallas_call(
        fused_kernel,
        in_specs=[hbm, hbm, vm, vm, hbm],
        out_specs=[vm, vm, hbm],
        out_shape=[
            jax.ShapeDtypeStruct(normed.shape, BF),
            jax.ShapeDtypeStruct((72, 16, 128), BF),
            jax.ShapeDtypeStruct((NT, 64, 16, 128), BF),
        ],
        scratch_shapes=[
            V((8, 27, 24, C), BF), V((8, 27, 24, C), BF), V((9, 3, 8, C), BF), V((9, 3, 8, C), BF),
            V((2 * WTOK, C), BF), V((2 * WTOK, C), BF), V((2 * WTOK, 768), BF), V((2 * WTOK, C), BF),
            V((2, WTOK, PACK), F32), V((2, WTOK, PACK), F32),
            V((2 * WTOK, C), BF), V((2 * WTOK, C), BF), V((2 * WTOK, 768), BF), V((2 * WTOK, C), BF),
            V((2, WTOK, PACK), F32), V((2, WTOK, PACK), F32),
            V((2, WTOK, PACK), BF), V((2, WTOK, PACK), BF),
            V((8, 27, 24, C), BF), V((8, 27, 8, C), BF), V((8, 27, 8, C), BF), V((8, 3, 24, C), BF),
            V((3, C, C), F32), V((C, C), F32), V((NT, WTOK, PACK), F32),
            V((NT, 64, 16, 128), BF), V((NT, 32, 16, 128), BF), V((NT, 32, 16, 128), BF),
            V((NT, 8, 16, 128), BF), V((NT, 16, 16, 128), BF), V((NT, 16, 16, 128), BF),
            V((NT, 8, 16, 128), BF), V((NT, 8, 16, 128), BF), V((NT, 64, 16, 128), BF),
            V((72, 16, 128), BF), V((36, 16, 128), BF), V((36, 16, 128), BF), V((3, 9, 16, 128), BF),
            V((4, 9, 16, 128), BF), V((4, 9, 16, 128), BF), V((72, 16, 128), BF),
            V((C, 768), BF), V((3, C, C), BF), V((C, C), BF),
            V((2, 72, 144), BF), V((5, 72, 128), BF), V((2, 144, 72), BF), V((2, 48, 72), BF),
            V((NT, WTOK, 6 * MAIN), BF), V((NT, 96, WTOK), BF), V((2, NT, WTOK * WTOK), BF),
            V((2, WTOK * ST, 128), F32), V((2, 4, 3, 128, 128), BF), V((2, 5, 3, 128, 128), BF),
            V((128, 168), BF), V((2, 72, 24), BF), pltpu.SemaphoreType.DMA((2,)),
            pltpu.SemaphoreType.DMA((2,)), pltpu.SemaphoreType.DMA((12,)), pltpu.SemaphoreType.DMA((12,)),
            pltpu.SemaphoreType.DMA((7,)), pltpu.SemaphoreType.DMA((7, NT)),
            pltpu.SemaphoreType.DMA((2,)), pltpu.SemaphoreType.DMA((6,)), pltpu.SemaphoreType.DMA,
        ],
        compiler_params=pltpu.CompilerParams(collective_id=0, has_side_effects=True, vmem_limit_bytes=66_000_000),
        name="fused",
    )(normed, cotangent, weight_qkv, weight_proj, bias_view)


def local(normed, cotangent, weight_qkv, weight_proj, bias_table):
    input_grad, w, f = fused(normed, cotangent, weight_qkv, weight_proj, bias_table.transpose(1, 0, 2))
    bias_grad, qkv_grad, proj_grad = unpack(f, w)
    return input_grad, qkv_grad, proj_grad, bias_grad.transpose(1, 0, 2)


def solution(mesh):
    in_specs = (P(None, "lat", "lon", None), P(None, "lat", "lon", None), P(), P(), P("lat", None, None))
    out_specs = (P(None, "lat", "lon", None), P(), P(), P("lat", None, None))
    return jax.shard_map(local, mesh=mesh, in_specs=in_specs, out_specs=out_specs, check_vma=False)
```
